128 devices in a mesh: batch: 1, src: 16 (over z, y), graph: 8 (over x, core).
Axes of the slice: x: 4, y: 4, z: 4, core: 2. Of those that a mesh axis runs over, the one named last changes fastest.
Arguments:
- adj: bfloat16 [9216, 9216], P(('batch', 'graph'))
- sources: int32 [4096], P(('batch', 'src'))
- level_weight: float32 [2], replicated
Outputs:
- output: float32 [9216], P(('batch', 'graph'))
All inputs are finite; a program needn't handle non-finite values.
Results may differ from the reference program's by a relative error of at most 0.001.
Values are sent between devices in bfloat16 or wider.
A program may use at most 1 GiB of HBM per device.

```python
import jax
import jax.numpy as jnp
from jax import lax

GRID_X = 96
GRID_Y = 96
GRID_Z = 1
NUM_SOURCES = 4096
LEVELS = 3


def setup_inputs(seed: int = 0, part: int = 0) -> dict:
    vertex_count = GRID_X * GRID_Y * GRID_Z
    base_key = jax.random.key(seed)
    shared_key, part_root = jax.random.split(base_key)
    part_key = jax.random.fold_in(part_root, part)
    graph_key, source_key = jax.random.split(part_key)
    hidden = jax.random.permutation(graph_key, vertex_count)
    coord_x = hidden % GRID_X
    coord_y = (hidden // GRID_X) % GRID_Y
    coord_z = hidden // (GRID_X * GRID_Y)
    manhattan = (jnp.abs(coord_x[:, None] - coord_x[None, :])
                 + jnp.abs(coord_y[:, None] - coord_y[None, :])
                 + jnp.abs(coord_z[:, None] - coord_z[None, :]))
    adj = jnp.where(manhattan == 1, 1.0, 0.0).astype(jnp.float32).astype(jnp.bfloat16)
    sources = jax.random.permutation(source_key, vertex_count)[:NUM_SOURCES].astype(jnp.int32)
    level_weight = jax.random.uniform(shared_key, (LEVELS - 1,), jnp.float32, 0.5, 1.5)
    return {"adj": adj, "sources": sources, "level_weight": level_weight}


def reference(adj, sources, level_weight):
    vertex_count = GRID_X * GRID_Y * GRID_Z
    row_block = vertex_count // 8
    adj_blocks = adj.reshape(8, row_block, vertex_count)
    vertex_ids = jnp.arange(vertex_count, dtype=jnp.int32)
    sigma_zero = jnp.where(vertex_ids[:, None] == sources[None, :], 1.0, 0.0).astype(jnp.float32)

    def push_forward(sigma):
        sigma_blocks = sigma.reshape(8, row_block, NUM_SOURCES)

        def accumulate(acc, pair):
            adj_blk, sig_blk = pair
            return acc + jnp.dot(adj_blk.astype(jnp.float32).T, sig_blk, preferred_element_type=jnp.float32), None

        result, _ = lax.scan(accumulate, jnp.zeros_like(sigma), (adj_blocks, sigma_blocks))
        return result

    def pull_back(weights):
        def block_product(adj_blk):
            return jnp.dot(adj_blk.astype(jnp.float32), weights, preferred_element_type=jnp.float32)

        return lax.map(block_product, adj_blocks).reshape(vertex_count, NUM_SOURCES)

    def forward_step(carry, unused):
        sigma, seen = carry
        sigma_next = push_forward(sigma) * (1.0 - seen)
        seen_next = jnp.maximum(seen, jnp.where(sigma_next > 0, 1.0, 0.0))
        return (sigma_next, seen_next), sigma_next

    _, sigmas = lax.scan(forward_step, (sigma_zero, sigma_zero), None, length=LEVELS)
    uppers = sigmas[1:][::-1]
    lowers = sigmas[:-1][::-1]
    weights_by_level = level_weight[::-1]

    def backward_step(carry, level_inputs):
        delta, total = carry
        sig_upper, sig_lower, weight = level_inputs
        reached = sig_upper > 0
        weights = jnp.where(reached, (weight + delta) / jnp.where(reached, sig_upper, 1.0), 0.0)
        delta_next = sig_lower * pull_back(weights)
        return (delta_next, total + delta_next), None

    zero_mat = jnp.zeros_like(sigma_zero)
    (_, total), _ = lax.scan(backward_step, (zero_mat, zero_mat), (uppers, lowers, weights_by_level))
    scale = vertex_count / (NUM_SOURCES * LEVELS ** 3)
    return jnp.sum(total, axis=1) * scale
```

```python
import functools

import jax
import jax.numpy as jnp
from jax import lax
from jax.experimental import pallas as pl
from jax.experimental.pallas import tpu as pltpu
from jax.sharding import PartitionSpec as P

MESH = pl.DeviceIdType.MESH
f32, bf16 = jnp.float32, jnp.bfloat16
CHUNKS = 2
RIGHT, LEFT = 0, 1


def rows_cols(lhs, rhs):
    return lax.dot_general(lhs, rhs, (((1,), (0,)), ((), ())), preferred_element_type=f32)


def rows_rows(lhs, rhs):
    return lax.dot_general(lhs, rhs, (((1,), (1,)), ((), ())), preferred_element_type=f32)


def kernel(ring, planes, scale, adj, src, lw, out,
           a_blk, a_oth, m_oth, m_mrg, onehot, x1, x2own, x2rcv, part, wg,
           near0, far0, near, far, bc, bc_send, bc_recv, plane,
           load_sem, ssem, rsem, d2d_s, d2d_r, plane_s, plane_r):
    slab = a_oth.shape[0]
    cols_all = a_oth.shape[1]
    src_count = src.shape[0]
    m = src_count // CHUNKS
    h = m // 2
    tile = 2 * slab // 3
    ring_tiles = cols_all // tile
    blk = min(32, h)

    g = lax.axis_index("graph")
    s_me = lax.axis_index("src")
    x, c = g // 2, g % 2
    to_right = {"graph": lax.rem(x + 1, ring) * 2 + c}
    to_left = {"graph": lax.rem(x + ring - 1, ring) * 2 + c}
    to_mate = {"graph": x * 2 + (1 - c)}
    slots = (2, 1, ring - 1, 0)

    loads = []
    for i, off in enumerate(slots):
        chip = lax.rem(x + off, ring)
        at = pl.ds(pl.multiple_of((chip * 2 + (1 - c)) * slab, 128), slab)
        loads.append(pltpu.make_async_copy(adj.at[:, at], a_oth.at[:, pl.ds(i * slab, slab)], load_sem.at[i]))
    for i, off in enumerate(slots):
        chip = lax.rem(x + off, ring)
        at = pl.ds(pl.multiple_of((chip * 2 + c) * slab, 128), slab)
        loads.append(pltpu.make_async_copy(adj.at[:, at], a_blk.at[pl.ds(0, slab), pl.ds(i * slab, slab)], load_sem.at[4 + i]))
    for load in loads:
        load.start()

    barrier = pltpu.get_barrier_semaphore()
    for dev in (to_right, to_left, to_mate):
        pl.semaphore_signal(barrier, inc=1, device_id=dev, device_id_type=MESH)
    for o in range(1, planes):
        pl.semaphore_signal(barrier, inc=1, device_id={"src": lax.rem(s_me + o, planes)}, device_id_type=MESH)

    base = g * slab
    chip_base = x * 2 * slab
    ids = src[...]
    here = (ids >= base) & (ids < base + slab)
    lane = lax.broadcasted_iota(jnp.int32, (blk, slab), 1) + base

    def one_hot_rows(i, carry):
        r = pl.ds(pl.multiple_of(i * blk, blk), blk)
        onehot[r, :] = jnp.where(src[r, :] == lane, 1.0, 0.0).astype(bf16)
        return carry

    lax.fori_loop(0, src_count // blk, one_hot_rows, 0)
    bc[...] = jnp.zeros_like(bc)

    def mate_copy(i, source, target):
        return pltpu.make_async_remote_copy(src_ref=source, dst_ref=target, send_sem=d2d_s.at[i], recv_sem=d2d_r.at[i],
                                            device_id=to_mate, device_id_type=MESH)

    a_copies = [mate_copy(i, a_oth.at[:, pl.ds(i * slab, slab)], a_blk.at[pl.ds(slab, slab), pl.ds(i * slab, slab)])
                for i in range(4)]
    half_cols = [pl.ds(0, 2 * slab), pl.ds(2 * slab, 2 * slab)]
    m_copies = [mate_copy(4 + i, m_oth.at[:, half_cols[i]], m_mrg.at[:, half_cols[i]]) for i in range(2)]

    loads[0].wait()
    pl.semaphore_wait(barrier, 3 + planes - 1)
    a_copies[0].start()
    loads[1].wait()

    def select_other(t, carry):
        at = pl.ds(pl.multiple_of(t * tile, 128), tile)
        m_oth[:, at] = rows_cols(onehot[...], a_oth[:, at]).astype(bf16)
        return carry

    lax.fori_loop(0, 3, select_other, 0)
    m_copies[0].start()
    loads[2].wait()
    loads[3].wait()
    lax.fori_loop(3, 6, select_other, 0)
    m_copies[1].start()
    for i in range(1, 4):
        a_copies[i].start()

    def select_own(t, carry):
        at = pl.ds(pl.multiple_of(t * tile, 128), tile)
        mine = rows_cols(onehot[...], a_blk[pl.ds(0, slab), at])
        m_mrg[:, at] = jnp.where(here, mine, m_mrg[:, at].astype(f32)).astype(bf16)
        return carry

    for i in range(4, 8):
        loads[i].wait()
    m_copies[0].wait_recv()
    lax.fori_loop(0, 3, select_own, 0)
    m_copies[1].wait_recv()
    lax.fori_loop(3, 6, select_own, 0)

    lo, hi = pl.ds(0, h), pl.ds(h, h)
    slot = [pl.ds(i * slab, slab) for i in range(4)]
    own_half, mate_half = pl.ds(0, slab), pl.ds(slab, slab)

    def ring_copy(stage, k, way, msg, source, target):
        i = ((stage * CHUNKS + k) * 2 + way) * 3 + msg
        return pltpu.make_async_remote_copy(src_ref=source, dst_ref=target, send_sem=ssem.at[i], recv_sem=rsem.at[i],
                                            device_id=to_right if way == RIGHT else to_left, device_id_type=MESH)

    def reduce_copies(stage, k):
        if stage == 0:
            send, nr, fr = m_mrg.at[pl.ds(k * m, m), :], near0.at[k], far0.at[k]
        else:
            send, nr, fr = part.at[k], near.at[stage - 1, k], far.at[stage - 1, k]
        return {
            (RIGHT, 0): ring_copy(stage, k, RIGHT, 0, send.at[lo, slot[0]], fr.at[RIGHT]),
            (LEFT, 0): ring_copy(stage, k, LEFT, 0, send.at[hi, slot[0]], fr.at[LEFT]),
            (RIGHT, 1): ring_copy(stage, k, RIGHT, 1, send.at[hi, slot[1]], nr.at[RIGHT, hi, :]),
            (LEFT, 1): ring_copy(stage, k, LEFT, 1, send.at[lo, slot[2]], nr.at[LEFT, lo, :]),
            (RIGHT, 2): ring_copy(stage, k, RIGHT, 2, send.at[lo, slot[1]], nr.at[RIGHT, lo, :]),
            (LEFT, 2): ring_copy(stage, k, LEFT, 2, send.at[hi, slot[2]], nr.at[LEFT, hi, :]),
        }

    def gather_copies(stage, k):
        buf = wg.at[k] if stage == 3 else part.at[k]
        return {
            (RIGHT, 0): ring_copy(stage, k, RIGHT, 0, buf.at[lo, slot[3]], buf.at[lo, slot[2]]),
            (LEFT, 0): ring_copy(stage, k, LEFT, 0, buf.at[hi, slot[3]], buf.at[hi, slot[1]]),
            (RIGHT, 1): ring_copy(stage, k, RIGHT, 1, buf.at[hi, slot[3]], buf.at[hi, slot[2]]),
            (LEFT, 1): ring_copy(stage, k, LEFT, 1, buf.at[lo, slot[3]], buf.at[lo, slot[1]]),
            (RIGHT, 2): ring_copy(stage, k, RIGHT, 2, buf.at[lo, slot[2]], buf.at[lo, slot[0]]),
            (LEFT, 2): ring_copy(stage, k, LEFT, 2, buf.at[hi, slot[1]], buf.at[hi, slot[0]]),
        }

    copies = {}
    for k in range(CHUNKS):
        for stage in range(5):
            copies[stage, k] = reduce_copies(stage, k) if stage < 3 else gather_copies(stage, k)
    x1_copies = [mate_copy(6 + k, x1.at[k, :, own_half], x1.at[k, :, mate_half]) for k in range(CHUNKS)]
    x2_copies = [mate_copy(6 + CHUNKS + k, x2own.at[k], x2rcv.at[k]) for k in range(CHUNKS)]
    z_copies = [mate_copy(6 + 2 * CHUNKS + k, near.at[1, k, 1], near.at[0, k, 1]) for k in range(CHUNKS)]
    bc_copy = mate_copy(6 + 3 * CHUNKS, bc_send, bc_recv)

    def by_rows(count, fn):
        def step(i, carry):
            fn(i)
            return carry
        lax.fori_loop(0, count // blk, step, 0)

    def rows_at(i, first=0):
        return pl.ds(pl.multiple_of(first + i * blk, blk), blk)

    def start(stage, k):
        cp = copies[stage, k]
        if stage in (1, 2):
            for c_ in copies[stage - 1, k].values():
                c_.wait_send()

            def push(t, carry):
                at = pl.ds(pl.multiple_of(t * tile, 128), tile)
                if stage == 1:
                    part[k, :, at] = rows_cols(x1[k], a_blk[:, at])
                else:
                    both = rows_cols(a_oth[pl.ds(0, 2 * m), pl.ds(0, 2 * slab)], a_blk[:, at])
                    part[k, :, at] = both[:m] + both[m:]
                return carry

            lax.fori_loop(0, 3, push, 0)
            cp[RIGHT, 0].start()
            cp[LEFT, 0].start()
            cp[RIGHT, 1].start()
            lax.fori_loop(3, 6, push, 0)
            cp[LEFT, 1].start()
        else:
            for msg in (0, 1):
                cp[RIGHT, msg].start()
                cp[LEFT, msg].start()

    def middle(stage, k):
        cp = copies[stage, k]
        for way in (RIGHT, LEFT):
            cp[way, 0].wait_recv()
            first = 0 if way == RIGHT else h
            dest = slot[1] if way == RIGHT else slot[2]
            if stage == 0:
                def select(i):
                    r = pl.ds(pl.multiple_of(k * m + first + i * blk, blk), blk)
                    here_chip = (src[r, :] >= chip_base) & (src[r, :] < chip_base + 2 * slab)
                    m_mrg[r, dest] = jnp.where(here_chip, m_mrg[r, dest].astype(f32),
                                               far0[k, way, rows_at(i), :].astype(f32)).astype(bf16)
                by_rows(h, select)
            elif stage < 3:
                def add(i):
                    r = rows_at(i, first)
                    part[k, r, dest] = part[k, r, dest] + far[stage - 1, k, way, rows_at(i), :]
                by_rows(h, add)
            cp[way, 2].start()

    def pull(k, buf, use):
        def split(i):
            r = rows_at(i)
            full = buf[k, r, :]
            top = full.astype(bf16)
            rest = full - top.astype(f32)
            mid = rest.astype(bf16)
            a_oth[r, :] = top
            a_oth[rows_at(i, m), :] = mid
            a_oth[rows_at(i, 2 * m), :] = (rest - mid.astype(f32)).astype(bf16)
        by_rows(m, split)
        for t in (2, 1, 0):
            three = rows_rows(a_oth[pl.ds(0, 3 * m), :], a_blk[pl.ds(t * tile, tile), :])
            use(t, three[:m] + three[m:2 * m] + three[2 * m:])

    def finish(stage, k):
        cp = copies[stage, k]
        for way in (RIGHT, LEFT):
            cp[way, 1].wait_recv()
            cp[way, 2].wait_recv()
        if stage == 0:
            def first_level(i):
                r = rows_at(i)
                rk = rows_at(i, k * m)
                x1[k, r, own_half] = (m_mrg[rk, slot[3]].astype(f32) + near0[k, RIGHT, r, :].astype(f32)
                                      + near0[k, LEFT, r, :].astype(f32)).astype(bf16)
            by_rows(m, first_level)
            x1_copies[k].start()
            for i in range(4):
                if k == 0:
                    a_copies[i].wait_recv()
            x1_copies[k].wait_recv()
        elif stage == 1:
            def second_level(i):
                r = rows_at(i)
                rk = rows_at(i, k * m)
                total = part[k, r, slot[3]] + near[0, k, RIGHT, r, :] + near[0, k, LEFT, r, :]
                seen = jnp.maximum(onehot[rk, :].astype(f32), x1[k, r, own_half].astype(f32))
                x2own[k, r, :] = total * (1.0 - seen)
            by_rows(m, second_level)
            x2_copies[k].start()
            if k == 0:
                for copy in a_copies:
                    copy.wait_send()

            def split(i, source, half):
                r = rows_at(i)
                full = source[k, r, :]
                top = full.astype(bf16)
                a_oth[r, half] = top
                a_oth[rows_at(i, m), half] = (full - top.astype(f32)).astype(bf16)
            by_rows(m, lambda i: split(i, x2own, own_half))
            x2_copies[k].wait_recv()
            by_rows(m, lambda i: split(i, x2rcv, mate_half))
        elif stage == 2:
            def third_level(i):
                r = rows_at(i)
                rk = rows_at(i, k * m)
                total = part[k, r, slot[3]] + near[1, k, RIGHT, r, :] + near[1, k, LEFT, r, :]
                seen = jnp.maximum(onehot[rk, :].astype(f32), x1[k, r, own_half].astype(f32))
                seen = jnp.maximum(seen, jnp.where(x2own[k, r, :] > 0, 1.0, 0.0))
                paths = total * (1.0 - seen)
                reached = paths > 0
                wg[k, r, slot[3]] = jnp.where(reached, lw[1] / jnp.where(reached, paths, 1.0), 0.0)
            by_rows(m, third_level)
            for c_ in cp.values():
                c_.wait_send()
        elif stage == 3:
            mine, theirs = near.at[1, k, 0], near.at[1, k, 1]

            def keep(t, z):
                first = t * tile
                if first >= slab:
                    theirs[:, pl.ds(first - slab, tile)] = z
                elif first + tile > slab:
                    cut = slab - first
                    mine[:, pl.ds(first, cut)] = z[:, :cut]
                    theirs[:, pl.ds(0, tile - cut)] = z[:, cut:]
                    z_copies[k].start()
                else:
                    mine[:, pl.ds(first, tile)] = z
            pull(k, wg, keep)
            z_copies[k].wait_recv()

            def second_weights(i):
                r = rows_at(i)
                paths = x2own[k, r, :]
                delta = paths * (mine[r, :] + near[0, k, 1, r, :])
                reached = paths > 0
                part[k, r, slot[3]] = jnp.where(reached, (lw[0] + delta) / jnp.where(reached, paths, 1.0), 0.0)
                bc[:, own_half] = bc[:, own_half] + jnp.sum(delta, axis=0, keepdims=True)
            by_rows(m, second_weights)
        else:
            def close(t, z):
                at = pl.ds(t * tile, tile)
                bc[:, at] = bc[:, at] + jnp.sum(x1[k, :, at].astype(f32) * z, axis=0, keepdims=True)
            pull(k, part, close)

    for k in range(CHUNKS):
        start(0, k)
    for k in range(CHUNKS):
        middle(0, k)
    for stage in range(1, 5):
        for k in range(CHUNKS):
            finish(stage - 1, k)
            start(stage, k)
            middle(stage, k)
    for k in range(CHUNKS):
        finish(4, k)

    bc_send[...] = bc[:, mate_half]
    bc_copy.start()
    bc_copy.wait_recv()
    plane[pl.ds(s_me, 1)] = ((bc[:, own_half] + bc_recv[...]) * scale)[None]
    plane_copies = []
    for o in range(1, planes):
        copy = pltpu.make_async_remote_copy(src_ref=plane.at[s_me], dst_ref=plane.at[s_me], send_sem=plane_s.at[o],
                                            recv_sem=plane_r.at[o],
                                            device_id={"src": lax.rem(s_me + o, planes)}, device_id_type=MESH)
        copy.start()
        plane_copies.append(copy)
    for o in range(1, planes):
        arrived = plane.at[lax.rem(s_me + planes - o, planes)]
        pltpu.make_async_remote_copy(src_ref=arrived, dst_ref=arrived, send_sem=plane_s.at[o], recv_sem=plane_r.at[o],
                                     device_id={"src": lax.rem(s_me + o, planes)}, device_id_type=MESH).wait_recv()
    out[...] = jnp.sum(plane[...], axis=0)

    for copy in plane_copies + m_copies + x1_copies + x2_copies + z_copies + [bc_copy]:
        copy.wait_send()
    for k in range(CHUNKS):
        for stage in (3, 4):
            for c_ in copies[stage, k].values():
                c_.wait_send()


def solution(mesh):
    planes = mesh.shape["src"]
    ring = mesh.shape["graph"] // 2

    def device_program(adj_slab, src_local, level_weight):
        slab, vertex_count = adj_slab.shape
        src_count = src_local.shape[0]
        m = src_count // CHUNKS
        scale = vertex_count / (src_count * planes * (level_weight.shape[0] + 1) ** 3)
        wide = 4 * slab
        vmem = pltpu.VMEM
        sem = pltpu.SemaphoreType.DMA
        mates = 7 + 3 * CHUNKS
        rings = 5 * CHUNKS * 6
        flops = 2 * 9 * src_count * slab * vertex_count
        bc = pl.pallas_call(
            functools.partial(kernel, ring, planes, scale),
            out_shape=jax.ShapeDtypeStruct((1, slab), f32),
            in_specs=[pl.BlockSpec(memory_space=pl.ANY), pl.BlockSpec(memory_space=vmem), pl.BlockSpec(memory_space=pltpu.SMEM)],
            out_specs=pl.BlockSpec(memory_space=vmem),
            scratch_shapes=[
                vmem((2 * slab, wide), bf16), vmem((slab, wide), bf16),
                vmem((src_count, wide), bf16), vmem((src_count, wide), bf16), vmem((src_count, slab), bf16),
                vmem((CHUNKS, m, 2 * slab), bf16), vmem((CHUNKS, m, slab), f32), vmem((CHUNKS, m, slab), f32),
                vmem((CHUNKS, m, wide), f32), vmem((CHUNKS, m, wide), f32),
                vmem((CHUNKS, 2, m, slab), bf16), vmem((CHUNKS, 2, m // 2, slab), bf16),
                vmem((2, CHUNKS, 2, m, slab), f32), vmem((2, CHUNKS, 2, m // 2, slab), f32),
                vmem((1, 2 * slab), f32), vmem((1, slab), f32), vmem((1, slab), f32), vmem((planes, 1, slab), f32),
                sem((8,)), sem((rings,)), sem((rings,)), sem((mates,)), sem((mates,)), sem((planes,)), sem((planes,)),
            ],
            compiler_params=pltpu.CompilerParams(collective_id=0, has_side_effects=True, vmem_limit_bytes=67043328),
            cost_estimate=pl.CostEstimate(flops=flops, bytes_accessed=2 * slab * vertex_count, transcendentals=0),
        )(adj_slab, src_local.reshape(src_count, 1), level_weight)
        return bc.reshape(slab)

    return jax.shard_map(device_program, mesh=mesh,
                         in_specs=(P(("batch", "graph"), None), P(("batch", "src")), P(None)),
                         out_specs=P(("batch", "graph")), check_vma=False)
```

```python
import functools

import jax
import jax.numpy as jnp
from jax import lax
from jax.experimental import pallas as pl
from jax.experimental.pallas import tpu as pltpu
from jax.sharding import PartitionSpec as P

MESH = pl.DeviceIdType.MESH
f32, bf16 = jnp.float32, jnp.bfloat16
CHUNKS = 2
TO_P, TO_Q = 0, 1


def rows_cols(lhs, rhs):
    return lax.dot_general(lhs, rhs, (((1,), (0,)), ((), ())), preferred_element_type=f32)


def rows_rows(lhs, rhs):
    return lax.dot_general(lhs, rhs, (((1,), (1,)), ((), ())), preferred_element_type=f32)


def kernel(ring, planes, scale, adj, src, lw, out,
           a_blk, a_oth, pick, ids, onehot, x1, x2own, x2rcv, part, wg,
           near0, far0, near, far, bc, bc_send, bc_recv, plane,
           load_sem, ssem, rsem, d2d_s, d2d_r, plane_s, plane_r):
    slab = a_oth.shape[0]
    cols_all = a_oth.shape[1]
    src_count = ids.shape[0]
    m = src_count // CHUNKS
    h = m // 2
    tile = 2 * slab // 3
    blk = min(32, h)

    g = lax.axis_index("graph")
    s_me = lax.axis_index("src")
    x, c = g // 2, g % 2
    odd = lax.rem(x, 2)
    chip_p = x + 1 - 2 * odd
    chip_q = lax.rem(x + ring - 1 + 2 * odd, ring)
    chip_far = lax.rem(x + 2, ring)
    to_p = {"graph": chip_p * 2 + c}
    to_q = {"graph": chip_q * 2 + c}
    to_mate = {"graph": x * 2 + (1 - c)}
    chips = (chip_far, chip_p, chip_q, x)
    slot = [pl.ds(i * slab, slab) for i in range(4)]
    FAR, NEAR_P, NEAR_Q, OWN = slot

    loads = {}
    for i, chip in enumerate(chips):
        for own in (0, 1):
            at = pl.ds(pl.multiple_of((chip * 2 + (c if own else 1 - c)) * slab, 128), slab)
            target = a_blk.at[pl.ds(0, slab), slot[i]] if own else a_oth.at[:, slot[i]]
            loads[own, i] = pltpu.make_async_copy(adj.at[:, at], target, load_sem.at[4 * own + i])
    for pair in ((0, 1), (2, 3)):
        for own in (0, 1):
            for i in pair:
                loads[own, i].start()

    barrier = pltpu.get_barrier_semaphore()
    for dev in (to_p, to_q, to_mate):
        pl.semaphore_signal(barrier, inc=1, device_id=dev, device_id_type=MESH)
    for o in range(1, planes):
        pl.semaphore_signal(barrier, inc=1, device_id={"src": lax.rem(s_me + o, planes)}, device_id_type=MESH)

    row = lax.broadcasted_iota(jnp.int32, (src_count, src_count), 0)
    col = lax.broadcasted_iota(jnp.int32, (src_count, src_count), 1)
    ids[...] = jnp.sum(jnp.where(row == col, src[...].astype(f32), 0.0), axis=1, keepdims=True)
    base = g * slab
    base_f = base.astype(f32)
    chip_f = (x * 2 * slab).astype(f32)
    lane = (lax.broadcasted_iota(jnp.int32, (blk, slab), 1) + base).astype(f32)

    def one_hot_rows(i, carry):
        r = pl.ds(pl.multiple_of(i * blk, blk), blk)
        onehot[r, :] = jnp.where(ids[r, :] == lane, 1.0, 0.0).astype(bf16)
        return carry

    lax.fori_loop(0, src_count // blk, one_hot_rows, 0)
    bc[...] = jnp.zeros_like(bc)

    def mate_copy(i, source, target):
        return pltpu.make_async_remote_copy(src_ref=source, dst_ref=target, send_sem=d2d_s.at[i], recv_sem=d2d_r.at[i],
                                            device_id=to_mate, device_id_type=MESH)

    def ring_copy(stage, k, way, msg, source, target):
        i = ((stage * CHUNKS + k) * 2 + way) * 3 + msg
        return pltpu.make_async_remote_copy(src_ref=source, dst_ref=target, send_sem=ssem.at[i], recv_sem=rsem.at[i],
                                            device_id=to_p if way == TO_P else to_q, device_id_type=MESH)

    lo, hi = pl.ds(0, h), pl.ds(h, h)
    side = [pl.ds(0, slab), pl.ds(slab, slab)]
    own_half, mate_half = side
    merged = [pick.at[pl.ds(src_count + k * m, m), :] for k in range(CHUNKS)]
    two = [pl.ds(0, 2 * slab), pl.ds(2 * slab, 2 * slab)]

    def reduce_copies(stage, k):
        if stage == 0:
            send, nr, fr = merged[k], near0.at[k], far0.at[k]
        else:
            send, nr, fr = part.at[k], near.at[stage - 1, k], far.at[stage - 1, k]
        return {
            (TO_P, 0): ring_copy(stage, k, TO_P, 0, send.at[lo, FAR], fr.at[TO_P]),
            (TO_Q, 0): ring_copy(stage, k, TO_Q, 0, send.at[hi, FAR], fr.at[TO_Q]),
            (TO_P, 1): ring_copy(stage, k, TO_P, 1, send.at[lo, NEAR_P], nr.at[lo, side[TO_P]]),
            (TO_Q, 1): ring_copy(stage, k, TO_Q, 1, send.at[hi, NEAR_Q], nr.at[hi, side[TO_Q]]),
            (TO_P, 2): ring_copy(stage, k, TO_P, 2, send.at[hi, NEAR_P], nr.at[hi, side[TO_P]]),
            (TO_Q, 2): ring_copy(stage, k, TO_Q, 2, send.at[lo, NEAR_Q], nr.at[lo, side[TO_Q]]),
        }

    def gather_copies(stage, k):
        buf = wg.at[k] if stage == 3 else part.at[k]
        return {
            (TO_P, 0): ring_copy(stage, k, TO_P, 0, buf.at[lo, OWN], buf.at[lo, NEAR_P]),
            (TO_Q, 0): ring_copy(stage, k, TO_Q, 0, buf.at[hi, OWN], buf.at[hi, NEAR_Q]),
            (TO_P, 1): ring_copy(stage, k, TO_P, 1, buf.at[hi, OWN], buf.at[hi, NEAR_P]),
            (TO_Q, 1): ring_copy(stage, k, TO_Q, 1, buf.at[lo, OWN], buf.at[lo, NEAR_Q]),
            (TO_P, 2): ring_copy(stage, k, TO_P, 2, buf.at[hi, NEAR_Q], buf.at[hi, FAR]),
            (TO_Q, 2): ring_copy(stage, k, TO_Q, 2, buf.at[lo, NEAR_P], buf.at[lo, FAR]),
        }

    copies = {}
    for k in range(CHUNKS):
        for stage in range(5):
            copies[stage, k] = reduce_copies(stage, k) if stage < 3 else gather_copies(stage, k)
    a_copies = [mate_copy(i, a_oth.at[:, slot[i]], a_blk.at[pl.ds(slab, slab), slot[i]]) for i in range(4)]
    m_copies = {(k, i): mate_copy(4 + 2 * k + i, pick.at[pl.ds(k * m, m), two[i]], merged[k].at[:, two[i]])
                for k in range(CHUNKS) for i in range(2)}
    first = 4 + 2 * CHUNKS
    x1_copies = [mate_copy(first + k, x1.at[k, :, own_half], x1.at[k, :, mate_half]) for k in range(CHUNKS)]
    x2_copies = [mate_copy(first + CHUNKS + k, x2own.at[k], x2rcv.at[k]) for k in range(CHUNKS)]
    z_copies = [mate_copy(first + 2 * CHUNKS + k, near.at[1, k, :, mate_half], near.at[0, k, :, mate_half]) for k in range(CHUNKS)]
    bc_copy = mate_copy(first + 3 * CHUNKS, bc_send, bc_recv)

    def by_rows(count, fn):
        def step(i, carry):
            fn(i)
            return carry
        lax.fori_loop(0, count // blk, step, 0)

    def rows_at(i, start=0):
        return pl.ds(pl.multiple_of(start + i * blk, blk), blk)

    def by_tiles(begin, end, fn):
        def step(t, carry):
            fn(pl.ds(pl.multiple_of(t * tile, 128), tile))
            return carry
        lax.fori_loop(begin, end, step, 0)

    def select_other(k, i):
        def one(at):
            pick[pl.ds(k * m, m), at] = rows_cols(onehot[pl.ds(k * m, m), :], a_oth[:, at]).astype(bf16)
        by_tiles(3 * i, 3 * i + 3, one)
        m_copies[k, i].start()

    def select_own(k, i):
        rk = pl.ds(k * m, m)
        here = (ids[rk, :] >= base_f) & (ids[rk, :] < base_f + slab)

        def one(at):
            mine = rows_cols(onehot[rk, :], a_blk[pl.ds(0, slab), at])
            merged[k][:, at] = jnp.where(here, mine, merged[k][:, at].astype(f32)).astype(bf16)
        m_copies[k, i].wait_recv()
        by_tiles(3 * i, 3 * i + 3, one)

    def send_first(stage, k):
        cp = copies[stage, k]
        cp[TO_P, 0].start()
        cp[TO_Q, 0].start()
        cp[TO_P, 1].start()

    def start(stage, k):
        cp = copies[stage, k]
        if stage in (1, 2):
            for c_ in copies[stage - 1, k].values():
                c_.wait_send()

            def push(at):
                if stage == 1:
                    part[k, :, at] = rows_cols(x1[k], a_blk[:, at])
                else:
                    both = rows_cols(pick[pl.ds(0, 2 * m), two[0]], a_blk[:, at])
                    part[k, :, at] = both[:m] + both[m:]

            by_tiles(0, 3, push)
            send_first(stage, k)
            by_tiles(3, 6, push)
            cp[TO_Q, 1].start()
        else:
            for msg in (0, 1):
                cp[TO_P, msg].start()
                cp[TO_Q, msg].start()

    def middle(stage, k):
        cp = copies[stage, k]
        for way in (TO_P, TO_Q):
            cp[way, 0].wait_recv()
            begin = 0 if way == TO_P else h
            dest = NEAR_Q if way == TO_P else NEAR_P
            if stage == 0:
                def select(i):
                    r = rows_at(i, begin)
                    rk = rows_at(i, k * m + begin)
                    here = (ids[rk, :] >= chip_f) & (ids[rk, :] < chip_f + 2 * slab)
                    merged[k][r, dest] = jnp.where(here, merged[k][r, dest].astype(f32),
                                                   far0[k, way, rows_at(i), :].astype(f32)).astype(bf16)
                by_rows(h, select)
            elif stage < 3:
                def add(i):
                    r = rows_at(i, begin)
                    part[k, r, dest] = part[k, r, dest] + far[stage - 1, k, way, rows_at(i), :]
                by_rows(h, add)
            cp[1 - way, 2].start()

    def pull(buf, k, at, use):
        def split(i):
            r = rows_at(i)
            full = buf[k, r, at]
            top = full.astype(bf16)
            rest = full - top.astype(f32)
            mid = rest.astype(bf16)
            pick[r, at] = top
            pick[rows_at(i, m), at] = mid
            pick[rows_at(i, 2 * m), at] = (rest - mid.astype(f32)).astype(bf16)
        by_rows(m, split)
        for t in (2, 1, 0):
            three = rows_rows(pick[pl.ds(0, 3 * m), at], a_blk[pl.ds(t * tile, tile), at])
            use(t, three[:m] + three[m:2 * m] + three[2 * m:])

    def close(k, t, z):
        at = pl.ds(t * tile, tile)
        bc[:, at] = bc[:, at] + jnp.sum(x1[k, :, at].astype(f32) * z, axis=0, keepdims=True)

    def nears(stage, k):
        cp = copies[stage, k]
        cp[TO_P, 1].wait_recv()
        cp[TO_Q, 1].wait_recv()

        def keep(t, z):
            if stage == 3:
                near[1, k, :, pl.ds(t * tile, tile)] = z
            else:
                close(k, t, z)
        pull(wg if stage == 3 else part, k, pl.ds(slab, 3 * slab), keep)

    def finish(stage, k):
        cp = copies[stage, k]
        for way in (TO_P, TO_Q):
            if stage < 3:
                cp[way, 1].wait_recv()
            cp[way, 2].wait_recv()
        if stage == 0:
            def first_level(i):
                r = rows_at(i)
                x1[k, r, own_half] = (merged[k][r, OWN].astype(f32) + near0[k, r, side[0]].astype(f32)
                                      + near0[k, r, side[1]].astype(f32)).astype(bf16)
            by_rows(m, first_level)
            x1_copies[k].start()
            if k == 0:
                for copy in a_copies:
                    copy.wait_recv()
                for copy in m_copies.values():
                    copy.wait_send()
            x1_copies[k].wait_recv()
        elif stage == 1:
            def second_level(i):
                r = rows_at(i)
                rk = rows_at(i, k * m)
                total = part[k, r, OWN] + near[0, k, r, side[0]] + near[0, k, r, side[1]]
                seen = jnp.maximum(onehot[rk, :].astype(f32), x1[k, r, own_half].astype(f32))
                x2own[k, r, :] = total * (1.0 - seen)
            by_rows(m, second_level)
            x2_copies[k].start()

            def split(i, source, half):
                r = rows_at(i)
                full = source[k, r, :]
                top = full.astype(bf16)
                pick[r, half] = top
                pick[rows_at(i, m), half] = (full - top.astype(f32)).astype(bf16)
            by_rows(m, lambda i: split(i, x2own, own_half))
            x2_copies[k].wait_recv()
            by_rows(m, lambda i: split(i, x2rcv, mate_half))
        elif stage == 2:
            def third_level(i):
                r = rows_at(i)
                rk = rows_at(i, k * m)
                total = part[k, r, OWN] + near[1, k, r, side[0]] + near[1, k, r, side[1]]
                seen = jnp.maximum(onehot[rk, :].astype(f32), x1[k, r, own_half].astype(f32))
                seen = jnp.maximum(seen, jnp.where(x2own[k, r, :] > 0, 1.0, 0.0))
                paths = total * (1.0 - seen)
                reached = paths > 0
                wg[k, r, OWN] = jnp.where(reached, lw[1] / jnp.where(reached, paths, 1.0), 0.0)
            by_rows(m, third_level)
            for c_ in cp.values():
                c_.wait_send()
        elif stage == 3:
            def keep(t, z):
                at = pl.ds(t * tile, tile)
                near[1, k, :, at] = near[1, k, :, at] + z
                if t == 1:
                    z_copies[k].start()
            pull(wg, k, FAR, keep)
            z_copies[k].wait_recv()

            def second_weights(i):
                r = rows_at(i)
                paths = x2own[k, r, :]
                delta = paths * (near[1, k, r, own_half] + near[0, k, r, mate_half])
                reached = paths > 0
                part[k, r, OWN] = jnp.where(reached, (lw[0] + delta) / jnp.where(reached, paths, 1.0), 0.0)
                bc[:, own_half] = bc[:, own_half] + jnp.sum(delta, axis=0, keepdims=True)
            by_rows(m, second_weights)
        else:
            pull(part, k, FAR, functools.partial(close, k))

    loads[0, 0].wait()
    loads[0, 1].wait()
    pl.semaphore_wait(barrier, 3 + planes - 1)
    for k in range(CHUNKS):
        select_other(k, 0)
    loads[1, 0].wait()
    loads[1, 1].wait()
    for k in range(CHUNKS):
        select_own(k, 0)
        send_first(0, k)
    loads[0, 2].wait()
    loads[0, 3].wait()
    for k in range(CHUNKS):
        select_other(k, 1)
    for copy in a_copies:
        copy.start()
    loads[1, 2].wait()
    loads[1, 3].wait()
    for k in range(CHUNKS):
        select_own(k, 1)
        copies[0, k][TO_Q, 1].start()
    for k in range(CHUNKS):
        middle(0, k)
    for stage in range(1, 5):
        finish(stage - 1, 0)
        start(stage, 0)
        if stage == 4:
            nears(3, 1)
        middle(stage, 0)
        finish(stage - 1, 1)
        start(stage, 1)
        if stage >= 3:
            nears(stage, 0)
        middle(stage, 1)
    finish(4, 0)
    nears(4, 1)
    finish(4, 1)

    bc_send[...] = bc[:, mate_half]
    bc_copy.start()
    bc_copy.wait_recv()
    plane[pl.ds(s_me, 1)] = ((bc[:, own_half] + bc_recv[...]) * scale)[None]
    plane_copies = []
    for o in range(1, planes):
        copy = pltpu.make_async_remote_copy(src_ref=plane.at[s_me], dst_ref=plane.at[s_me], send_sem=plane_s.at[o],
                                            recv_sem=plane_r.at[o],
                                            device_id={"src": lax.rem(s_me + o, planes)}, device_id_type=MESH)
        copy.start()
        plane_copies.append(copy)
    for o in range(1, planes):
        arrived = plane.at[lax.rem(s_me + planes - o, planes)]
        pltpu.make_async_remote_copy(src_ref=arrived, dst_ref=arrived, send_sem=plane_s.at[o], recv_sem=plane_r.at[o],
                                     device_id={"src": lax.rem(s_me + o, planes)}, device_id_type=MESH).wait_recv()
    out[...] = jnp.sum(plane[...], axis=0)

    for copy in plane_copies + a_copies + x1_copies + x2_copies + z_copies + [bc_copy]:
        copy.wait_send()
    for k in range(CHUNKS):
        for stage in (3, 4):
            for c_ in copies[stage, k].values():
                c_.wait_send()


def solution(mesh):
    planes = mesh.shape["src"]
    ring = mesh.shape["graph"] // 2

    def device_program(adj_slab, src_local, level_weight):
        slab, vertex_count = adj_slab.shape
        src_count = src_local.shape[0]
        m = src_count // CHUNKS
        scale = vertex_count / (src_count * planes * (level_weight.shape[0] + 1) ** 3)
        wide = 4 * slab
        vmem = pltpu.VMEM
        sem = pltpu.SemaphoreType.DMA
        mates = 5 + 5 * CHUNKS
        rings = 5 * CHUNKS * 6
        flops = 2 * 9 * src_count * slab * vertex_count
        bc = pl.pallas_call(
            functools.partial(kernel, ring, planes, scale),
            out_shape=jax.ShapeDtypeStruct((1, slab), f32),
            in_specs=[pl.BlockSpec(memory_space=pl.ANY), pl.BlockSpec(memory_space=vmem), pl.BlockSpec(memory_space=pltpu.SMEM)],
            out_specs=pl.BlockSpec(memory_space=vmem),
            scratch_shapes=[
                vmem((2 * slab, wide), bf16), vmem((slab, wide), bf16),
                vmem((2 * src_count, wide), bf16), vmem((src_count, 1), f32), vmem((src_count, slab), bf16),
                vmem((CHUNKS, m, 2 * slab), bf16), vmem((CHUNKS, m, slab), f32), vmem((CHUNKS, m, slab), f32),
                vmem((CHUNKS, m, wide), f32), vmem((CHUNKS, m, wide), f32),
                vmem((CHUNKS, m, 2 * slab), bf16), vmem((CHUNKS, 2, m // 2, slab), bf16),
                vmem((2, CHUNKS, m, 2 * slab), f32), vmem((2, CHUNKS, 2, m // 2, slab), f32),
                vmem((1, 2 * slab), f32), vmem((1, slab), f32), vmem((1, slab), f32), vmem((planes, 1, slab), f32),
                sem((8,)), sem((rings,)), sem((rings,)), sem((mates,)), sem((mates,)), sem((planes,)), sem((planes,)),
            ],
            compiler_params=pltpu.CompilerParams(collective_id=0, has_side_effects=True, vmem_limit_bytes=67043328),
            cost_estimate=pl.CostEstimate(flops=flops, bytes_accessed=2 * slab * vertex_count, transcendentals=0),
        )(adj_slab, src_local.reshape(1, src_count), level_weight)
        return bc.reshape(slab)

    return jax.shard_map(device_program, mesh=mesh,
                         in_specs=(P(("batch", "graph"), None), P(("batch", "src")), P(None)),
                         out_specs=P(("batch", "graph")), check_vma=False)
```

```python
import functools

import jax
import jax.numpy as jnp
from jax import lax
from jax.experimental import pallas as pl
from jax.experimental.pallas import tpu as pltpu
from jax.sharding import PartitionSpec as P

MESH = pl.DeviceIdType.MESH
f32, bf16 = jnp.float32, jnp.bfloat16
CHUNKS = 2
TO_P, TO_Q = 0, 1


def rows_cols(lhs, rhs):
    return lax.dot_general(lhs, rhs, (((1,), (0,)), ((), ())), preferred_element_type=f32)


def rows_rows(lhs, rhs):
    return lax.dot_general(lhs, rhs, (((1,), (1,)), ((), ())), preferred_element_type=f32)


def kernel(ring, planes, scale, adj, src, lw, out,
           a_blk, a_oth, pick, ids, onehot, x1, x2own, x2rcv, part, wg,
           near0, far0, near, far, bc, total, plane,
           load_sem, ssem, rsem, d2d_s, d2d_r, plane_s, plane_r):
    slab = a_oth.shape[0]
    cols_all = a_oth.shape[1]
    src_count = ids.shape[0]
    m = src_count // CHUNKS
    h = m // 2
    tile = 2 * slab // 3
    blk = min(32, h)

    g = lax.axis_index("graph")
    s_me = lax.axis_index("src")
    x, c = g // 2, g % 2
    odd = lax.rem(x, 2)
    chip_p = x + 1 - 2 * odd
    chip_q = lax.rem(x + ring - 1 + 2 * odd, ring)
    chip_far = lax.rem(x + 2, ring)
    to_p = {"graph": chip_p * 2 + c}
    to_q = {"graph": chip_q * 2 + c}
    to_mate = {"graph": x * 2 + (1 - c)}
    chips = (chip_far, chip_p, chip_q, x)
    slot = [pl.ds(i * slab, slab) for i in range(4)]
    FAR, NEAR_P, NEAR_Q, OWN = slot

    loads = {}
    for i, chip in enumerate(chips):
        for own in (0, 1):
            at = pl.ds(pl.multiple_of((chip * 2 + (c if own else 1 - c)) * slab, 128), slab)
            target = a_blk.at[pl.ds(0, slab), slot[i]] if own else a_oth.at[:, slot[i]]
            loads[own, i] = pltpu.make_async_copy(adj.at[:, at], target, load_sem.at[4 * own + i])
    for own, i in ((0, 0), (0, 1), (1, 0), (1, 1), (0, 2), (1, 2), (0, 3), (1, 3)):
        loads[own, i].start()

    barrier = pltpu.get_barrier_semaphore()
    for dev in (to_p, to_q, to_mate):
        pl.semaphore_signal(barrier, inc=1, device_id=dev, device_id_type=MESH)
    for o in range(1, planes):
        there = lax.rem(s_me + o, planes)
        pl.semaphore_signal(barrier, inc=1, device_id={"src": there}, device_id_type=MESH)
        pl.semaphore_signal(barrier, inc=1, device_id={"src": there, "graph": x * 2 + (1 - c)}, device_id_type=MESH)

    row = lax.broadcasted_iota(jnp.int32, (src_count, src_count), 0)
    col = lax.broadcasted_iota(jnp.int32, (src_count, src_count), 1)
    ids[...] = jnp.sum(jnp.where(row == col, src[...].astype(f32), 0.0), axis=1, keepdims=True)
    base = g * slab
    base_f = base.astype(f32)
    chip_f = (x * 2 * slab).astype(f32)
    lane = (lax.broadcasted_iota(jnp.int32, (blk, slab), 1) + base).astype(f32)

    def one_hot_rows(i, carry):
        r = pl.ds(pl.multiple_of(i * blk, blk), blk)
        onehot[r, :] = jnp.where(ids[r, :] == lane, 1.0, 0.0).astype(bf16)
        return carry

    lax.fori_loop(0, src_count // blk, one_hot_rows, 0)
    bc[...] = jnp.zeros_like(bc)

    def mate_copy(i, source, target):
        return pltpu.make_async_remote_copy(src_ref=source, dst_ref=target, send_sem=d2d_s.at[i], recv_sem=d2d_r.at[i],
                                            device_id=to_mate, device_id_type=MESH)

    def ring_copy(stage, k, way, msg, source, target):
        i = ((stage * CHUNKS + k) * 2 + way) * 3 + msg
        return pltpu.make_async_remote_copy(src_ref=source, dst_ref=target, send_sem=ssem.at[i], recv_sem=rsem.at[i],
                                            device_id=to_p if way == TO_P else to_q, device_id_type=MESH)

    lo, hi = pl.ds(0, h), pl.ds(h, h)
    side = [pl.ds(0, slab), pl.ds(slab, slab)]
    own_half, mate_half = side
    merged = [pick.at[pl.ds(src_count + k * m, m), :] for k in range(CHUNKS)]
    two = [pl.ds(0, 2 * slab), pl.ds(2 * slab, 2 * slab)]

    def reduce_copies(stage, k):
        if stage == 0:
            send, nr, fr = merged[k], near0.at[k], far0.at[k]
        else:
            send, nr, fr = part.at[k], near.at[stage - 1, k], far.at[stage - 1, k]
        return {
            (TO_P, 0): ring_copy(stage, k, TO_P, 0, send.at[lo, FAR], fr.at[TO_P]),
            (TO_Q, 0): ring_copy(stage, k, TO_Q, 0, send.at[hi, FAR], fr.at[TO_Q]),
            (TO_P, 1): ring_copy(stage, k, TO_P, 1, send.at[lo, NEAR_P], nr.at[lo, side[TO_P]]),
            (TO_Q, 1): ring_copy(stage, k, TO_Q, 1, send.at[hi, NEAR_Q], nr.at[hi, side[TO_Q]]),
            (TO_P, 2): ring_copy(stage, k, TO_P, 2, send.at[hi, NEAR_P], nr.at[hi, side[TO_P]]),
            (TO_Q, 2): ring_copy(stage, k, TO_Q, 2, send.at[lo, NEAR_Q], nr.at[lo, side[TO_Q]]),
        }

    def gather_copies(stage, k):
        buf = wg.at[k] if stage == 3 else part.at[k]
        return {
            (TO_P, 0): ring_copy(stage, k, TO_P, 0, buf.at[lo, OWN], buf.at[lo, NEAR_P]),
            (TO_Q, 0): ring_copy(stage, k, TO_Q, 0, buf.at[hi, OWN], buf.at[hi, NEAR_Q]),
            (TO_P, 1): ring_copy(stage, k, TO_P, 1, buf.at[hi, OWN], buf.at[hi, NEAR_P]),
            (TO_Q, 1): ring_copy(stage, k, TO_Q, 1, buf.at[lo, OWN], buf.at[lo, NEAR_Q]),
            (TO_P, 2): ring_copy(stage, k, TO_P, 2, buf.at[hi, NEAR_Q], buf.at[hi, FAR]),
            (TO_Q, 2): ring_copy(stage, k, TO_Q, 2, buf.at[lo, NEAR_P], buf.at[lo, FAR]),
        }

    copies = {}
    for k in range(CHUNKS):
        for stage in range(5):
            copies[stage, k] = reduce_copies(stage, k) if stage < 3 else gather_copies(stage, k)
    a_copies = [mate_copy(i, a_oth.at[:, slot[i]], a_blk.at[pl.ds(slab, slab), slot[i]]) for i in range(4)]
    m_copies = {(k, i): mate_copy(4 + 4 * k + i, pick.at[pl.ds(k * m, m), slot[i]], merged[k].at[:, slot[i]])
                for k in range(CHUNKS) for i in range(4)}
    first = 4 + 4 * CHUNKS
    x1_copies = [mate_copy(first + k, x1.at[k, :, own_half], x1.at[k, :, mate_half]) for k in range(CHUNKS)]
    x2_copies = [mate_copy(first + CHUNKS + k, x2own.at[k], x2rcv.at[k]) for k in range(CHUNKS)]
    z_copies = [mate_copy(first + 2 * CHUNKS + k, near.at[1, k, :, mate_half], near.at[0, k, :, mate_half]) for k in range(CHUNKS)]

    def by_rows(count, fn):
        def step(i, carry):
            fn(i)
            return carry
        lax.fori_loop(0, count // blk, step, 0)

    def rows_at(i, start=0):
        return pl.ds(pl.multiple_of(start + i * blk, blk), blk)

    def by_tiles(begin, end, fn):
        def step(t, carry):
            fn(pl.ds(pl.multiple_of(t * tile, 128), tile))
            return carry
        lax.fori_loop(begin, end, step, 0)

    def select_other(k, i):
        pick[pl.ds(k * m, m), slot[i]] = rows_cols(onehot[pl.ds(k * m, m), :], a_oth[:, slot[i]]).astype(bf16)

    def select_own(k, i):
        rk = pl.ds(k * m, m)
        here = (ids[rk, :] >= base_f) & (ids[rk, :] < base_f + slab)
        m_copies[k, i].wait_recv()
        mine = rows_cols(onehot[rk, :], a_blk[pl.ds(0, slab), slot[i]])
        merged[k][:, slot[i]] = jnp.where(here, mine, merged[k][:, slot[i]].astype(f32)).astype(bf16)

    def send_first(stage, k):
        cp = copies[stage, k]
        cp[TO_P, 0].start()
        cp[TO_Q, 0].start()
        cp[TO_P, 1].start()

    def start(stage, k):
        cp = copies[stage, k]
        if stage in (1, 2):
            for c_ in copies[stage - 1, k].values():
                c_.wait_send()

            def push(at):
                if stage == 1:
                    part[k, :, at] = rows_cols(x1[k], a_blk[:, at])
                else:
                    both = rows_cols(pick[pl.ds(0, 2 * m), two[0]], a_blk[:, at])
                    part[k, :, at] = both[:m] + both[m:]

            by_tiles(0, 3, push)
            send_first(stage, k)
            by_tiles(3, 6, push)
            cp[TO_Q, 1].start()
        else:
            for msg in (0, 1):
                cp[TO_P, msg].start()
                cp[TO_Q, msg].start()

    def middle(stage, k):
        cp = copies[stage, k]
        for way in (TO_P, TO_Q):
            cp[way, 0].wait_recv()
            begin = 0 if way == TO_P else h
            dest = NEAR_Q if way == TO_P else NEAR_P
            if stage == 0:
                def select(i):
                    r = rows_at(i, begin)
                    rk = rows_at(i, k * m + begin)
                    here = (ids[rk, :] >= chip_f) & (ids[rk, :] < chip_f + 2 * slab)
                    merged[k][r, dest] = jnp.where(here, merged[k][r, dest].astype(f32),
                                                   far0[k, way, rows_at(i), :].astype(f32)).astype(bf16)
                by_rows(h, select)
            elif stage < 3:
                def add(i):
                    r = rows_at(i, begin)
                    part[k, r, dest] = part[k, r, dest] + far[stage - 1, k, way, rows_at(i), :]
                by_rows(h, add)
            cp[1 - way, 2].start()

    def pull(buf, k, at, use, meanwhile=None):
        def split(i):
            r = rows_at(i)
            full = buf[k, r, at]
            top = full.astype(bf16)
            rest = full - top.astype(f32)
            mid = rest.astype(bf16)
            pick[r, at] = top
            pick[rows_at(i, m), at] = mid
            pick[rows_at(i, 2 * m), at] = (rest - mid.astype(f32)).astype(bf16)
        by_rows(m, split)

        def product(r):
            three = rows_rows(pick[pl.ds(0, 3 * m), at], a_blk[r, at])
            use(r, three[:m] + three[m:2 * m] + three[2 * m:])
        if meanwhile is None:
            by_tiles(0, 3, product)
        else:
            by_tiles(1, 3, product)
            meanwhile()
            by_tiles(0, 1, product)

    def close(k, at, z):
        bc[:, at] = bc[:, at] + jnp.sum(x1[k, :, at].astype(f32) * z, axis=0, keepdims=True)

    def nears(stage, k):
        cp = copies[stage, k]
        cp[TO_P, 1].wait_recv()
        cp[TO_Q, 1].wait_recv()

        def keep(r, z):
            if stage == 3:
                near[1, k, :, r] = z
            else:
                close(k, r, z)
        pull(wg if stage == 3 else part, k, pl.ds(slab, 3 * slab), keep)

    def finish(stage, k):
        cp = copies[stage, k]
        for way in (TO_P, TO_Q):
            if stage < 3:
                cp[way, 1].wait_recv()
            cp[way, 2].wait_recv()
        if stage == 0:
            def first_level(i):
                r = rows_at(i)
                x1[k, r, own_half] = (merged[k][r, OWN].astype(f32) + near0[k, r, side[0]].astype(f32)
                                      + near0[k, r, side[1]].astype(f32)).astype(bf16)
            by_rows(m, first_level)
            x1_copies[k].start()
            if k == 0:
                for copy in a_copies:
                    copy.wait_recv()
                for copy in m_copies.values():
                    copy.wait_send()
            x1_copies[k].wait_recv()
        elif stage == 1:
            def second_level(i):
                r = rows_at(i)
                rk = rows_at(i, k * m)
                total = part[k, r, OWN] + near[0, k, r, side[0]] + near[0, k, r, side[1]]
                seen = jnp.maximum(onehot[rk, :].astype(f32), x1[k, r, own_half].astype(f32))
                x2own[k, r, :] = total * (1.0 - seen)
            by_rows(m, second_level)
            x2_copies[k].start()

            def split(i, source, half):
                r = rows_at(i)
                full = source[k, r, :]
                top = full.astype(bf16)
                pick[r, half] = top
                pick[rows_at(i, m), half] = (full - top.astype(f32)).astype(bf16)
            by_rows(m, lambda i: split(i, x2own, own_half))
            x2_copies[k].wait_recv()
            by_rows(m, lambda i: split(i, x2rcv, mate_half))
        elif stage == 2:
            def third_level(i):
                r = rows_at(i)
                rk = rows_at(i, k * m)
                total = part[k, r, OWN] + near[1, k, r, side[0]] + near[1, k, r, side[1]]
                seen = jnp.maximum(onehot[rk, :].astype(f32), x1[k, r, own_half].astype(f32))
                seen = jnp.maximum(seen, jnp.where(x2own[k, r, :] > 0, 1.0, 0.0))
                paths = total * (1.0 - seen)
                reached = paths > 0
                wg[k, r, OWN] = jnp.where(reached, lw[1] / jnp.where(reached, paths, 1.0), 0.0)
            by_rows(m, third_level)
            for c_ in cp.values():
                c_.wait_send()
        elif stage == 3:
            def keep(r, z):
                near[1, k, :, r] = near[1, k, :, r] + z
            pull(wg, k, FAR, keep, z_copies[k].start)
            z_copies[k].wait_recv()

            def second_weights(i):
                r = rows_at(i)
                paths = x2own[k, r, :]
                delta = paths * (near[1, k, r, own_half] + near[0, k, r, mate_half])
                reached = paths > 0
                part[k, r, OWN] = jnp.where(reached, (lw[0] + delta) / jnp.where(reached, paths, 1.0), 0.0)
                bc[:, own_half] = bc[:, own_half] + jnp.sum(delta, axis=0, keepdims=True)
            by_rows(m, second_weights)
        else:
            pull(part, k, FAR, functools.partial(close, k))

    def other(k, i):
        if k == 0:
            loads[0, i].wait()
        select_other(k, i)
        if (k, i) == (0, 0):
            pl.semaphore_wait(barrier, 3 + 2 * (planes - 1))
        m_copies[k, i].start()

    def own(k, i):
        if k == 0:
            loads[1, i].wait()
        select_own(k, i)

    for k in range(CHUNKS):
        for i in range(3):
            other(k, i)
        own(k, 0)
        copies[0, k][TO_P, 0].start()
        copies[0, k][TO_Q, 0].start()
        own(k, 1)
        copies[0, k][TO_P, 1].start()
        own(k, 2)
        copies[0, k][TO_Q, 1].start()
    for k in range(CHUNKS):
        other(k, 3)
    for copy in a_copies:
        copy.start()
    middle(0, 0)
    for k in range(CHUNKS):
        own(k, 3)
    middle(0, 1)
    for stage in range(1, 5):
        finish(stage - 1, 0)
        start(stage, 0)
        if stage == 4:
            nears(3, 1)
        middle(stage, 0)
        finish(stage - 1, 1)
        start(stage, 1)
        if stage >= 3:
            nears(stage, 0)
        middle(stage, 1)
    finish(4, 0)
    nears(4, 1)
    finish(4, 1)

    total[...] = bc[...] * scale
    plane[0, pl.ds(s_me, 1)] = total[:, own_half][None]
    plane_copies = []
    for o in range(planes):
        there = lax.rem(s_me + o, planes)
        back = lax.rem(s_me + planes - o, planes)
        for other_core in (0, 1):
            if o == 0 and not other_core:
                continue
            device = {"src": there, "graph": x * 2 + (1 - c)} if other_core else {"src": there}

            def plane_copy(target):
                return pltpu.make_async_remote_copy(src_ref=total.at[:, side[other_core]], dst_ref=plane.at[other_core, target],
                                                    send_sem=plane_s.at[other_core * planes + o],
                                                    recv_sem=plane_r.at[other_core * planes + o],
                                                    device_id=device, device_id_type=MESH)
            plane_copy(s_me).start()
            plane_copies.append(plane_copy(back))
    for copy in plane_copies:
        copy.wait_recv()
    out[...] = jnp.sum(plane[0], axis=0) + jnp.sum(plane[1], axis=0)

    for copy in plane_copies + a_copies + x1_copies + x2_copies + z_copies:
        copy.wait_send()
    for k in range(CHUNKS):
        for stage in (3, 4):
            for c_ in copies[stage, k].values():
                c_.wait_send()


def solution(mesh):
    planes = mesh.shape["src"]
    ring = mesh.shape["graph"] // 2

    def device_program(adj_slab, src_local, level_weight):
        slab, vertex_count = adj_slab.shape
        src_count = src_local.shape[0]
        m = src_count // CHUNKS
        scale = vertex_count / (src_count * planes * (level_weight.shape[0] + 1) ** 3)
        wide = 4 * slab
        vmem = pltpu.VMEM
        sem = pltpu.SemaphoreType.DMA
        mates = 4 + 7 * CHUNKS
        rings = 5 * CHUNKS * 6
        flops = 2 * 9 * src_count * slab * vertex_count
        bc = pl.pallas_call(
            functools.partial(kernel, ring, planes, scale),
            out_shape=jax.ShapeDtypeStruct((1, slab), f32),
            in_specs=[pl.BlockSpec(memory_space=pl.ANY), pl.BlockSpec(memory_space=vmem), pl.BlockSpec(memory_space=pltpu.SMEM)],
            out_specs=pl.BlockSpec(memory_space=vmem),
            scratch_shapes=[
                vmem((2 * slab, wide), bf16), vmem((slab, wide), bf16),
                vmem((2 * src_count, wide), bf16), vmem((src_count, 1), f32), vmem((src_count, slab), bf16),
                vmem((CHUNKS, m, 2 * slab), bf16), vmem((CHUNKS, m, slab), f32), vmem((CHUNKS, m, slab), f32),
                vmem((CHUNKS, m, wide), f32), vmem((CHUNKS, m, wide), f32),
                vmem((CHUNKS, m, 2 * slab), bf16), vmem((CHUNKS, 2, m // 2, slab), bf16),
                vmem((2, CHUNKS, m, 2 * slab), f32), vmem((2, CHUNKS, 2, m // 2, slab), f32),
                vmem((1, 2 * slab), f32), vmem((1, 2 * slab), f32), vmem((2, planes, 1, slab), f32),
                sem((8,)), sem((rings,)), sem((rings,)), sem((mates,)), sem((mates,)), sem((2 * planes,)), sem((2 * planes,)),
            ],
            compiler_params=pltpu.CompilerParams(collective_id=0, has_side_effects=True, vmem_limit_bytes=67043328),
            cost_estimate=pl.CostEstimate(flops=flops, bytes_accessed=2 * slab * vertex_count, transcendentals=0),
        )(adj_slab, src_local.reshape(1, src_count), level_weight)
        return bc.reshape(slab)

    return jax.shard_map(device_program, mesh=mesh,
                         in_specs=(P(("batch", "graph"), None), P(("batch", "src")), P(None)),
                         out_specs=P(("batch", "graph")), check_vma=False)
```

```python
import functools

import jax
import jax.numpy as jnp
from jax import lax
from jax.experimental import pallas as pl
from jax.experimental.pallas import tpu as pltpu
from jax.sharding import PartitionSpec as P

MESH = pl.DeviceIdType.MESH
f32, bf16 = jnp.float32, jnp.bfloat16
CHUNKS = 2
TO_P, TO_Q = 0, 1


def scoped(name):
    def wrap(fn):
        def inner(*a, **kw):
            tag = name + "".join(f"_{v}" for v in a if isinstance(v, int))
            with jax.named_scope(tag):
                return fn(*a, **kw)
        return inner
    return wrap


def rows_cols(lhs, rhs):
    return lax.dot_general(lhs, rhs, (((1,), (0,)), ((), ())), preferred_element_type=f32)


def rows_rows(lhs, rhs):
    return lax.dot_general(lhs, rhs, (((1,), (1,)), ((), ())), preferred_element_type=f32)


def kernel(ring, planes, scale, adj, src, lw, out,
           a_blk, a_oth, pick, ids, onehot, x1, x2own, x2rcv, part, wg,
           near0, far0, near, far, bc, total, plane,
           load_sem, ssem, rsem, d2d_s, d2d_r, plane_s, plane_r):
    slab = a_oth.shape[0]
    cols_all = a_oth.shape[1]
    src_count = ids.shape[0]
    m = src_count // CHUNKS
    h = m // 2
    tile = 2 * slab // 3
    blk = min(32, h)

    g = lax.axis_index("graph")
    s_me = lax.axis_index("src")
    x, c = g // 2, g % 2
    odd = lax.rem(x, 2)
    chip_p = x + 1 - 2 * odd
    chip_q = lax.rem(x + ring - 1 + 2 * odd, ring)
    chip_far = lax.rem(x + 2, ring)
    to_p = {"graph": chip_p * 2 + c}
    to_q = {"graph": chip_q * 2 + c}
    to_mate = {"graph": x * 2 + (1 - c)}
    chips = (chip_far, chip_p, chip_q, x)
    slot = [pl.ds(i * slab, slab) for i in range(4)]
    FAR, NEAR_P, NEAR_Q, OWN = slot

    loads = {}
    for i, chip in enumerate(chips):
        for own in (0, 1):
            at = pl.ds(pl.multiple_of((chip * 2 + (c if own else 1 - c)) * slab, 128), slab)
            target = a_blk.at[pl.ds(0, slab), slot[i]] if own else a_oth.at[:, slot[i]]
            loads[own, i] = pltpu.make_async_copy(adj.at[:, at], target, load_sem.at[4 * own + i])
    for own, i in ((0, 0), (0, 1), (0, 2), (1, 0), (1, 1), (1, 2), (0, 3), (1, 3)):
        loads[own, i].start()

    barrier = pltpu.get_barrier_semaphore()
    for dev in (to_p, to_q, to_mate):
        pl.semaphore_signal(barrier, inc=1, device_id=dev, device_id_type=MESH)
    for o in range(1, planes):
        there = lax.rem(s_me + o, planes)
        pl.semaphore_signal(barrier, inc=1, device_id={"src": there}, device_id_type=MESH)
        pl.semaphore_signal(barrier, inc=1, device_id={"src": there, "graph": x * 2 + (1 - c)}, device_id_type=MESH)

    row = lax.broadcasted_iota(jnp.int32, (src_count, src_count), 0)
    col = lax.broadcasted_iota(jnp.int32, (src_count, src_count), 1)
    ids[...] = jnp.sum(jnp.where(row == col, src[...].astype(f32), 0.0), axis=1, keepdims=True)
    base = g * slab
    base_f = base.astype(f32)
    chip_f = (x * 2 * slab).astype(f32)
    lane = (lax.broadcasted_iota(jnp.int32, (blk, slab), 1) + base).astype(f32)

    def one_hot_rows(i, carry):
        r = pl.ds(pl.multiple_of(i * blk, blk), blk)
        onehot[r, :] = jnp.where(ids[r, :] == lane, 1.0, 0.0).astype(bf16)
        return carry

    lax.fori_loop(0, m // blk, one_hot_rows, 0)

    def mate_copy(i, source, target):
        return pltpu.make_async_remote_copy(src_ref=source, dst_ref=target, send_sem=d2d_s.at[i], recv_sem=d2d_r.at[i],
                                            device_id=to_mate, device_id_type=MESH)

    def ring_copy(stage, k, way, msg, source, target):
        i = ((stage * CHUNKS + k) * 2 + way) * 3 + msg
        return pltpu.make_async_remote_copy(src_ref=source, dst_ref=target, send_sem=ssem.at[i], recv_sem=rsem.at[i],
                                            device_id=to_p if way == TO_P else to_q, device_id_type=MESH)

    lo, hi = pl.ds(0, h), pl.ds(h, h)
    side = [pl.ds(0, slab), pl.ds(slab, slab)]
    own_half, mate_half = side
    merged = [pick.at[pl.ds(src_count + k * m, m), :] for k in range(CHUNKS)]
    two = [pl.ds(0, 2 * slab), pl.ds(2 * slab, 2 * slab)]

    def reduce_copies(stage, k):
        if stage == 0:
            send, nr, fr = merged[k], near0.at[k], far0.at[k]
        else:
            send, nr, fr = part.at[k], near.at[stage - 1, k], far.at[stage - 1, k]
        return {
            (TO_P, 0): ring_copy(stage, k, TO_P, 0, send.at[lo, FAR], fr.at[TO_P]),
            (TO_Q, 0): ring_copy(stage, k, TO_Q, 0, send.at[hi, FAR], fr.at[TO_Q]),
            (TO_P, 1): ring_copy(stage, k, TO_P, 1, send.at[lo, NEAR_P], nr.at[lo, side[TO_P]]),
            (TO_Q, 1): ring_copy(stage, k, TO_Q, 1, send.at[hi, NEAR_Q], nr.at[hi, side[TO_Q]]),
            (TO_P, 2): ring_copy(stage, k, TO_P, 2, send.at[hi, NEAR_P], nr.at[hi, side[TO_P]]),
            (TO_Q, 2): ring_copy(stage, k, TO_Q, 2, send.at[lo, NEAR_Q], nr.at[lo, side[TO_Q]]),
        }

    def gather_copies(stage, k):
        buf = wg.at[k] if stage == 3 else part.at[k]
        return {
            (TO_P, 0): ring_copy(stage, k, TO_P, 0, buf.at[lo, OWN], buf.at[lo, NEAR_P]),
            (TO_Q, 0): ring_copy(stage, k, TO_Q, 0, buf.at[hi, OWN], buf.at[hi, NEAR_Q]),
            (TO_P, 1): ring_copy(stage, k, TO_P, 1, buf.at[hi, OWN], buf.at[hi, NEAR_P]),
            (TO_Q, 1): ring_copy(stage, k, TO_Q, 1, buf.at[lo, OWN], buf.at[lo, NEAR_Q]),
            (TO_P, 2): ring_copy(stage, k, TO_P, 2, buf.at[hi, NEAR_Q], buf.at[hi, FAR]),
            (TO_Q, 2): ring_copy(stage, k, TO_Q, 2, buf.at[lo, NEAR_P], buf.at[lo, FAR]),
        }

    copies = {}
    for k in range(CHUNKS):
        for stage in range(5):
            copies[stage, k] = reduce_copies(stage, k) if stage < 3 else gather_copies(stage, k)
    a_copies = [mate_copy(i, a_oth.at[:, slot[i]], a_blk.at[pl.ds(slab, slab), slot[i]]) for i in range(4)]
    m_copies = {(k, i): mate_copy(4 + 4 * k + i, pick.at[pl.ds(k * m, m), slot[i]], merged[k].at[:, slot[i]])
                for k in range(CHUNKS) for i in range(4)}
    first = 4 + 4 * CHUNKS
    x1_copies = [mate_copy(first + k, x1.at[k, :, own_half], x1.at[k, :, mate_half]) for k in range(CHUNKS)]
    x2_copies = [mate_copy(first + CHUNKS + k, x2own.at[k], x2rcv.at[k]) for k in range(CHUNKS)]
    z_copies = [mate_copy(first + 2 * CHUNKS + k, near.at[1, k, :, mate_half], near.at[0, k, :, mate_half]) for k in range(CHUNKS)]

    def by_rows(count, fn):
        def step(i, carry):
            fn(i)
            return carry
        lax.fori_loop(0, count // blk, step, 0)

    def rows_at(i, start=0):
        return pl.ds(pl.multiple_of(start + i * blk, blk), blk)

    def by_tiles(begin, end, fn):
        def step(t, carry):
            fn(pl.ds(pl.multiple_of(t * tile, 128), tile))
            return carry
        lax.fori_loop(begin, end, step, 0)

    def select_other(k, i):
        pick[pl.ds(k * m, m), slot[i]] = rows_cols(onehot[pl.ds(k * m, m), :], a_oth[:, slot[i]]).astype(bf16)

    def select_own(k, i):
        rk = pl.ds(k * m, m)
        here = (ids[rk, :] >= base_f) & (ids[rk, :] < base_f + slab)
        m_copies[k, i].wait_recv()
        mine = rows_cols(onehot[rk, :], a_blk[pl.ds(0, slab), slot[i]])
        merged[k][:, slot[i]] = jnp.where(here, mine, merged[k][:, slot[i]].astype(f32)).astype(bf16)

    def send_first(stage, k):
        cp = copies[stage, k]
        cp[TO_P, 0].start()
        cp[TO_Q, 0].start()
        cp[TO_P, 1].start()

    @scoped('start')
    def start(stage, k):
        cp = copies[stage, k]
        if stage in (1, 2):
            for c_ in copies[stage - 1, k].values():
                c_.wait_send()

            def push(at):
                if stage == 1:
                    part[k, :, at] = rows_cols(x1[k], a_blk[:, at])
                else:
                    both = rows_cols(pick[pl.ds(0, 2 * m), two[0]], a_blk[:, at])
                    part[k, :, at] = both[:m] + both[m:]

            def mate_rows(pair):
                if (stage, k) == (1, 0):
                    for i in pair:
                        a_copies[i].wait_recv()

            mate_rows((0, 1))
            by_tiles(0, 3, push)
            send_first(stage, k)
            mate_rows((2, 3))
            by_tiles(3, 6, push)
            cp[TO_Q, 1].start()
        else:
            for msg in (0, 1):
                cp[TO_P, msg].start()
                cp[TO_Q, msg].start()

    @scoped('middle')
    def middle(stage, k):
        cp = copies[stage, k]
        for way in (TO_P, TO_Q):
            with jax.named_scope('wait'):
                cp[way, 0].wait_recv()
            begin = 0 if way == TO_P else h
            dest = NEAR_Q if way == TO_P else NEAR_P
            if stage == 0:
                def select(i):
                    r = rows_at(i, begin)
                    rk = rows_at(i, k * m + begin)
                    here = (ids[rk, :] >= chip_f) & (ids[rk, :] < chip_f + 2 * slab)
                    merged[k][r, dest] = jnp.where(here, merged[k][r, dest].astype(f32),
                                                   far0[k, way, rows_at(i), :].astype(f32)).astype(bf16)
                by_rows(h, select)
            elif stage < 3:
                def add(i):
                    r = rows_at(i, begin)
                    part[k, r, dest] = part[k, r, dest] + far[stage - 1, k, way, rows_at(i), :]
                by_rows(h, add)
            cp[1 - way, 2].start()

    def pull(buf, k, at, use, meanwhile=None):
        def split(i):
            r = rows_at(i)
            full = buf[k, r, at]
            top = full.astype(bf16)
            rest = full - top.astype(f32)
            mid = rest.astype(bf16)
            pick[r, at] = top
            pick[rows_at(i, m), at] = mid
            pick[rows_at(i, 2 * m), at] = (rest - mid.astype(f32)).astype(bf16)
        by_rows(m, split)

        def product(r):
            three = rows_rows(pick[pl.ds(0, 3 * m), at], a_blk[r, at])
            use(r, three[:m] + three[m:2 * m] + three[2 * m:])
        if meanwhile is None:
            by_tiles(0, 3, product)
        else:
            by_tiles(1, 3, product)
            meanwhile()
            by_tiles(0, 1, product)

    def close(k, at, z):
        bc[:, at] = bc[:, at] + jnp.sum(x1[k, :, at].astype(f32) * z, axis=0, keepdims=True)

    @scoped('nears')
    def nears(stage, k, last=False):
        cp = copies[stage, k]
        if last:
            pull(part, k, OWN, functools.partial(close, k))
        with jax.named_scope('wait'):
            cp[TO_P, 1].wait_recv()
            cp[TO_Q, 1].wait_recv()

        def keep(r, z):
            if stage == 3:
                near[1, k, :, r] = z
            else:
                close(k, r, z)
        pull(wg if stage == 3 else part, k, pl.ds(slab, (2 if last else 3) * slab), keep)

    @scoped('finish')
    def finish(stage, k):
        cp = copies[stage, k]
        for way in (TO_P, TO_Q):
            with jax.named_scope('wait'):
                if stage < 3:
                    cp[way, 1].wait_recv()
                cp[way, 2].wait_recv()
        if stage == 0:
            def first_level(i):
                r = rows_at(i)
                x1[k, r, own_half] = (merged[k][r, OWN].astype(f32) + near0[k, r, side[0]].astype(f32)
                                      + near0[k, r, side[1]].astype(f32)).astype(bf16)
            by_rows(m, first_level)
            x1_copies[k].start()
            if k == 0:
                a_copies[3].start()
                for copy in m_copies.values():
                    copy.wait_send()
            with jax.named_scope('wait_mate'):
                x1_copies[k].wait_recv()
        elif stage == 1:
            def second_level(i):
                r = rows_at(i)
                rk = rows_at(i, k * m)
                total = part[k, r, OWN] + near[0, k, r, side[0]] + near[0, k, r, side[1]]
                seen = jnp.maximum(onehot[rk, :].astype(f32), x1[k, r, own_half].astype(f32))
                x2own[k, r, :] = total * (1.0 - seen)
            by_rows(m, second_level)
            x2_copies[k].start()

            def split(i, source, half):
                r = rows_at(i)
                full = source[k, r, :]
                top = full.astype(bf16)
                pick[r, half] = top
                pick[rows_at(i, m), half] = (full - top.astype(f32)).astype(bf16)
            by_rows(m, lambda i: split(i, x2own, own_half))
            with jax.named_scope('wait_mate'):
                x2_copies[k].wait_recv()
            by_rows(m, lambda i: split(i, x2rcv, mate_half))
        elif stage == 2:
            def third_level(i):
                r = rows_at(i)
                rk = rows_at(i, k * m)
                total = part[k, r, OWN] + near[1, k, r, side[0]] + near[1, k, r, side[1]]
                seen = jnp.maximum(onehot[rk, :].astype(f32), x1[k, r, own_half].astype(f32))
                seen = jnp.maximum(seen, jnp.where(x2own[k, r, :] > 0, 1.0, 0.0))
                paths = total * (1.0 - seen)
                reached = paths > 0
                wg[k, r, OWN] = jnp.where(reached, lw[1] / jnp.where(reached, paths, 1.0), 0.0)
            by_rows(m, third_level)
            for c_ in cp.values():
                c_.wait_send()
        elif stage == 3:
            def keep(r, z):
                near[1, k, :, r] = near[1, k, :, r] + z
            pull(wg, k, FAR, keep, z_copies[k].start)
            with jax.named_scope('wait_mate'):
                z_copies[k].wait_recv()

            def second_weights(i):
                r = rows_at(i)
                paths = x2own[k, r, :]
                delta = paths * (near[1, k, r, own_half] + near[0, k, r, mate_half])
                reached = paths > 0
                part[k, r, OWN] = jnp.where(reached, (lw[0] + delta) / jnp.where(reached, paths, 1.0), 0.0)
                bc[:, own_half] = bc[:, own_half] + jnp.sum(delta, axis=0, keepdims=True)
            by_rows(m, second_weights)
        else:
            pull(part, k, FAR, functools.partial(close, k))

    @scoped('other')
    def other(k, i):
        if k == 0:
            loads[0, i].wait()
        select_other(k, i)
        if (k, i) == (0, 0):
            with jax.named_scope('wait_barrier'):
                pl.semaphore_wait(barrier, 3 + 2 * (planes - 1))
        m_copies[k, i].start()

    @scoped('own')
    def own(k, i):
        if k == 0:
            loads[1, i].wait()
        select_own(k, i)

    def first_level_sends(k):
        own(k, 0)
        copies[0, k][TO_P, 0].start()
        copies[0, k][TO_Q, 0].start()
        own(k, 1)
        copies[0, k][TO_P, 1].start()
        own(k, 2)
        copies[0, k][TO_Q, 1].start()

    for i in range(3):
        other(0, i)
    a_copies[0].start()
    first_level_sends(0)
    lax.fori_loop(m // blk, src_count // blk, one_hot_rows, 0)
    bc[...] = jnp.zeros_like(bc)
    for i in range(3):
        other(1, i)
    a_copies[1].start()
    for k in range(CHUNKS):
        other(k, 3)
    a_copies[2].start()
    middle(0, 0)
    first_level_sends(1)
    for k in range(CHUNKS):
        own(k, 3)
    middle(0, 1)
    for stage in range(1, 5):
        finish(stage - 1, 0)
        start(stage, 0)
        if stage == 4:
            nears(3, 1)
        middle(stage, 0)
        finish(stage - 1, 1)
        start(stage, 1)
        if stage >= 3:
            nears(stage, 0)
        middle(stage, 1)
    finish(4, 0)
    nears(4, 1, last=True)
    finish(4, 1)

    total[...] = bc[...] * scale
    plane[pl.ds(s_me, 1)] = total[:, own_half][None]
    for o in range(planes):
        there = lax.rem(s_me + o, planes)
        for other_core in (0, 1):
            if o == 0 and not other_core:
                continue
            device = {"src": there, "graph": x * 2 + (1 - c)} if other_core else {"src": there}
            pltpu.make_async_remote_copy(src_ref=total.at[:, side[other_core]], dst_ref=plane.at[other_core * planes + s_me],
                                         send_sem=plane_s, recv_sem=plane_r,
                                         device_id=device, device_id_type=MESH).start()

    for copy in a_copies + x1_copies + x2_copies + z_copies:
        copy.wait_send()
    for k in range(CHUNKS):
        for stage in (3, 4):
            for c_ in copies[stage, k].values():
                c_.wait_send()
    arrivals = plane.at[pl.ds(0, 2 * planes - 1)]
    every = pltpu.make_async_remote_copy(src_ref=arrivals, dst_ref=arrivals, send_sem=plane_s, recv_sem=plane_r,
                                         device_id=to_mate, device_id_type=MESH)
    with jax.named_scope("wait_plane"):
        every.wait_recv()
    with jax.named_scope("sum_plane"):
        out[...] = jnp.sum(plane[...], axis=0)
    every.wait_send()


def solution(mesh):
    planes = mesh.shape["src"]
    ring = mesh.shape["graph"] // 2

    def device_program(adj_slab, src_local, level_weight):
        slab, vertex_count = adj_slab.shape
        src_count = src_local.shape[0]
        m = src_count // CHUNKS
        scale = vertex_count / (src_count * planes * (level_weight.shape[0] + 1) ** 3)
        wide = 4 * slab
        vmem = pltpu.VMEM
        sem = pltpu.SemaphoreType.DMA
        mates = 4 + 7 * CHUNKS
        rings = 5 * CHUNKS * 6
        flops = 2 * 9 * src_count * slab * vertex_count
        bc = pl.pallas_call(
            functools.partial(kernel, ring, planes, scale),
            out_shape=jax.ShapeDtypeStruct((1, slab), f32),
            in_specs=[pl.BlockSpec(memory_space=pl.ANY), pl.BlockSpec(memory_space=vmem), pl.BlockSpec(memory_space=pltpu.SMEM)],
            out_specs=pl.BlockSpec(memory_space=vmem),
            scratch_shapes=[
                vmem((2 * slab, wide), bf16), vmem((slab, wide), bf16),
                vmem((2 * src_count, wide), bf16), vmem((src_count, 1), f32), vmem((src_count, slab), bf16),
                vmem((CHUNKS, m, 2 * slab), bf16), vmem((CHUNKS, m, slab), f32), vmem((CHUNKS, m, slab), f32),
                vmem((CHUNKS, m, wide), f32), vmem((CHUNKS, m, wide), f32),
                vmem((CHUNKS, m, 2 * slab), bf16), vmem((CHUNKS, 2, m // 2, slab), bf16),
                vmem((2, CHUNKS, m, 2 * slab), f32), vmem((2, CHUNKS, 2, m // 2, slab), f32),
                vmem((1, 2 * slab), f32), vmem((1, 2 * slab), f32), vmem((2 * planes, 1, slab), f32),
                sem((8,)), sem((rings,)), sem((rings,)), sem((mates,)), sem((mates,)), sem, sem,
            ],
            compiler_params=pltpu.CompilerParams(collective_id=0, has_side_effects=True, vmem_limit_bytes=67043328),
            cost_estimate=pl.CostEstimate(flops=flops, bytes_accessed=2 * slab * vertex_count, transcendentals=0),
        )(adj_slab, src_local.reshape(1, src_count), level_weight)
        return bc.reshape(slab)

    return jax.shard_map(device_program, mesh=mesh,
                         in_specs=(P(("batch", "graph"), None), P(("batch", "src")), P(None)),
                         out_specs=P(("batch", "graph")), check_vma=False)
```

```python
import functools

import jax
import jax.numpy as jnp
from jax import lax
from jax.experimental import pallas as pl
from jax.experimental.pallas import tpu as pltpu
from jax.sharding import PartitionSpec as P

MESH = pl.DeviceIdType.MESH
f32, bf16 = jnp.float32, jnp.bfloat16
CHUNKS = 2
TO_P, TO_Q = 0, 1


def scoped(name):
    def wrap(fn):
        def inner(*a, **kw):
            tag = name + "".join(f"_{v}" for v in a if isinstance(v, int))
            with jax.named_scope(tag):
                return fn(*a, **kw)
        return inner
    return wrap


def rows_cols(lhs, rhs):
    return lax.dot_general(lhs, rhs, (((1,), (0,)), ((), ())), preferred_element_type=f32)


def rows_rows(lhs, rhs):
    return lax.dot_general(lhs, rhs, (((1,), (1,)), ((), ())), preferred_element_type=f32)


def kernel(ring, planes, scale, adj, src, lw, out,
           a_blk, a_oth, pick, ids, onehot, x1, x2own, x2rcv, part, wg,
           near0, far0, near, far, bc, total,
           load_sem, ssem, rsem, d2d_s, d2d_r, plane_s, plane_r):
    slab = a_oth.shape[0]
    cols_all = a_oth.shape[1]
    src_count = ids.shape[0]
    m = src_count // CHUNKS
    h = m // 2
    tile = 2 * slab // 3
    blk = min(32, h // 2)

    g = lax.axis_index("graph")
    s_me = lax.axis_index("src")
    x, c = g // 2, g % 2
    odd = lax.rem(x, 2)
    chip_p = x + 1 - 2 * odd
    chip_q = lax.rem(x + ring - 1 + 2 * odd, ring)
    chip_far = lax.rem(x + 2, ring)
    to_p = {"graph": chip_p * 2 + c}
    to_q = {"graph": chip_q * 2 + c}
    to_mate = {"graph": x * 2 + (1 - c)}
    chips = (chip_far, chip_p, chip_q, x)
    slot = [pl.ds(i * slab, slab) for i in range(4)]
    FAR, NEAR_P, NEAR_Q, OWN = slot

    loads = {}
    for i, chip in enumerate(chips):
        for own in (0, 1):
            at = pl.ds(pl.multiple_of((chip * 2 + (c if own else 1 - c)) * slab, 128), slab)
            target = a_blk.at[pl.ds(0, slab), slot[i]] if own else a_oth.at[:, slot[i]]
            loads[own, i] = pltpu.make_async_copy(adj.at[:, at], target, load_sem.at[4 * own + i])
    for own, i in ((0, 0), (0, 1), (0, 2), (1, 0), (1, 1), (1, 2), (0, 3), (1, 3)):
        loads[own, i].start()

    barrier = pltpu.get_barrier_semaphore()
    for dev in (to_p, to_q, to_mate):
        pl.semaphore_signal(barrier, inc=1, device_id=dev, device_id_type=MESH)
    for o in range(1, planes):
        there = lax.rem(s_me + o, planes)
        pl.semaphore_signal(barrier, inc=1, device_id={"src": there}, device_id_type=MESH)
        pl.semaphore_signal(barrier, inc=1, device_id={"src": there, "graph": x * 2 + (1 - c)}, device_id_type=MESH)

    row = lax.broadcasted_iota(jnp.int32, (src_count, src_count), 0)
    col = lax.broadcasted_iota(jnp.int32, (src_count, src_count), 1)
    ids[...] = jnp.sum(jnp.where(row == col, src[...].astype(f32), 0.0), axis=1, keepdims=True)
    base = g * slab
    base_f = base.astype(f32)
    chip_f = (x * 2 * slab).astype(f32)
    lane = (lax.broadcasted_iota(jnp.int32, (blk, slab), 1) + base).astype(f32)

    def one_hot_rows(i, carry):
        r = pl.ds(pl.multiple_of(i * blk, blk), blk)
        onehot[r, :] = jnp.where(ids[r, :] == lane, 1.0, 0.0).astype(bf16)
        return carry

    lax.fori_loop(0, m // blk, one_hot_rows, 0)

    def mate_copy(i, source, target):
        return pltpu.make_async_remote_copy(src_ref=source, dst_ref=target, send_sem=d2d_s.at[i], recv_sem=d2d_r.at[i],
                                            device_id=to_mate, device_id_type=MESH)

    def ring_copy(stage, k, way, msg, source, target):
        i = ((stage * CHUNKS + k) * 2 + way) * 4 + msg
        return pltpu.make_async_remote_copy(src_ref=source, dst_ref=target, send_sem=ssem.at[i], recv_sem=rsem.at[i],
                                            device_id=to_p if way == TO_P else to_q, device_id_type=MESH)

    lo, hi = pl.ds(0, h), pl.ds(h, h)
    side = [pl.ds(0, slab), pl.ds(slab, slab)]
    own_half, mate_half = side
    merged = [pick.at[pl.ds(src_count + k * m, m), :] for k in range(CHUNKS)]
    two = [pl.ds(0, 2 * slab), pl.ds(2 * slab, 2 * slab)]

    def reduce_copies(stage, k):
        if stage == 0:
            send, nr, fr = merged[k], near0.at[k], far0.at[k]
        else:
            send, nr, fr = part.at[k], near.at[stage - 1, k], far.at[stage - 1, k]
        return {
            (TO_P, 0): ring_copy(stage, k, TO_P, 0, send.at[lo, FAR], fr.at[TO_P]),
            (TO_Q, 0): ring_copy(stage, k, TO_Q, 0, send.at[hi, FAR], fr.at[TO_Q]),
            (TO_P, 1): ring_copy(stage, k, TO_P, 1, send.at[lo, NEAR_P], nr.at[lo, side[TO_P]]),
            (TO_Q, 1): ring_copy(stage, k, TO_Q, 1, send.at[hi, NEAR_Q], nr.at[hi, side[TO_Q]]),
            (TO_P, 2): ring_copy(stage, k, TO_P, 2, send.at[hi, NEAR_P], nr.at[hi, side[TO_P]]),
            (TO_Q, 2): ring_copy(stage, k, TO_Q, 2, send.at[lo, NEAR_Q], nr.at[lo, side[TO_Q]]),
        }

    def gather_copies(stage, k):
        buf = wg.at[k] if stage == 3 else part.at[k]
        if (stage, k) == (4, CHUNKS - 1):
            bands = [(2 + i, pl.ds(i * h // 2, h // 2), pl.ds(h + i * h // 2, h // 2)) for i in range(2)]
        else:
            bands = [(2, lo, hi)]
        relay = {}
        for msg, low, high in bands:
            relay[TO_P, msg] = ring_copy(stage, k, TO_P, msg, buf.at[high, NEAR_Q], buf.at[high, FAR])
            relay[TO_Q, msg] = ring_copy(stage, k, TO_Q, msg, buf.at[low, NEAR_P], buf.at[low, FAR])
        return {
            **relay,
            (TO_P, 0): ring_copy(stage, k, TO_P, 0, buf.at[lo, OWN], buf.at[lo, NEAR_P]),
            (TO_Q, 0): ring_copy(stage, k, TO_Q, 0, buf.at[hi, OWN], buf.at[hi, NEAR_Q]),
            (TO_P, 1): ring_copy(stage, k, TO_P, 1, buf.at[hi, OWN], buf.at[hi, NEAR_P]),
            (TO_Q, 1): ring_copy(stage, k, TO_Q, 1, buf.at[lo, OWN], buf.at[lo, NEAR_Q]),
        }

    copies = {}
    for k in range(CHUNKS):
        for stage in range(5):
            copies[stage, k] = reduce_copies(stage, k) if stage < 3 else gather_copies(stage, k)
    a_copies = [mate_copy(i, a_oth.at[:, slot[i]], a_blk.at[pl.ds(slab, slab), slot[i]]) for i in range(4)]
    m_copies = {(k, i): mate_copy(4 + 4 * k + i, pick.at[pl.ds(k * m, m), slot[i]], merged[k].at[:, slot[i]])
                for k in range(CHUNKS) for i in range(4)}
    first = 4 + 4 * CHUNKS
    x1_copies = [mate_copy(first + k, x1.at[k, :, own_half], x1.at[k, :, mate_half]) for k in range(CHUNKS)]
    x2_copies = [mate_copy(first + CHUNKS + k, x2own.at[k], x2rcv.at[k]) for k in range(CHUNKS)]
    z_copies = [mate_copy(first + 2 * CHUNKS + k, near.at[1, k, :, mate_half], near.at[0, k, :, mate_half]) for k in range(CHUNKS)]

    def by_rows(count, fn):
        def step(i, carry):
            fn(i)
            return carry
        lax.fori_loop(0, count // blk, step, 0)

    def rows_at(i, start=0):
        return pl.ds(pl.multiple_of(start + i * blk, blk), blk)

    def by_tiles(begin, end, fn):
        def step(t, carry):
            fn(pl.ds(pl.multiple_of(t * tile, 128), tile))
            return carry
        lax.fori_loop(begin, end, step, 0)

    def select_other(k, i):
        pick[pl.ds(k * m, m), slot[i]] = rows_cols(onehot[pl.ds(k * m, m), :], a_oth[:, slot[i]]).astype(bf16)

    def select_own(k, i):
        rk = pl.ds(k * m, m)
        here = (ids[rk, :] >= base_f) & (ids[rk, :] < base_f + slab)
        m_copies[k, i].wait_recv()
        mine = rows_cols(onehot[rk, :], a_blk[pl.ds(0, slab), slot[i]])
        merged[k][:, slot[i]] = jnp.where(here, mine, merged[k][:, slot[i]].astype(f32)).astype(bf16)

    def send_first(stage, k):
        cp = copies[stage, k]
        cp[TO_P, 0].start()
        cp[TO_Q, 0].start()
        cp[TO_P, 1].start()

    @scoped('start')
    def start(stage, k):
        cp = copies[stage, k]
        if stage in (1, 2):
            for c_ in copies[stage - 1, k].values():
                c_.wait_send()

            def push(at):
                if stage == 1:
                    part[k, :, at] = rows_cols(x1[k], a_blk[:, at])
                else:
                    both = rows_cols(pick[pl.ds(0, 2 * m), two[0]], a_blk[:, at])
                    part[k, :, at] = both[:m] + both[m:]

            def mate_rows(pair):
                if (stage, k) == (1, 0):
                    for i in pair:
                        a_copies[i].wait_recv()

            mate_rows((0, 1))
            by_tiles(0, 3, push)
            send_first(stage, k)
            mate_rows((2, 3))
            by_tiles(3, 6, push)
            cp[TO_Q, 1].start()
        else:
            for msg in (0, 1):
                cp[TO_P, msg].start()
                cp[TO_Q, msg].start()

    @scoped('middle')
    def middle(stage, k):
        cp = copies[stage, k]
        for way in (TO_P, TO_Q):
            with jax.named_scope('wait'):
                cp[way, 0].wait_recv()
            begin = 0 if way == TO_P else h
            dest = NEAR_Q if way == TO_P else NEAR_P
            if stage == 0:
                def select(i):
                    r = rows_at(i, begin)
                    rk = rows_at(i, k * m + begin)
                    here = (ids[rk, :] >= chip_f) & (ids[rk, :] < chip_f + 2 * slab)
                    merged[k][r, dest] = jnp.where(here, merged[k][r, dest].astype(f32),
                                                   far0[k, way, rows_at(i), :].astype(f32)).astype(bf16)
                by_rows(h, select)
            elif stage < 3:
                def add(i):
                    r = rows_at(i, begin)
                    part[k, r, dest] = part[k, r, dest] + far[stage - 1, k, way, rows_at(i), :]
                by_rows(h, add)
            cp[1 - way, 2].start()
            if (1 - way, 3) in cp:
                cp[1 - way, 3].start()

    def pull(buf, k, at, use, meanwhile=None):
        def split(i):
            r = rows_at(i)
            full = buf[k, r, at]
            top = full.astype(bf16)
            rest = full - top.astype(f32)
            mid = rest.astype(bf16)
            pick[r, at] = top
            pick[rows_at(i, m), at] = mid
            pick[rows_at(i, 2 * m), at] = (rest - mid.astype(f32)).astype(bf16)
        by_rows(m, split)

        def product(r):
            three = rows_rows(pick[pl.ds(0, 3 * m), at], a_blk[r, at])
            use(r, three[:m] + three[m:2 * m] + three[2 * m:])
        if meanwhile is None:
            by_tiles(0, 3, product)
        else:
            by_tiles(1, 3, product)
            meanwhile()
            by_tiles(0, 1, product)

    def close(k, at, z):
        bc[:, at] = bc[:, at] + jnp.sum(x1[k, :, at].astype(f32) * z, axis=0, keepdims=True)

    def last_rows(at, begin, count):
        k = CHUNKS - 1
        rows = pl.ds(begin, count)
        full = part[k, rows, at]
        top = full.astype(bf16)
        rest = full - top.astype(f32)
        mid = rest.astype(bf16)
        pick[pl.ds(0, count), at] = top
        pick[pl.ds(count, count), at] = mid
        pick[pl.ds(2 * count, count), at] = (rest - mid.astype(f32)).astype(bf16)

        def product(r):
            three = rows_rows(pick[pl.ds(0, 3 * count), at], a_blk[r, at])
            z = three[:count] + three[count:2 * count] + three[2 * count:]
            bc[:, r] = bc[:, r] + jnp.sum(x1[k, rows, r].astype(f32) * z, axis=0, keepdims=True)
        by_tiles(0, 3, product)

    @scoped('last_far')
    def last_far(msg):
        k = CHUNKS - 1
        cp = copies[4, k]
        cp[TO_P, 2 + msg].wait_recv()
        cp[TO_Q, 2 + msg].wait_recv()
        q = h // 2
        for n, begin in enumerate((msg * q, h + msg * q)):
            full = part[k, pl.ds(begin, q), FAR]
            top = full.astype(bf16)
            rest = full - top.astype(f32)
            mid = rest.astype(bf16)
            pick[pl.ds(n * q, q), FAR] = top
            pick[pl.ds((2 + n) * q, q), FAR] = mid
            pick[pl.ds((4 + n) * q, q), FAR] = (rest - mid.astype(f32)).astype(bf16)

        def product(r):
            three = rows_rows(pick[pl.ds(0, 3 * h), FAR], a_blk[r, FAR])
            z = three[:h] + three[h:2 * h] + three[2 * h:]
            weighted = (x1[k, pl.ds(msg * q, q), r].astype(f32) * z[:q] + x1[k, pl.ds(h + msg * q, q), r].astype(f32) * z[q:])
            bc[:, r] = bc[:, r] + jnp.sum(weighted, axis=0, keepdims=True)
        by_tiles(0, 3, product)

    @scoped('last_own')
    def last_own():
        pull(part, CHUNKS - 1, OWN, functools.partial(close, CHUNKS - 1))

    @scoped('last_nears')
    def last_nears(msg):
        cp = copies[4, CHUNKS - 1]
        if msg:
            cp[TO_P, 1].wait_recv()
            cp[TO_Q, 1].wait_recv()
        last_rows(NEAR_P, h * msg, h)
        last_rows(NEAR_Q, h * (1 - msg), h)

    @scoped('nears')
    def nears(stage, k):
        cp = copies[stage, k]
        with jax.named_scope('wait'):
            cp[TO_P, 1].wait_recv()
            cp[TO_Q, 1].wait_recv()

        def keep(r, z):
            if stage == 3:
                near[1, k, :, r] = z
            else:
                close(k, r, z)
        pull(wg if stage == 3 else part, k, pl.ds(slab, 3 * slab), keep)

    @scoped('finish')
    def finish(stage, k):
        cp = copies[stage, k]
        for way in (TO_P, TO_Q):
            with jax.named_scope('wait'):
                if stage < 3:
                    cp[way, 1].wait_recv()
                cp[way, 2].wait_recv()
        if stage == 0:
            def first_level(i):
                r = rows_at(i)
                x1[k, r, own_half] = (merged[k][r, OWN].astype(f32) + near0[k, r, side[0]].astype(f32)
                                      + near0[k, r, side[1]].astype(f32)).astype(bf16)
            by_rows(m, first_level)
            x1_copies[k].start()
            if k == 0:
                a_copies[3].start()
                for copy in m_copies.values():
                    copy.wait_send()
            with jax.named_scope('wait_mate'):
                x1_copies[k].wait_recv()
        elif stage == 1:
            def second_level(i):
                r = rows_at(i)
                rk = rows_at(i, k * m)
                total = part[k, r, OWN] + near[0, k, r, side[0]] + near[0, k, r, side[1]]
                seen = jnp.maximum(onehot[rk, :].astype(f32), x1[k, r, own_half].astype(f32))
                x2own[k, r, :] = total * (1.0 - seen)
            by_rows(m, second_level)
            x2_copies[k].start()

            def split(i, source, half):
                r = rows_at(i)
                full = source[k, r, :]
                top = full.astype(bf16)
                pick[r, half] = top
                pick[rows_at(i, m), half] = (full - top.astype(f32)).astype(bf16)
            by_rows(m, lambda i: split(i, x2own, own_half))
            with jax.named_scope('wait_mate'):
                x2_copies[k].wait_recv()
            by_rows(m, lambda i: split(i, x2rcv, mate_half))
        elif stage == 2:
            def third_level(i):
                r = rows_at(i)
                rk = rows_at(i, k * m)
                total = part[k, r, OWN] + near[1, k, r, side[0]] + near[1, k, r, side[1]]
                seen = jnp.maximum(onehot[rk, :].astype(f32), x1[k, r, own_half].astype(f32))
                seen = jnp.maximum(seen, jnp.where(x2own[k, r, :] > 0, 1.0, 0.0))
                paths = total * (1.0 - seen)
                reached = paths > 0
                wg[k, r, OWN] = jnp.where(reached, lw[1] / jnp.where(reached, paths, 1.0), 0.0)
            by_rows(m, third_level)
            for c_ in cp.values():
                c_.wait_send()
        elif stage == 3:
            def keep(r, z):
                near[1, k, :, r] = near[1, k, :, r] + z
            pull(wg, k, FAR, keep, z_copies[k].start)
            with jax.named_scope('wait_mate'):
                z_copies[k].wait_recv()

            def second_weights(i):
                r = rows_at(i)
                paths = x2own[k, r, :]
                delta = paths * (near[1, k, r, own_half] + near[0, k, r, mate_half])
                reached = paths > 0
                part[k, r, OWN] = jnp.where(reached, (lw[0] + delta) / jnp.where(reached, paths, 1.0), 0.0)
                bc[:, own_half] = bc[:, own_half] + jnp.sum(delta, axis=0, keepdims=True)
            by_rows(m, second_weights)
        else:
            pull(part, k, FAR, functools.partial(close, k))

    @scoped('other')
    def other(k, i):
        if k == 0:
            loads[0, i].wait()
        select_other(k, i)
        if (k, i) == (0, 0):
            with jax.named_scope('wait_barrier'):
                pl.semaphore_wait(barrier, 3 + 2 * (planes - 1))
        m_copies[k, i].start()

    @scoped('own')
    def own(k, i):
        if k == 0:
            loads[1, i].wait()
        select_own(k, i)

    def first_level_sends(k):
        own(k, 0)
        copies[0, k][TO_P, 0].start()
        copies[0, k][TO_Q, 0].start()
        own(k, 1)
        copies[0, k][TO_P, 1].start()
        own(k, 2)
        copies[0, k][TO_Q, 1].start()

    for i in range(3):
        other(0, i)
    a_copies[0].start()
    first_level_sends(0)
    lax.fori_loop(m // blk, src_count // blk, one_hot_rows, 0)
    bc[...] = jnp.zeros_like(bc)
    for i in range(3):
        other(1, i)
    a_copies[1].start()
    for k in range(CHUNKS):
        other(k, 3)
    a_copies[2].start()
    middle(0, 0)
    first_level_sends(1)
    for k in range(CHUNKS):
        own(k, 3)
    middle(0, 1)
    for stage in range(1, 5):
        finish(stage - 1, 0)
        start(stage, 0)
        if stage == 4:
            nears(3, 1)
        middle(stage, 0)
        finish(stage - 1, 1)
        start(stage, 1)
        if stage >= 3:
            nears(stage, 0)
        if stage == 4:
            last_own()
        middle(stage, 1)
    finish(4, 0)
    last_nears(0)
    last_nears(1)
    last_far(0)
    last_far(1)

    total[...] = bc[...] * scale
    keep_own = pltpu.make_async_copy(total.at[:, own_half], out.at[s_me], load_sem.at[0])
    keep_own.start()
    for o in range(planes):
        there = lax.rem(s_me + o, planes)
        for other_core in (0, 1):
            if o == 0 and not other_core:
                continue
            device = {"src": there, "graph": x * 2 + (1 - c)} if other_core else {"src": there}
            pltpu.make_async_remote_copy(src_ref=total.at[:, side[other_core]], dst_ref=out.at[other_core * planes + s_me],
                                         send_sem=plane_s, recv_sem=plane_r,
                                         device_id=device, device_id_type=MESH).start()

    for copy in a_copies + x1_copies + x2_copies + z_copies:
        copy.wait_send()
    for k in range(CHUNKS):
        for stage in (3, 4):
            for c_ in copies[stage, k].values():
                c_.wait_send()
    keep_own.wait()
    arrivals = out.at[pl.ds(0, 2 * planes - 1)]
    every = pltpu.make_async_remote_copy(src_ref=arrivals, dst_ref=arrivals, send_sem=plane_s, recv_sem=plane_r,
                                         device_id=to_mate, device_id_type=MESH)
    with jax.named_scope("wait_plane"):
        every.wait_recv()
    every.wait_send()


def solution(mesh):
    planes = mesh.shape["src"]
    ring = mesh.shape["graph"] // 2

    def device_program(adj_slab, src_local, level_weight):
        slab, vertex_count = adj_slab.shape
        src_count = src_local.shape[0]
        m = src_count // CHUNKS
        scale = vertex_count / (src_count * planes * (level_weight.shape[0] + 1) ** 3)
        wide = 4 * slab
        vmem = pltpu.VMEM
        sem = pltpu.SemaphoreType.DMA
        mates = 4 + 7 * CHUNKS
        rings = 5 * CHUNKS * 8
        flops = 2 * 9 * src_count * slab * vertex_count
        bc = pl.pallas_call(
            functools.partial(kernel, ring, planes, scale),
            out_shape=jax.ShapeDtypeStruct((2 * planes, 1, slab), f32),
            in_specs=[pl.BlockSpec(memory_space=pl.ANY), pl.BlockSpec(memory_space=vmem), pl.BlockSpec(memory_space=pltpu.SMEM)],
            out_specs=pl.BlockSpec(memory_space=pl.ANY),
            scratch_shapes=[
                vmem((2 * slab, wide), bf16), vmem((slab, wide), bf16),
                vmem((2 * src_count, wide), bf16), vmem((src_count, 1), f32), vmem((src_count, slab), bf16),
                vmem((CHUNKS, m, 2 * slab), bf16), vmem((CHUNKS, m, slab), f32), vmem((CHUNKS, m, slab), f32),
                vmem((CHUNKS, m, wide), f32), vmem((CHUNKS, m, wide), f32),
                vmem((CHUNKS, m, 2 * slab), bf16), vmem((CHUNKS, 2, m // 2, slab), bf16),
                vmem((2, CHUNKS, m, 2 * slab), f32), vmem((2, CHUNKS, 2, m // 2, slab), f32),
                vmem((1, 2 * slab), f32), vmem((1, 2 * slab), f32),
                sem((8,)), sem((rings,)), sem((rings,)), sem((mates,)), sem((mates,)), sem, sem,
            ],
            compiler_params=pltpu.CompilerParams(collective_id=0, has_side_effects=True, vmem_limit_bytes=67043328),
            cost_estimate=pl.CostEstimate(flops=flops, bytes_accessed=2 * slab * vertex_count, transcendentals=0),
        )(adj_slab, src_local.reshape(1, src_count), level_weight)
        return jnp.sum(bc, axis=(0, 1))

    return jax.shard_map(device_program, mesh=mesh,
                         in_specs=(P(("batch", "graph"), None), P(("batch", "src")), P(None)),
                         out_specs=P(("batch", "graph")), check_vma=False)
```

```python
import functools

import jax
import jax.numpy as jnp
from jax import lax
from jax.experimental import pallas as pl
from jax.experimental.pallas import tpu as pltpu
from jax.sharding import PartitionSpec as P

MESH = pl.DeviceIdType.MESH
f32, bf16 = jnp.float32, jnp.bfloat16
CHUNKS = 2
TO_P, TO_Q = 0, 1


def scoped(name):
    def wrap(fn):
        def inner(*a, **kw):
            tag = name + "".join(f"_{v}" for v in a if isinstance(v, int))
            with jax.named_scope(tag):
                return fn(*a, **kw)
        return inner
    return wrap


def rows_cols(lhs, rhs):
    return lax.dot_general(lhs, rhs, (((1,), (0,)), ((), ())), preferred_element_type=f32)


def rows_rows(lhs, rhs):
    return lax.dot_general(lhs, rhs, (((1,), (1,)), ((), ())), preferred_element_type=f32)


def kernel(ring, planes, scale, adj, src, lw, out,
           a_blk, a_oth, pick, ids, onehot, x1, x2own, x2rcv, part, wg,
           near0, far0, near, far, bc, total,
           load_sem, ssem, rsem, d2d_s, d2d_r, plane_s, plane_r):
    slab = a_oth.shape[0]
    cols_all = a_oth.shape[1]
    src_count = ids.shape[0]
    m = src_count // CHUNKS
    h = m // 2
    tile = 2 * slab // 3
    blk = min(32, h)

    g = lax.axis_index("graph")
    s_me = lax.axis_index("src")
    x, c = g // 2, g % 2
    odd = lax.rem(x, 2)
    chip_p = x + 1 - 2 * odd
    chip_q = lax.rem(x + ring - 1 + 2 * odd, ring)
    chip_far = lax.rem(x + 2, ring)
    to_p = {"graph": chip_p * 2 + c}
    to_q = {"graph": chip_q * 2 + c}
    to_mate = {"graph": x * 2 + (1 - c)}
    chips = (chip_far, chip_p, chip_q, x)
    slot = [pl.ds(i * slab, slab) for i in range(4)]
    FAR, NEAR_P, NEAR_Q, OWN = slot

    loads = {}
    for i, chip in enumerate(chips):
        for own in (0, 1):
            at = pl.ds(pl.multiple_of((chip * 2 + (c if own else 1 - c)) * slab, 128), slab)
            target = a_blk.at[pl.ds(0, slab), slot[i]] if own else a_oth.at[:, slot[i]]
            loads[own, i] = pltpu.make_async_copy(adj.at[:, at], target, load_sem.at[4 * own + i])
    for own, i in ((0, 0), (1, 0), (0, 1), (0, 2), (1, 1), (1, 2), (0, 3), (1, 3)):
        loads[own, i].start()

    barrier = pltpu.get_barrier_semaphore()
    for dev in (to_p, to_q, to_mate):
        pl.semaphore_signal(barrier, inc=1, device_id=dev, device_id_type=MESH)
    for o in range(1, planes):
        there = lax.rem(s_me + o, planes)
        pl.semaphore_signal(barrier, inc=1, device_id={"src": there}, device_id_type=MESH)
        pl.semaphore_signal(barrier, inc=1, device_id={"src": there, "graph": x * 2 + (1 - c)}, device_id_type=MESH)

    row = lax.broadcasted_iota(jnp.int32, (src_count, src_count), 0)
    col = lax.broadcasted_iota(jnp.int32, (src_count, src_count), 1)
    ids[...] = jnp.sum(jnp.where(row == col, src[...].astype(f32), 0.0), axis=1, keepdims=True)
    base = g * slab
    base_f = base.astype(f32)
    chip_f = (x * 2 * slab).astype(f32)
    lane = (lax.broadcasted_iota(jnp.int32, (blk, slab), 1) + base).astype(f32)

    def one_hot_rows(i, carry):
        r = pl.ds(pl.multiple_of(i * blk, blk), blk)
        onehot[r, :] = jnp.where(ids[r, :] == lane, 1.0, 0.0).astype(bf16)
        return carry

    lax.fori_loop(0, m // blk, one_hot_rows, 0)

    def mate_copy(i, source, target):
        return pltpu.make_async_remote_copy(src_ref=source, dst_ref=target, send_sem=d2d_s.at[i], recv_sem=d2d_r.at[i],
                                            device_id=to_mate, device_id_type=MESH)

    def ring_copy(stage, k, way, msg, source, target):
        i = ((stage * CHUNKS + k) * 2 + way) * 4 + msg
        return pltpu.make_async_remote_copy(src_ref=source, dst_ref=target, send_sem=ssem.at[i], recv_sem=rsem.at[i],
                                            device_id=to_p if way == TO_P else to_q, device_id_type=MESH)

    lo, hi = pl.ds(0, h), pl.ds(h, h)
    side = [pl.ds(0, slab), pl.ds(slab, slab)]
    own_half, mate_half = side
    merged = [pick.at[pl.ds(src_count + k * m, m), :] for k in range(CHUNKS)]
    two = [pl.ds(0, 2 * slab), pl.ds(2 * slab, 2 * slab)]

    def reduce_copies(stage, k):
        if stage == 0:
            send, nr, fr = merged[k], near0.at[k], far0.at[k]
        else:
            send, nr, fr = part.at[k], near.at[stage - 1, k], far.at[stage - 1, k]
        return {
            (TO_P, 0): ring_copy(stage, k, TO_P, 0, send.at[lo, FAR], fr.at[TO_P]),
            (TO_Q, 0): ring_copy(stage, k, TO_Q, 0, send.at[hi, FAR], fr.at[TO_Q]),
            (TO_P, 1): ring_copy(stage, k, TO_P, 1, send.at[lo, NEAR_P], nr.at[lo, side[TO_P]]),
            (TO_Q, 1): ring_copy(stage, k, TO_Q, 1, send.at[hi, NEAR_Q], nr.at[hi, side[TO_Q]]),
            (TO_P, 2): ring_copy(stage, k, TO_P, 2, send.at[hi, NEAR_P], nr.at[hi, side[TO_P]]),
            (TO_Q, 2): ring_copy(stage, k, TO_Q, 2, send.at[lo, NEAR_Q], nr.at[lo, side[TO_Q]]),
        }

    tail = slab // 256 * 128
    far_parts = [(2, 0, slab - tail), (3, slab - tail, tail)]

    def gather_copies(stage, k):
        buf = wg.at[k] if stage == 3 else part.at[k]
        if (stage, k) == (4, CHUNKS - 1):
            bands = far_parts
        else:
            bands = [(2, 0, slab)]
        relay = {}
        for msg, begin, width in bands:
            from_p, from_q, to_far = [pl.ds(n * slab + begin, width) for n in (1, 2, 0)]
            relay[TO_P, msg] = ring_copy(stage, k, TO_P, msg, buf.at[hi, from_q], buf.at[hi, to_far])
            relay[TO_Q, msg] = ring_copy(stage, k, TO_Q, msg, buf.at[lo, from_p], buf.at[lo, to_far])
        return {
            **relay,
            (TO_P, 0): ring_copy(stage, k, TO_P, 0, buf.at[lo, OWN], buf.at[lo, NEAR_P]),
            (TO_Q, 0): ring_copy(stage, k, TO_Q, 0, buf.at[hi, OWN], buf.at[hi, NEAR_Q]),
            (TO_P, 1): ring_copy(stage, k, TO_P, 1, buf.at[hi, OWN], buf.at[hi, NEAR_P]),
            (TO_Q, 1): ring_copy(stage, k, TO_Q, 1, buf.at[lo, OWN], buf.at[lo, NEAR_Q]),
        }

    copies = {}
    for k in range(CHUNKS):
        for stage in range(5):
            copies[stage, k] = reduce_copies(stage, k) if stage < 3 else gather_copies(stage, k)
    a_copies = [mate_copy(i, a_oth.at[:, slot[i]], a_blk.at[pl.ds(slab, slab), slot[i]]) for i in range(4)]
    m_copies = {(k, i): mate_copy(4 + 4 * k + i, pick.at[pl.ds(k * m, m), slot[i]], merged[k].at[:, slot[i]])
                for k in range(CHUNKS) for i in range(4)}
    first = 4 + 4 * CHUNKS
    x1_copies = [mate_copy(first + k, x1.at[k, :, own_half], x1.at[k, :, mate_half]) for k in range(CHUNKS)]
    x2_copies = [mate_copy(first + CHUNKS + k, x2own.at[k], x2rcv.at[k]) for k in range(CHUNKS)]
    z_copies = [mate_copy(first + 2 * CHUNKS + k, near.at[1, k, :, mate_half], near.at[0, k, :, mate_half]) for k in range(CHUNKS)]

    def by_rows(count, fn):
        def step(i, carry):
            fn(i)
            return carry
        lax.fori_loop(0, count // blk, step, 0)

    def rows_at(i, start=0):
        return pl.ds(pl.multiple_of(start + i * blk, blk), blk)

    def by_tiles(begin, end, fn):
        def step(t, carry):
            fn(pl.ds(pl.multiple_of(t * tile, 128), tile))
            return carry
        lax.fori_loop(begin, end, step, 0)

    def select_other(k, i):
        pick[pl.ds(k * m, m), slot[i]] = rows_cols(onehot[pl.ds(k * m, m), :], a_oth[:, slot[i]]).astype(bf16)

    def select_own(k, i):
        rk = pl.ds(k * m, m)
        here = (ids[rk, :] >= base_f) & (ids[rk, :] < base_f + slab)
        if (k, i) == (0, 0):
            x1[k, :, own_half] = rows_cols(onehot[rk, :], a_blk[pl.ds(0, slab), slot[i]]).astype(bf16)
            other(0, 1)
            m_copies[k, i].wait_recv()
            mine = x1[k, :, own_half].astype(f32)
        else:
            m_copies[k, i].wait_recv()
            mine = rows_cols(onehot[rk, :], a_blk[pl.ds(0, slab), slot[i]])
        merged[k][:, slot[i]] = jnp.where(here, mine, merged[k][:, slot[i]].astype(f32)).astype(bf16)

    def send_first(stage, k):
        cp = copies[stage, k]
        cp[TO_P, 0].start()
        cp[TO_Q, 0].start()
        cp[TO_P, 1].start()

    @scoped('start')
    def start(stage, k):
        cp = copies[stage, k]
        if stage in (1, 2):
            for c_ in copies[stage - 1, k].values():
                c_.wait_send()

            def push(at):
                if stage == 1:
                    part[k, :, at] = rows_cols(x1[k], a_blk[:, at])
                else:
                    both = rows_cols(pick[pl.ds(0, 2 * m), two[0]], a_blk[:, at])
                    part[k, :, at] = both[:m] + both[m:]

            def mate_rows(pair):
                if (stage, k) == (1, 0):
                    for i in pair:
                        a_copies[i].wait_recv()

            mate_rows((0, 1))
            by_tiles(0, 3, push)
            send_first(stage, k)
            mate_rows((2, 3))
            by_tiles(3, 6, push)
            cp[TO_Q, 1].start()
        else:
            for msg in (0, 1):
                cp[TO_P, msg].start()
                cp[TO_Q, msg].start()

    @scoped('middle')
    def middle(stage, k):
        cp = copies[stage, k]
        for way in (TO_P, TO_Q):
            with jax.named_scope('wait'):
                cp[way, 0].wait_recv()
            begin = 0 if way == TO_P else h
            dest = NEAR_Q if way == TO_P else NEAR_P
            if stage == 0:
                def select(i):
                    r = rows_at(i, begin)
                    rk = rows_at(i, k * m + begin)
                    here = (ids[rk, :] >= chip_f) & (ids[rk, :] < chip_f + 2 * slab)
                    merged[k][r, dest] = jnp.where(here, merged[k][r, dest].astype(f32),
                                                   far0[k, way, rows_at(i), :].astype(f32)).astype(bf16)
                by_rows(h, select)
            elif stage < 3:
                def add(i):
                    r = rows_at(i, begin)
                    part[k, r, dest] = part[k, r, dest] + far[stage - 1, k, way, rows_at(i), :]
                by_rows(h, add)
            cp[1 - way, 2].start()
            if (1 - way, 3) in cp:
                cp[1 - way, 3].start()

    def pull(buf, k, at, use, meanwhile=None):
        def split(i):
            r = rows_at(i)
            full = buf[k, r, at]
            top = full.astype(bf16)
            rest = full - top.astype(f32)
            mid = rest.astype(bf16)
            pick[r, at] = top
            pick[rows_at(i, m), at] = mid
            pick[rows_at(i, 2 * m), at] = (rest - mid.astype(f32)).astype(bf16)
        by_rows(m, split)

        def product(r):
            three = rows_rows(pick[pl.ds(0, 3 * m), at], a_blk[r, at])
            use(r, three[:m] + three[m:2 * m] + three[2 * m:])
        if meanwhile is None:
            by_tiles(0, 3, product)
        else:
            by_tiles(1, 3, product)
            meanwhile()
            by_tiles(0, 1, product)

    def close(k, at, z):
        bc[:, at] = bc[:, at] + jnp.sum(x1[k, :, at].astype(f32) * z, axis=0, keepdims=True)

    @scoped('last_far')
    def last_far(n):
        k = CHUNKS - 1
        msg, begin, width = far_parts[n]
        copies[4, k][TO_P, msg].wait_recv()
        copies[4, k][TO_Q, msg].wait_recv()
        pull(part, k, pl.ds(begin, width), functools.partial(close, k))

    @scoped('last_own')
    def last_own():
        pull(part, CHUNKS - 1, OWN, functools.partial(close, CHUNKS - 1))

    @scoped('last_nears')
    def last_nears():
        k = CHUNKS - 1
        copies[4, k][TO_P, 1].wait_recv()
        copies[4, k][TO_Q, 1].wait_recv()
        pull(part, k, pl.ds(slab, 2 * slab), functools.partial(close, k))

    @scoped('nears')
    def nears(stage, k):
        cp = copies[stage, k]
        with jax.named_scope('wait'):
            cp[TO_P, 1].wait_recv()
            cp[TO_Q, 1].wait_recv()

        def keep(r, z):
            if stage == 3:
                near[1, k, :, r] = z
            else:
                close(k, r, z)
        pull(wg if stage == 3 else part, k, pl.ds(slab, 3 * slab), keep)

    @scoped('finish')
    def finish(stage, k):
        cp = copies[stage, k]
        for way in (TO_P, TO_Q):
            with jax.named_scope('wait'):
                if stage < 3:
                    cp[way, 1].wait_recv()
                cp[way, 2].wait_recv()
        if stage == 0:
            def first_level(i):
                r = rows_at(i)
                x1[k, r, own_half] = (merged[k][r, OWN].astype(f32) + near0[k, r, side[0]].astype(f32)
                                      + near0[k, r, side[1]].astype(f32)).astype(bf16)
            by_rows(m, first_level)
            x1_copies[k].start()
            if k == 0:
                a_copies[3].start()
                for copy in m_copies.values():
                    copy.wait_send()
            with jax.named_scope('wait_mate'):
                x1_copies[k].wait_recv()
        elif stage == 1:
            def second_level(i):
                r = rows_at(i)
                rk = rows_at(i, k * m)
                total = part[k, r, OWN] + near[0, k, r, side[0]] + near[0, k, r, side[1]]
                seen = jnp.maximum(onehot[rk, :].astype(f32), x1[k, r, own_half].astype(f32))
                x2own[k, r, :] = total * (1.0 - seen)
            by_rows(m, second_level)
            x2_copies[k].start()

            def split(i, source, half):
                r = rows_at(i)
                full = source[k, r, :]
                top = full.astype(bf16)
                pick[r, half] = top
                pick[rows_at(i, m), half] = (full - top.astype(f32)).astype(bf16)
            by_rows(m, lambda i: split(i, x2own, own_half))
            with jax.named_scope('wait_mate'):
                x2_copies[k].wait_recv()
            by_rows(m, lambda i: split(i, x2rcv, mate_half))
        elif stage == 2:
            def third_level(i):
                r = rows_at(i)
                rk = rows_at(i, k * m)
                total = part[k, r, OWN] + near[1, k, r, side[0]] + near[1, k, r, side[1]]
                seen = jnp.maximum(onehot[rk, :].astype(f32), x1[k, r, own_half].astype(f32))
                seen = jnp.maximum(seen, jnp.where(x2own[k, r, :] > 0, 1.0, 0.0))
                paths = total * (1.0 - seen)
                reached = paths > 0
                wg[k, r, OWN] = jnp.where(reached, lw[1] / jnp.where(reached, paths, 1.0), 0.0)
            by_rows(m, third_level)
            for c_ in cp.values():
                c_.wait_send()
        elif stage == 3:
            def keep(r, z):
                near[1, k, :, r] = near[1, k, :, r] + z
            pull(wg, k, FAR, keep, z_copies[k].start)
            with jax.named_scope('wait_mate'):
                z_copies[k].wait_recv()

            def second_weights(i):
                r = rows_at(i)
                paths = x2own[k, r, :]
                delta = paths * (near[1, k, r, own_half] + near[0, k, r, mate_half])
                reached = paths > 0
                part[k, r, OWN] = jnp.where(reached, (lw[0] + delta) / jnp.where(reached, paths, 1.0), 0.0)
                bc[:, own_half] = bc[:, own_half] + jnp.sum(delta, axis=0, keepdims=True)
            by_rows(m, second_weights)
        else:
            pull(part, k, FAR, functools.partial(close, k))

    @scoped('other')
    def other(k, i):
        if k == 0:
            loads[0, i].wait()
        select_other(k, i)
        if (k, i) == (0, 0):
            with jax.named_scope('wait_barrier'):
                pl.semaphore_wait(barrier, 3 + 2 * (planes - 1))
        m_copies[k, i].start()

    @scoped('own')
    def own(k, i):
        if k == 0:
            loads[1, i].wait()
        select_own(k, i)

    def first_level_sends(k):
        own(k, 0)
        copies[0, k][TO_P, 0].start()
        copies[0, k][TO_Q, 0].start()
        if k == 0:
            other(0, 2)
            a_copies[0].start()
        own(k, 1)
        copies[0, k][TO_P, 1].start()
        own(k, 2)
        copies[0, k][TO_Q, 1].start()

    other(0, 0)
    first_level_sends(0)
    lax.fori_loop(m // blk, src_count // blk, one_hot_rows, 0)
    bc[...] = jnp.zeros_like(bc)
    for i in range(3):
        other(1, i)
    a_copies[1].start()
    for k in range(CHUNKS):
        other(k, 3)
    a_copies[2].start()
    middle(0, 0)
    first_level_sends(1)
    for k in range(CHUNKS):
        own(k, 3)
    middle(0, 1)
    for stage in range(1, 5):
        finish(stage - 1, 0)
        start(stage, 0)
        if stage == 4:
            nears(3, 1)
        middle(stage, 0)
        finish(stage - 1, 1)
        start(stage, 1)
        if stage >= 3:
            nears(stage, 0)
        if stage == 4:
            last_own()
        middle(stage, 1)
    finish(4, 0)
    last_nears()
    last_far(0)
    last_far(1)

    total[...] = bc[...] * scale
    keep_own = pltpu.make_async_copy(total.at[:, own_half], out.at[s_me], load_sem.at[0])
    keep_own.start()
    for o in range(planes):
        there = lax.rem(s_me + o, planes)
        for other_core in (0, 1):
            if o == 0 and not other_core:
                continue
            device = {"src": there, "graph": x * 2 + (1 - c)} if other_core else {"src": there}
            pltpu.make_async_remote_copy(src_ref=total.at[:, side[other_core]], dst_ref=out.at[other_core * planes + s_me],
                                         send_sem=plane_s, recv_sem=plane_r,
                                         device_id=device, device_id_type=MESH).start()

    for copy in a_copies + x1_copies + x2_copies + z_copies:
        copy.wait_send()
    for k in range(CHUNKS):
        for stage in (3, 4):
            for c_ in copies[stage, k].values():
                c_.wait_send()
    keep_own.wait()
    arrivals = out.at[pl.ds(0, 2 * planes - 1)]
    every = pltpu.make_async_remote_copy(src_ref=arrivals, dst_ref=arrivals, send_sem=plane_s, recv_sem=plane_r,
                                         device_id=to_mate, device_id_type=MESH)
    with jax.named_scope("wait_plane"):
        every.wait_recv()
    every.wait_send()


def solution(mesh):
    planes = mesh.shape["src"]
    ring = mesh.shape["graph"] // 2

    def device_program(adj_slab, src_local, level_weight):
        slab, vertex_count = adj_slab.shape
        src_count = src_local.shape[0]
        m = src_count // CHUNKS
        scale = vertex_count / (src_count * planes * (level_weight.shape[0] + 1) ** 3)
        wide = 4 * slab
        vmem = pltpu.VMEM
        sem = pltpu.SemaphoreType.DMA
        mates = 4 + 7 * CHUNKS
        rings = 5 * CHUNKS * 8
        flops = 2 * 9 * src_count * slab * vertex_count
        bc = pl.pallas_call(
            functools.partial(kernel, ring, planes, scale),
            out_shape=jax.ShapeDtypeStruct((2 * planes, 1, slab), f32),
            in_specs=[pl.BlockSpec(memory_space=pl.ANY), pl.BlockSpec(memory_space=vmem), pl.BlockSpec(memory_space=pltpu.SMEM)],
            out_specs=pl.BlockSpec(memory_space=pl.ANY),
            scratch_shapes=[
                vmem((2 * slab, wide), bf16), vmem((slab, wide), bf16),
                vmem((2 * src_count, wide), bf16), vmem((src_count, 1), f32), vmem((src_count, slab), bf16),
                vmem((CHUNKS, m, 2 * slab), bf16), vmem((CHUNKS, m, slab), f32), vmem((CHUNKS, m, slab), f32),
                vmem((CHUNKS, m, wide), f32), vmem((CHUNKS, m, wide), f32),
                vmem((CHUNKS, m, 2 * slab), bf16), vmem((CHUNKS, 2, m // 2, slab), bf16),
                vmem((2, CHUNKS, m, 2 * slab), f32), vmem((2, CHUNKS, 2, m // 2, slab), f32),
                vmem((1, 2 * slab), f32), vmem((1, 2 * slab), f32),
                sem((8,)), sem((rings,)), sem((rings,)), sem((mates,)), sem((mates,)), sem, sem,
            ],
            compiler_params=pltpu.CompilerParams(collective_id=0, has_side_effects=True, vmem_limit_bytes=67043328),
            cost_estimate=pl.CostEstimate(flops=flops, bytes_accessed=2 * slab * vertex_count, transcendentals=0),
        )(adj_slab, src_local.reshape(1, src_count), level_weight)
        return jnp.sum(bc, axis=(0, 1))

    return jax.shard_map(device_program, mesh=mesh,
                         in_specs=(P(("batch", "graph"), None), P(("batch", "src")), P(None)),
                         out_specs=P(("batch", "graph")), check_vma=False)
```

```python
import functools

import jax
import jax.numpy as jnp
from jax import lax
from jax.experimental import pallas as pl
from jax.experimental.pallas import tpu as pltpu
from jax.sharding import PartitionSpec as P

MESH = pl.DeviceIdType.MESH
f32, bf16 = jnp.float32, jnp.bfloat16
CHUNKS = 2
TO_P, TO_Q = 0, 1


def rows_cols(lhs, rhs):
    return lax.dot_general(lhs, rhs, (((1,), (0,)), ((), ())), preferred_element_type=f32)


def rows_rows(lhs, rhs):
    return lax.dot_general(lhs, rhs, (((1,), (1,)), ((), ())), preferred_element_type=f32)


def kernel(ring, planes, scale, adj, src, lw, out,
           a_blk, a_oth, pick, ids, onehot, x1, x2own, x2rcv, part, wg,
           near0, far0, near, far, bc, total,
           load_sem, ssem, rsem, d2d_s, d2d_r, plane_s, plane_r):
    slab = a_oth.shape[0]
    cols_all = a_oth.shape[1]
    src_count = ids.shape[0]
    m = src_count // CHUNKS
    h = m // 2
    tile = 2 * slab // 3
    blk = min(32, h)

    g = lax.axis_index("graph")
    s_me = lax.axis_index("src")
    x, c = g // 2, g % 2
    odd = lax.rem(x, 2)
    chip_p = x + 1 - 2 * odd
    chip_q = lax.rem(x + ring - 1 + 2 * odd, ring)
    chip_far = lax.rem(x + 2, ring)
    to_p = {"graph": chip_p * 2 + c}
    to_q = {"graph": chip_q * 2 + c}
    to_mate = {"graph": x * 2 + (1 - c)}
    chips = (chip_far, chip_p, chip_q, x)
    slot = [pl.ds(i * slab, slab) for i in range(4)]
    FAR, NEAR_P, NEAR_Q, OWN = slot

    loads = {}
    for i, chip in enumerate(chips):
        for own in (0, 1):
            at = pl.ds(pl.multiple_of((chip * 2 + (c if own else 1 - c)) * slab, 128), slab)
            target = a_blk.at[pl.ds(0, slab), slot[i]] if own else a_oth.at[:, slot[i]]
            loads[own, i] = pltpu.make_async_copy(adj.at[:, at], target, load_sem.at[4 * own + i])
    for own, i in ((0, 0), (1, 0), (0, 1), (0, 2), (1, 1), (1, 2), (0, 3), (1, 3)):
        loads[own, i].start()

    barrier = pltpu.get_barrier_semaphore()
    for dev in (to_p, to_q, to_mate):
        pl.semaphore_signal(barrier, inc=1, device_id=dev, device_id_type=MESH)
    for o in range(1, planes):
        there = lax.rem(s_me + o, planes)
        pl.semaphore_signal(barrier, inc=1, device_id={"src": there}, device_id_type=MESH)
        pl.semaphore_signal(barrier, inc=1, device_id={"src": there, "graph": x * 2 + (1 - c)}, device_id_type=MESH)

    row = lax.broadcasted_iota(jnp.int32, (src_count, src_count), 0)
    col = lax.broadcasted_iota(jnp.int32, (src_count, src_count), 1)
    ids[...] = jnp.sum(jnp.where(row == col, src[...].astype(f32), 0.0), axis=1, keepdims=True)
    base = g * slab
    base_f = base.astype(f32)
    chip_f = (x * 2 * slab).astype(f32)
    lane = (lax.broadcasted_iota(jnp.int32, (blk, slab), 1) + base).astype(f32)

    def one_hot_rows(i, carry):
        r = pl.ds(pl.multiple_of(i * blk, blk), blk)
        onehot[r, :] = jnp.where(ids[r, :] == lane, 1.0, 0.0).astype(bf16)
        return carry

    lax.fori_loop(0, m // blk, one_hot_rows, 0)

    def mate_copy(i, source, target):
        return pltpu.make_async_remote_copy(src_ref=source, dst_ref=target, send_sem=d2d_s.at[i], recv_sem=d2d_r.at[i],
                                            device_id=to_mate, device_id_type=MESH)

    def ring_copy(stage, k, way, msg, source, target):
        i = ((stage * CHUNKS + k) * 2 + way) * 4 + msg
        return pltpu.make_async_remote_copy(src_ref=source, dst_ref=target, send_sem=ssem.at[i], recv_sem=rsem.at[i],
                                            device_id=to_p if way == TO_P else to_q, device_id_type=MESH)

    lo, hi = pl.ds(0, h), pl.ds(h, h)
    side = [pl.ds(0, slab), pl.ds(slab, slab)]
    own_half, mate_half = side
    merged = [pick.at[pl.ds(src_count + k * m, m), :] for k in range(CHUNKS)]
    two = [pl.ds(0, 2 * slab), pl.ds(2 * slab, 2 * slab)]

    def reduce_copies(stage, k):
        if stage == 0:
            send, nr, fr = merged[k], near0.at[k], far0.at[k]
        else:
            send, nr, fr = part.at[k], near.at[stage - 1, k], far.at[stage - 1, k]
        return {
            (TO_P, 0): ring_copy(stage, k, TO_P, 0, send.at[lo, FAR], fr.at[TO_P]),
            (TO_Q, 0): ring_copy(stage, k, TO_Q, 0, send.at[hi, FAR], fr.at[TO_Q]),
            (TO_P, 1): ring_copy(stage, k, TO_P, 1, send.at[lo, NEAR_P], nr.at[lo, side[TO_P]]),
            (TO_Q, 1): ring_copy(stage, k, TO_Q, 1, send.at[hi, NEAR_Q], nr.at[hi, side[TO_Q]]),
            (TO_P, 2): ring_copy(stage, k, TO_P, 2, send.at[hi, NEAR_P], nr.at[hi, side[TO_P]]),
            (TO_Q, 2): ring_copy(stage, k, TO_Q, 2, send.at[lo, NEAR_Q], nr.at[lo, side[TO_Q]]),
        }

    tail = slab // 256 * 128
    far_parts = [(2, 0, slab - tail), (3, slab - tail, tail)]

    def gather_copies(stage, k):
        buf = wg.at[k] if stage == 3 else part.at[k]
        if (stage, k) == (4, CHUNKS - 1):
            bands = far_parts
        else:
            bands = [(2, 0, slab)]
        relay = {}
        for msg, begin, width in bands:
            from_p, from_q, to_far = [pl.ds(n * slab + begin, width) for n in (1, 2, 0)]
            relay[TO_P, msg] = ring_copy(stage, k, TO_P, msg, buf.at[hi, from_q], buf.at[hi, to_far])
            relay[TO_Q, msg] = ring_copy(stage, k, TO_Q, msg, buf.at[lo, from_p], buf.at[lo, to_far])
        return {
            **relay,
            (TO_P, 0): ring_copy(stage, k, TO_P, 0, buf.at[lo, OWN], buf.at[lo, NEAR_P]),
            (TO_Q, 0): ring_copy(stage, k, TO_Q, 0, buf.at[hi, OWN], buf.at[hi, NEAR_Q]),
            (TO_P, 1): ring_copy(stage, k, TO_P, 1, buf.at[hi, OWN], buf.at[hi, NEAR_P]),
            (TO_Q, 1): ring_copy(stage, k, TO_Q, 1, buf.at[lo, OWN], buf.at[lo, NEAR_Q]),
        }

    copies = {}
    for k in range(CHUNKS):
        for stage in range(5):
            copies[stage, k] = reduce_copies(stage, k) if stage < 3 else gather_copies(stage, k)
    a_copies = [mate_copy(i, a_oth.at[:, slot[i]], a_blk.at[pl.ds(slab, slab), slot[i]]) for i in range(4)]
    m_copies = {(k, i): mate_copy(4 + 4 * k + i, pick.at[pl.ds(k * m, m), slot[i]], merged[k].at[:, slot[i]])
                for k in range(CHUNKS) for i in range(4)}
    first = 4 + 4 * CHUNKS
    x1_copies = [mate_copy(first + k, x1.at[k, :, own_half], x1.at[k, :, mate_half]) for k in range(CHUNKS)]
    x2_copies = [mate_copy(first + CHUNKS + k, x2own.at[k], x2rcv.at[k]) for k in range(CHUNKS)]
    z_copies = [mate_copy(first + 2 * CHUNKS + k, near.at[1, k, :, mate_half], near.at[0, k, :, mate_half]) for k in range(CHUNKS)]

    def by_rows(count, fn):
        def step(i, carry):
            fn(i)
            return carry
        lax.fori_loop(0, count // blk, step, 0)

    def rows_at(i, start=0):
        return pl.ds(pl.multiple_of(start + i * blk, blk), blk)

    def by_tiles(begin, end, fn):
        def step(t, carry):
            fn(pl.ds(pl.multiple_of(t * tile, 128), tile))
            return carry
        lax.fori_loop(begin, end, step, 0)

    def select_other(k, i):
        pick[pl.ds(k * m, m), slot[i]] = rows_cols(onehot[pl.ds(k * m, m), :], a_oth[:, slot[i]]).astype(bf16)

    def select_own(k, i):
        rk = pl.ds(k * m, m)
        here = (ids[rk, :] >= base_f) & (ids[rk, :] < base_f + slab)
        if (k, i) == (0, 0):
            x1[k, :, own_half] = rows_cols(onehot[rk, :], a_blk[pl.ds(0, slab), slot[i]]).astype(bf16)
            other(0, 1)
            m_copies[k, i].wait_recv()
            mine = x1[k, :, own_half].astype(f32)
        else:
            m_copies[k, i].wait_recv()
            mine = rows_cols(onehot[rk, :], a_blk[pl.ds(0, slab), slot[i]])
        merged[k][:, slot[i]] = jnp.where(here, mine, merged[k][:, slot[i]].astype(f32)).astype(bf16)

    def send_first(stage, k):
        cp = copies[stage, k]
        cp[TO_P, 0].start()
        cp[TO_Q, 0].start()
        cp[TO_P, 1].start()

    def start(stage, k):
        cp = copies[stage, k]
        if stage in (1, 2):
            for c_ in copies[stage - 1, k].values():
                c_.wait_send()

            def push(at):
                if stage == 1:
                    part[k, :, at] = rows_cols(x1[k], a_blk[:, at])
                else:
                    both = rows_cols(pick[pl.ds(0, 2 * m), two[0]], a_blk[:, at])
                    part[k, :, at] = both[:m] + both[m:]

            def mate_rows(pair):
                if (stage, k) == (1, 0):
                    for i in pair:
                        a_copies[i].wait_recv()

            mate_rows((0, 1))
            by_tiles(0, 3, push)
            send_first(stage, k)
            mate_rows((2, 3))
            by_tiles(3, 6, push)
            cp[TO_Q, 1].start()
        else:
            for msg in (0, 1):
                cp[TO_P, msg].start()
                cp[TO_Q, msg].start()

    def middle(stage, k):
        cp = copies[stage, k]
        for way in (TO_P, TO_Q):
            cp[way, 0].wait_recv()
            begin = 0 if way == TO_P else h
            dest = NEAR_Q if way == TO_P else NEAR_P
            if stage == 0:
                def select(i):
                    r = rows_at(i, begin)
                    rk = rows_at(i, k * m + begin)
                    here = (ids[rk, :] >= chip_f) & (ids[rk, :] < chip_f + 2 * slab)
                    merged[k][r, dest] = jnp.where(here, merged[k][r, dest].astype(f32),
                                                   far0[k, way, rows_at(i), :].astype(f32)).astype(bf16)
                by_rows(h, select)
            elif stage < 3:
                def add(i):
                    r = rows_at(i, begin)
                    part[k, r, dest] = part[k, r, dest] + far[stage - 1, k, way, rows_at(i), :]
                by_rows(h, add)
            cp[1 - way, 2].start()
            if (1 - way, 3) in cp:
                cp[1 - way, 3].start()

    def pull(buf, k, at, use, meanwhile=None):
        def split(i):
            r = rows_at(i)
            full = buf[k, r, at]
            top = full.astype(bf16)
            rest = full - top.astype(f32)
            mid = rest.astype(bf16)
            pick[r, at] = top
            pick[rows_at(i, m), at] = mid
            pick[rows_at(i, 2 * m), at] = (rest - mid.astype(f32)).astype(bf16)
        by_rows(m, split)

        def product(r):
            three = rows_rows(pick[pl.ds(0, 3 * m), at], a_blk[r, at])
            use(r, three[:m] + three[m:2 * m] + three[2 * m:])
        if meanwhile is None:
            by_tiles(0, 3, product)
        else:
            by_tiles(1, 3, product)
            meanwhile()
            by_tiles(0, 1, product)

    def close(k, at, z):
        bc[:, at] = bc[:, at] + jnp.sum(x1[k, :, at].astype(f32) * z, axis=0, keepdims=True)

    def last_far(n):
        k = CHUNKS - 1
        msg, begin, width = far_parts[n]
        copies[4, k][TO_P, msg].wait_recv()
        copies[4, k][TO_Q, msg].wait_recv()
        pull(part, k, pl.ds(begin, width), functools.partial(close, k))

    def last_own():
        pull(part, CHUNKS - 1, OWN, functools.partial(close, CHUNKS - 1))

    def last_nears():
        k = CHUNKS - 1
        copies[4, k][TO_P, 1].wait_recv()
        copies[4, k][TO_Q, 1].wait_recv()
        pull(part, k, pl.ds(slab, 2 * slab), functools.partial(close, k))

    def nears(stage, k):
        cp = copies[stage, k]
        cp[TO_P, 1].wait_recv()
        cp[TO_Q, 1].wait_recv()

        def keep(r, z):
            if stage == 3:
                near[1, k, :, r] = z
            else:
                close(k, r, z)
        pull(wg if stage == 3 else part, k, pl.ds(slab, 3 * slab), keep)

    def finish(stage, k):
        cp = copies[stage, k]
        for way in (TO_P, TO_Q):
            if stage < 3:
                cp[way, 1].wait_recv()
            cp[way, 2].wait_recv()
        if stage == 0:
            def first_level(i):
                r = rows_at(i)
                x1[k, r, own_half] = (merged[k][r, OWN].astype(f32) + near0[k, r, side[0]].astype(f32)
                                      + near0[k, r, side[1]].astype(f32)).astype(bf16)
            by_rows(m, first_level)
            x1_copies[k].start()
            if k == 0:
                a_copies[2].start()
                a_copies[3].start()
                for copy in m_copies.values():
                    copy.wait_send()
            x1_copies[k].wait_recv()
        elif stage == 1:
            def second_level(i):
                r = rows_at(i)
                rk = rows_at(i, k * m)
                total = part[k, r, OWN] + near[0, k, r, side[0]] + near[0, k, r, side[1]]
                seen = jnp.maximum(onehot[rk, :].astype(f32), x1[k, r, own_half].astype(f32))
                x2own[k, r, :] = total * (1.0 - seen)
            by_rows(m, second_level)
            x2_copies[k].start()

            def split(i, source, half):
                r = rows_at(i)
                full = source[k, r, :]
                top = full.astype(bf16)
                pick[r, half] = top
                pick[rows_at(i, m), half] = (full - top.astype(f32)).astype(bf16)
            by_rows(m, lambda i: split(i, x2own, own_half))
            x2_copies[k].wait_recv()
            by_rows(m, lambda i: split(i, x2rcv, mate_half))
        elif stage == 2:
            def third_level(i):
                r = rows_at(i)
                rk = rows_at(i, k * m)
                total = part[k, r, OWN] + near[1, k, r, side[0]] + near[1, k, r, side[1]]
                seen = jnp.maximum(onehot[rk, :].astype(f32), x1[k, r, own_half].astype(f32))
                seen = jnp.maximum(seen, jnp.where(x2own[k, r, :] > 0, 1.0, 0.0))
                paths = total * (1.0 - seen)
                reached = paths > 0
                wg[k, r, OWN] = jnp.where(reached, lw[1] / jnp.where(reached, paths, 1.0), 0.0)
            by_rows(m, third_level)
            for c_ in cp.values():
                c_.wait_send()
        elif stage == 3:
            def keep(r, z):
                near[1, k, :, r] = near[1, k, :, r] + z
            pull(wg, k, FAR, keep, z_copies[k].start)
            z_copies[k].wait_recv()

            def second_weights(i):
                r = rows_at(i)
                paths = x2own[k, r, :]
                delta = paths * (near[1, k, r, own_half] + near[0, k, r, mate_half])
                reached = paths > 0
                part[k, r, OWN] = jnp.where(reached, (lw[0] + delta) / jnp.where(reached, paths, 1.0), 0.0)
                bc[:, own_half] = bc[:, own_half] + jnp.sum(delta, axis=0, keepdims=True)
            by_rows(m, second_weights)
        else:
            pull(part, k, FAR, functools.partial(close, k))

    def other(k, i):
        if k == 0:
            loads[0, i].wait()
        select_other(k, i)
        if (k, i) == (0, 0):
            pl.semaphore_wait(barrier, 3 + 2 * (planes - 1))
        m_copies[k, i].start()

    def own(k, i):
        if k == 0:
            loads[1, i].wait()
        select_own(k, i)

    def first_level_sends(k):
        own(k, 0)
        copies[0, k][TO_P, 0].start()
        copies[0, k][TO_Q, 0].start()
        if k == 0:
            other(0, 2)
            a_copies[0].start()
        own(k, 1)
        copies[0, k][TO_P, 1].start()
        own(k, 2)
        copies[0, k][TO_Q, 1].start()

    other(0, 0)
    first_level_sends(0)
    lax.fori_loop(m // blk, src_count // blk, one_hot_rows, 0)
    bc[...] = jnp.zeros_like(bc)
    for i in range(3):
        other(1, i)
    a_copies[1].start()
    for k in range(CHUNKS):
        other(k, 3)
    middle(0, 0)
    first_level_sends(1)
    for k in range(CHUNKS):
        own(k, 3)
    middle(0, 1)
    for stage in range(1, 5):
        finish(stage - 1, 0)
        start(stage, 0)
        if stage == 4:
            nears(3, 1)
        middle(stage, 0)
        finish(stage - 1, 1)
        start(stage, 1)
        if stage >= 3:
            nears(stage, 0)
        if stage == 4:
            last_own()
        middle(stage, 1)
    finish(4, 0)
    last_nears()
    last_far(0)
    last_far(1)

    total[...] = bc[...] * scale
    keep_own = pltpu.make_async_copy(total.at[:, own_half], out.at[s_me], load_sem.at[0])
    keep_own.start()
    for o in range(planes):
        there = lax.rem(s_me + o, planes)
        for other_core in (0, 1):
            if o == 0 and not other_core:
                continue
            device = {"src": there, "graph": x * 2 + (1 - c)} if other_core else {"src": there}
            pltpu.make_async_remote_copy(src_ref=total.at[:, side[other_core]], dst_ref=out.at[other_core * planes + s_me],
                                         send_sem=plane_s, recv_sem=plane_r,
                                         device_id=device, device_id_type=MESH).start()

    for copy in a_copies + x1_copies + x2_copies + z_copies:
        copy.wait_send()
    for k in range(CHUNKS):
        for stage in (3, 4):
            for c_ in copies[stage, k].values():
                c_.wait_send()
    keep_own.wait()
    arrivals = out.at[pl.ds(0, 2 * planes - 1)]
    every = pltpu.make_async_remote_copy(src_ref=arrivals, dst_ref=arrivals, send_sem=plane_s, recv_sem=plane_r,
                                         device_id=to_mate, device_id_type=MESH)
    every.wait_recv()
    every.wait_send()


def solution(mesh):
    planes = mesh.shape["src"]
    ring = mesh.shape["graph"] // 2

    def device_program(adj_slab, src_local, level_weight):
        slab, vertex_count = adj_slab.shape
        src_count = src_local.shape[0]
        m = src_count // CHUNKS
        scale = vertex_count / (src_count * planes * (level_weight.shape[0] + 1) ** 3)
        wide = 4 * slab
        vmem = pltpu.VMEM
        sem = pltpu.SemaphoreType.DMA
        mates = 4 + 7 * CHUNKS
        rings = 5 * CHUNKS * 8
        flops = 2 * 9 * src_count * slab * vertex_count
        bc = pl.pallas_call(
            functools.partial(kernel, ring, planes, scale),
            out_shape=jax.ShapeDtypeStruct((2 * planes, 1, slab), f32),
            in_specs=[pl.BlockSpec(memory_space=pl.ANY), pl.BlockSpec(memory_space=vmem), pl.BlockSpec(memory_space=pltpu.SMEM)],
            out_specs=pl.BlockSpec(memory_space=pl.ANY),
            scratch_shapes=[
                vmem((2 * slab, wide), bf16), vmem((slab, wide), bf16),
                vmem((2 * src_count, wide), bf16), vmem((src_count, 1), f32), vmem((src_count, slab), bf16),
                vmem((CHUNKS, m, 2 * slab), bf16), vmem((CHUNKS, m, slab), f32), vmem((CHUNKS, m, slab), f32),
                vmem((CHUNKS, m, wide), f32), vmem((CHUNKS, m, wide), f32),
                vmem((CHUNKS, m, 2 * slab), bf16), vmem((CHUNKS, 2, m // 2, slab), bf16),
                vmem((2, CHUNKS, m, 2 * slab), f32), vmem((2, CHUNKS, 2, m // 2, slab), f32),
                vmem((1, 2 * slab), f32), vmem((1, 2 * slab), f32),
                sem((8,)), sem((rings,)), sem((rings,)), sem((mates,)), sem((mates,)), sem, sem,
            ],
            compiler_params=pltpu.CompilerParams(collective_id=0, has_side_effects=True, vmem_limit_bytes=67043328),
            cost_estimate=pl.CostEstimate(flops=flops, bytes_accessed=2 * slab * vertex_count, transcendentals=0),
        )(adj_slab, src_local.reshape(1, src_count), level_weight)
        return jnp.sum(bc, axis=(0, 1))

    return jax.shard_map(device_program, mesh=mesh,
                         in_specs=(P(("batch", "graph"), None), P(("batch", "src")), P(None)),
                         out_specs=P(("batch", "graph")), check_vma=False)
```

```python
import functools

import jax
import jax.numpy as jnp
from jax import lax
from jax.experimental import pallas as pl
from jax.experimental.pallas import tpu as pltpu
from jax.sharding import PartitionSpec as P

MESH = pl.DeviceIdType.MESH
f32, bf16 = jnp.float32, jnp.bfloat16
CHUNKS = 2
TO_P, TO_Q = 0, 1


def rows_cols(lhs, rhs):
    return lax.dot_general(lhs, rhs, (((1,), (0,)), ((), ())), preferred_element_type=f32)


def rows_rows(lhs, rhs):
    return lax.dot_general(lhs, rhs, (((1,), (1,)), ((), ())), preferred_element_type=f32)


def kernel(ring, planes, scale, adj, src, lw, out,
           a_blk, a_oth, pick, ids, onehot, x1, x2own, x2rcv, part, wg,
           near0, far0, near, far, bc, total,
           load_sem, ssem, rsem, d2d_s, d2d_r, plane_s, plane_r):
    slab = a_oth.shape[0]
    cols_all = a_oth.shape[1]
    src_count = ids.shape[0]
    m = src_count // CHUNKS
    h = m // 2
    tile = 2 * slab // 3
    blk = min(32, h)

    g = lax.axis_index("graph")
    s_me = lax.axis_index("src")
    x, c = g // 2, g % 2
    odd = lax.rem(x, 2)
    chip_p = x + 1 - 2 * odd
    chip_q = lax.rem(x + ring - 1 + 2 * odd, ring)
    chip_far = lax.rem(x + 2, ring)
    to_p = {"graph": chip_p * 2 + c}
    to_q = {"graph": chip_q * 2 + c}
    to_mate = {"graph": x * 2 + (1 - c)}
    chips = (chip_far, chip_p, chip_q, x)
    slot = [pl.ds(i * slab, slab) for i in range(4)]
    FAR, NEAR_P, NEAR_Q, OWN = slot

    loads = {}
    for i, chip in enumerate(chips):
        for own in (0, 1):
            at = pl.ds(pl.multiple_of((chip * 2 + (c if own else 1 - c)) * slab, 128), slab)
            target = a_blk.at[pl.ds(0, slab), slot[i]] if own else a_oth.at[:, slot[i]]
            loads[own, i] = pltpu.make_async_copy(adj.at[:, at], target, load_sem.at[4 * own + i])
    load_order = ((0, 0), (1, 0), (0, 1), (0, 2), (1, 1), (1, 2), (0, 3), (1, 3))
    for at in load_order[:2]:
        loads[at].start()

    barrier = pltpu.get_barrier_semaphore()
    for dev in (to_p, to_q, to_mate):
        pl.semaphore_signal(barrier, inc=1, device_id=dev, device_id_type=MESH)
    for o in range(1, planes):
        there = lax.rem(s_me + o, planes)
        pl.semaphore_signal(barrier, inc=1, device_id={"src": there}, device_id_type=MESH)
        pl.semaphore_signal(barrier, inc=1, device_id={"src": there, "graph": x * 2 + (1 - c)}, device_id_type=MESH)

    row = lax.broadcasted_iota(jnp.int32, (src_count, src_count), 0)
    col = lax.broadcasted_iota(jnp.int32, (src_count, src_count), 1)
    ids[...] = jnp.sum(jnp.where(row == col, src[...].astype(f32), 0.0), axis=1, keepdims=True)
    base = g * slab
    base_f = base.astype(f32)
    chip_f = (x * 2 * slab).astype(f32)
    lane = (lax.broadcasted_iota(jnp.int32, (blk, slab), 1) + base).astype(f32)

    def one_hot_rows(i, carry):
        r = pl.ds(pl.multiple_of(i * blk, blk), blk)
        onehot[r, :] = jnp.where(ids[r, :] == lane, 1.0, 0.0).astype(bf16)
        return carry

    lax.fori_loop(0, m // blk, one_hot_rows, 0)

    def mate_copy(i, source, target):
        return pltpu.make_async_remote_copy(src_ref=source, dst_ref=target, send_sem=d2d_s.at[i], recv_sem=d2d_r.at[i],
                                            device_id=to_mate, device_id_type=MESH)

    def ring_copy(stage, k, way, msg, source, target):
        i = ((stage * CHUNKS + k) * 2 + way) * 4 + msg
        return pltpu.make_async_remote_copy(src_ref=source, dst_ref=target, send_sem=ssem.at[i], recv_sem=rsem.at[i],
                                            device_id=to_p if way == TO_P else to_q, device_id_type=MESH)

    lo, hi = pl.ds(0, h), pl.ds(h, h)
    side = [pl.ds(0, slab), pl.ds(slab, slab)]
    own_half, mate_half = side
    merged = [pick.at[pl.ds(src_count + k * m, m), :] for k in range(CHUNKS)]
    two = [pl.ds(0, 2 * slab), pl.ds(2 * slab, 2 * slab)]

    def reduce_copies(stage, k):
        if stage == 0:
            send, nr, fr = merged[k], near0.at[k], far0.at[k]
        else:
            send, nr, fr = part.at[k], near.at[stage - 1, k], far.at[stage - 1, k]
        return {
            (TO_P, 0): ring_copy(stage, k, TO_P, 0, send.at[lo, FAR], fr.at[TO_P]),
            (TO_Q, 0): ring_copy(stage, k, TO_Q, 0, send.at[hi, FAR], fr.at[TO_Q]),
            (TO_P, 1): ring_copy(stage, k, TO_P, 1, send.at[lo, NEAR_P], nr.at[lo, side[TO_P]]),
            (TO_Q, 1): ring_copy(stage, k, TO_Q, 1, send.at[hi, NEAR_Q], nr.at[hi, side[TO_Q]]),
            (TO_P, 2): ring_copy(stage, k, TO_P, 2, send.at[hi, NEAR_P], nr.at[hi, side[TO_P]]),
            (TO_Q, 2): ring_copy(stage, k, TO_Q, 2, send.at[lo, NEAR_Q], nr.at[lo, side[TO_Q]]),
        }

    tail = slab // 256 * 128
    far_parts = [(2, 0, slab - tail), (3, slab - tail, tail)]

    def gather_copies(stage, k):
        buf = wg.at[k] if stage == 3 else part.at[k]
        if (stage, k) == (4, CHUNKS - 1):
            bands = far_parts
        else:
            bands = [(2, 0, slab)]
        relay = {}
        for msg, begin, width in bands:
            from_p, from_q, to_far = [pl.ds(n * slab + begin, width) for n in (1, 2, 0)]
            relay[TO_P, msg] = ring_copy(stage, k, TO_P, msg, buf.at[hi, from_q], buf.at[hi, to_far])
            relay[TO_Q, msg] = ring_copy(stage, k, TO_Q, msg, buf.at[lo, from_p], buf.at[lo, to_far])
        return {
            **relay,
            (TO_P, 0): ring_copy(stage, k, TO_P, 0, buf.at[lo, OWN], buf.at[lo, NEAR_P]),
            (TO_Q, 0): ring_copy(stage, k, TO_Q, 0, buf.at[hi, OWN], buf.at[hi, NEAR_Q]),
            (TO_P, 1): ring_copy(stage, k, TO_P, 1, buf.at[hi, OWN], buf.at[hi, NEAR_P]),
            (TO_Q, 1): ring_copy(stage, k, TO_Q, 1, buf.at[lo, OWN], buf.at[lo, NEAR_Q]),
        }

    copies = {}
    for k in range(CHUNKS):
        for stage in range(5):
            copies[stage, k] = reduce_copies(stage, k) if stage < 3 else gather_copies(stage, k)
    a_copies = [mate_copy(i, a_oth.at[:, slot[i]], a_blk.at[pl.ds(slab, slab), slot[i]]) for i in range(4)]
    m_copies = {(k, i): mate_copy(4 + 4 * k + i, pick.at[pl.ds(k * m, m), slot[i]], merged[k].at[:, slot[i]])
                for k in range(CHUNKS) for i in range(4)}
    first = 4 + 4 * CHUNKS
    x1_copies = [mate_copy(first + k, x1.at[k, :, own_half], x1.at[k, :, mate_half]) for k in range(CHUNKS)]
    x2_copies = [mate_copy(first + CHUNKS + k, x2own.at[k], x2rcv.at[k]) for k in range(CHUNKS)]
    z_copies = [mate_copy(first + 2 * CHUNKS + k, near.at[1, k, :, mate_half], near.at[0, k, :, mate_half]) for k in range(CHUNKS)]

    def by_rows(count, fn):
        def step(i, carry):
            fn(i)
            return carry
        lax.fori_loop(0, count // blk, step, 0)

    def rows_at(i, start=0):
        return pl.ds(pl.multiple_of(start + i * blk, blk), blk)

    def by_tiles(begin, end, fn):
        def step(t, carry):
            fn(pl.ds(pl.multiple_of(t * tile, 128), tile))
            return carry
        lax.fori_loop(begin, end, step, 0)

    def select_other(k, i):
        pick[pl.ds(k * m, m), slot[i]] = rows_cols(onehot[pl.ds(k * m, m), :], a_oth[:, slot[i]]).astype(bf16)

    def select_own(k, i):
        rk = pl.ds(k * m, m)
        here = (ids[rk, :] >= base_f) & (ids[rk, :] < base_f + slab)
        if (k, i) == (0, 0):
            x1[k, :, own_half] = rows_cols(onehot[rk, :], a_blk[pl.ds(0, slab), slot[i]]).astype(bf16)
            other(0, 1)
            m_copies[k, i].wait_recv()
            mine = x1[k, :, own_half].astype(f32)
        else:
            m_copies[k, i].wait_recv()
            mine = rows_cols(onehot[rk, :], a_blk[pl.ds(0, slab), slot[i]])
        merged[k][:, slot[i]] = jnp.where(here, mine, merged[k][:, slot[i]].astype(f32)).astype(bf16)

    def send_first(stage, k):
        cp = copies[stage, k]
        cp[TO_P, 0].start()
        cp[TO_Q, 0].start()
        cp[TO_P, 1].start()

    def start(stage, k):
        cp = copies[stage, k]
        if stage in (1, 2):
            for c_ in copies[stage - 1, k].values():
                c_.wait_send()

            def push(at):
                if stage == 1:
                    part[k, :, at] = rows_cols(x1[k], a_blk[:, at])
                else:
                    both = rows_cols(pick[pl.ds(0, 2 * m), two[0]], a_blk[:, at])
                    part[k, :, at] = both[:m] + both[m:]

            def mate_rows(pair):
                if (stage, k) == (1, 0):
                    for i in pair:
                        a_copies[i].wait_recv()

            mate_rows((0, 1))
            by_tiles(0, 3, push)
            send_first(stage, k)
            mate_rows((2, 3))
            by_tiles(3, 6, push)
            cp[TO_Q, 1].start()
        else:
            for msg in (0, 1):
                cp[TO_P, msg].start()
                cp[TO_Q, msg].start()

    def middle(stage, k):
        cp = copies[stage, k]
        for way in (TO_P, TO_Q):
            cp[way, 0].wait_recv()
            begin = 0 if way == TO_P else h
            dest = NEAR_Q if way == TO_P else NEAR_P
            if stage == 0:
                def select(i):
                    r = rows_at(i, begin)
                    rk = rows_at(i, k * m + begin)
                    here = (ids[rk, :] >= chip_f) & (ids[rk, :] < chip_f + 2 * slab)
                    merged[k][r, dest] = jnp.where(here, merged[k][r, dest].astype(f32),
                                                   far0[k, way, rows_at(i), :].astype(f32)).astype(bf16)
                by_rows(h, select)
            elif stage < 3:
                def add(i):
                    r = rows_at(i, begin)
                    part[k, r, dest] = part[k, r, dest] + far[stage - 1, k, way, rows_at(i), :]
                by_rows(h, add)
            cp[1 - way, 2].start()
            if (1 - way, 3) in cp:
                cp[1 - way, 3].start()

    def pull(buf, k, at, use, meanwhile=None):
        def split(i):
            r = rows_at(i)
            full = buf[k, r, at]
            top = full.astype(bf16)
            rest = full - top.astype(f32)
            mid = rest.astype(bf16)
            pick[r, at] = top
            pick[rows_at(i, m), at] = mid
            pick[rows_at(i, 2 * m), at] = (rest - mid.astype(f32)).astype(bf16)
        by_rows(m, split)

        def product(r):
            three = rows_rows(pick[pl.ds(0, 3 * m), at], a_blk[r, at])
            use(r, three[:m] + three[m:2 * m] + three[2 * m:])
        if meanwhile is None:
            by_tiles(0, 3, product)
        else:
            by_tiles(1, 3, product)
            meanwhile()
            by_tiles(0, 1, product)

    def close(k, at, z):
        bc[:, at] = bc[:, at] + jnp.sum(x1[k, :, at].astype(f32) * z, axis=0, keepdims=True)

    def last_far(n):
        k = CHUNKS - 1
        msg, begin, width = far_parts[n]
        copies[4, k][TO_P, msg].wait_recv()
        copies[4, k][TO_Q, msg].wait_recv()
        pull(part, k, pl.ds(begin, width), functools.partial(close, k))

    def last_own():
        pull(part, CHUNKS - 1, OWN, functools.partial(close, CHUNKS - 1))

    def last_nears():
        k = CHUNKS - 1
        copies[4, k][TO_P, 1].wait_recv()
        copies[4, k][TO_Q, 1].wait_recv()
        pull(part, k, pl.ds(slab, 2 * slab), functools.partial(close, k))

    def nears(stage, k):
        cp = copies[stage, k]
        cp[TO_P, 1].wait_recv()
        cp[TO_Q, 1].wait_recv()

        def keep(r, z):
            if stage == 3:
                near[1, k, :, r] = z
            else:
                close(k, r, z)
        pull(wg if stage == 3 else part, k, pl.ds(slab, 3 * slab), keep)

    def finish(stage, k):
        cp = copies[stage, k]
        for way in (TO_P, TO_Q):
            if stage < 3:
                cp[way, 1].wait_recv()
            cp[way, 2].wait_recv()
        if stage == 0:
            def first_level(i):
                r = rows_at(i)
                x1[k, r, own_half] = (merged[k][r, OWN].astype(f32) + near0[k, r, side[0]].astype(f32)
                                      + near0[k, r, side[1]].astype(f32)).astype(bf16)
            by_rows(m, first_level)
            x1_copies[k].start()
            if k == 0:
                a_copies[3].start()
                for copy in m_copies.values():
                    copy.wait_send()
            x1_copies[k].wait_recv()
        elif stage == 1:
            def second_level(i):
                r = rows_at(i)
                rk = rows_at(i, k * m)
                total = part[k, r, OWN] + near[0, k, r, side[0]] + near[0, k, r, side[1]]
                seen = jnp.maximum(onehot[rk, :].astype(f32), x1[k, r, own_half].astype(f32))
                x2own[k, r, :] = total * (1.0 - seen)
            by_rows(m, second_level)
            x2_copies[k].start()

            def split(i, source, half):
                r = rows_at(i)
                full = source[k, r, :]
                top = full.astype(bf16)
                pick[r, half] = top
                pick[rows_at(i, m), half] = (full - top.astype(f32)).astype(bf16)
            by_rows(m, lambda i: split(i, x2own, own_half))
            x2_copies[k].wait_recv()
            by_rows(m, lambda i: split(i, x2rcv, mate_half))
        elif stage == 2:
            def third_level(i):
                r = rows_at(i)
                rk = rows_at(i, k * m)
                total = part[k, r, OWN] + near[1, k, r, side[0]] + near[1, k, r, side[1]]
                seen = jnp.maximum(onehot[rk, :].astype(f32), x1[k, r, own_half].astype(f32))
                seen = jnp.maximum(seen, jnp.where(x2own[k, r, :] > 0, 1.0, 0.0))
                paths = total * (1.0 - seen)
                reached = paths > 0
                wg[k, r, OWN] = jnp.where(reached, lw[1] / jnp.where(reached, paths, 1.0), 0.0)
            by_rows(m, third_level)
            for c_ in cp.values():
                c_.wait_send()
        elif stage == 3:
            def keep(r, z):
                near[1, k, :, r] = near[1, k, :, r] + z
            pull(wg, k, FAR, keep, z_copies[k].start)
            z_copies[k].wait_recv()

            def second_weights(i):
                r = rows_at(i)
                paths = x2own[k, r, :]
                delta = paths * (near[1, k, r, own_half] + near[0, k, r, mate_half])
                reached = paths > 0
                part[k, r, OWN] = jnp.where(reached, (lw[0] + delta) / jnp.where(reached, paths, 1.0), 0.0)
                bc[:, own_half] = bc[:, own_half] + jnp.sum(delta, axis=0, keepdims=True)
            by_rows(m, second_weights)
        else:
            pull(part, k, FAR, functools.partial(close, k))

    def other(k, i):
        if k == 0:
            loads[0, i].wait()
        if (k, i) == (0, 0):
            for at in load_order[2:]:
                loads[at].start()
        select_other(k, i)
        if (k, i) == (0, 0):
            pl.semaphore_wait(barrier, 3 + 2 * (planes - 1))
        m_copies[k, i].start()

    def own(k, i):
        if k == 0:
            loads[1, i].wait()
        select_own(k, i)

    def first_level_sends(k):
        own(k, 0)
        copies[0, k][TO_P, 0].start()
        copies[0, k][TO_Q, 0].start()
        if k == 0:
            other(0, 2)
            a_copies[0].start()
        own(k, 1)
        copies[0, k][TO_P, 1].start()
        own(k, 2)
        copies[0, k][TO_Q, 1].start()

    other(0, 0)
    first_level_sends(0)
    lax.fori_loop(m // blk, src_count // blk, one_hot_rows, 0)
    bc[...] = jnp.zeros_like(bc)
    for i in range(3):
        other(1, i)
    a_copies[1].start()
    for k in range(CHUNKS):
        other(k, 3)
    a_copies[2].start()
    middle(0, 0)
    first_level_sends(1)
    for k in range(CHUNKS):
        own(k, 3)
    middle(0, 1)
    for stage in range(1, 5):
        finish(stage - 1, 0)
        start(stage, 0)
        if stage == 4:
            nears(3, 1)
        middle(stage, 0)
        finish(stage - 1, 1)
        start(stage, 1)
        if stage >= 3:
            nears(stage, 0)
        if stage == 4:
            last_own()
        middle(stage, 1)
    finish(4, 0)
    last_nears()
    last_far(0)
    last_far(1)

    total[...] = bc[...] * scale
    keep_own = pltpu.make_async_copy(total.at[:, own_half], out.at[s_me], load_sem.at[0])
    keep_own.start()
    for o in range(planes):
        there = lax.rem(s_me + o, planes)
        for other_core in (0, 1):
            if o == 0 and not other_core:
                continue
            device = {"src": there, "graph": x * 2 + (1 - c)} if other_core else {"src": there}
            pltpu.make_async_remote_copy(src_ref=total.at[:, side[other_core]], dst_ref=out.at[other_core * planes + s_me],
                                         send_sem=plane_s, recv_sem=plane_r,
                                         device_id=device, device_id_type=MESH).start()

    for copy in a_copies + x1_copies + x2_copies + z_copies:
        copy.wait_send()
    for k in range(CHUNKS):
        for stage in (3, 4):
            for c_ in copies[stage, k].values():
                c_.wait_send()
    keep_own.wait()
    arrivals = out.at[pl.ds(0, 2 * planes - 1)]
    every = pltpu.make_async_remote_copy(src_ref=arrivals, dst_ref=arrivals, send_sem=plane_s, recv_sem=plane_r,
                                         device_id=to_mate, device_id_type=MESH)
    every.wait_recv()
    every.wait_send()


def solution(mesh):
    planes = mesh.shape["src"]
    ring = mesh.shape["graph"] // 2

    def device_program(adj_slab, src_local, level_weight):
        slab, vertex_count = adj_slab.shape
        src_count = src_local.shape[0]
        m = src_count // CHUNKS
        scale = vertex_count / (src_count * planes * (level_weight.shape[0] + 1) ** 3)
        wide = 4 * slab
        vmem = pltpu.VMEM
        sem = pltpu.SemaphoreType.DMA
        mates = 4 + 7 * CHUNKS
        rings = 5 * CHUNKS * 8
        flops = 2 * 9 * src_count * slab * vertex_count
        bc = pl.pallas_call(
            functools.partial(kernel, ring, planes, scale),
            out_shape=jax.ShapeDtypeStruct((2 * planes, 1, slab), f32),
            in_specs=[pl.BlockSpec(memory_space=pl.ANY), pl.BlockSpec(memory_space=vmem), pl.BlockSpec(memory_space=pltpu.SMEM)],
            out_specs=pl.BlockSpec(memory_space=pl.ANY),
            scratch_shapes=[
                vmem((2 * slab, wide), bf16), vmem((slab, wide), bf16),
                vmem((2 * src_count, wide), bf16), vmem((src_count, 1), f32), vmem((src_count, slab), bf16),
                vmem((CHUNKS, m, 2 * slab), bf16), vmem((CHUNKS, m, slab), f32), vmem((CHUNKS, m, slab), f32),
                vmem((CHUNKS, m, wide), f32), vmem((CHUNKS, m, wide), f32),
                vmem((CHUNKS, m, 2 * slab), bf16), vmem((CHUNKS, 2, m // 2, slab), bf16),
                vmem((2, CHUNKS, m, 2 * slab), f32), vmem((2, CHUNKS, 2, m // 2, slab), f32),
                vmem((1, 2 * slab), f32), vmem((1, 2 * slab), f32),
                sem((8,)), sem((rings,)), sem((rings,)), sem((mates,)), sem((mates,)), sem, sem,
            ],
            compiler_params=pltpu.CompilerParams(collective_id=0, has_side_effects=True, vmem_limit_bytes=67043328),
            cost_estimate=pl.CostEstimate(flops=flops, bytes_accessed=2 * slab * vertex_count, transcendentals=0),
        )(adj_slab, src_local.reshape(1, src_count), level_weight)
        return jnp.sum(bc, axis=(0, 1))

    return jax.shard_map(device_program, mesh=mesh,
                         in_specs=(P(("batch", "graph"), None), P(("batch", "src")), P(None)),
                         out_specs=P(("batch", "graph")), check_vma=False)
```

```python
import functools

import jax
import jax.numpy as jnp
from jax import lax
from jax.experimental import pallas as pl
from jax.experimental.pallas import tpu as pltpu
from jax.sharding import PartitionSpec as P

MESH = pl.DeviceIdType.MESH
f32, bf16 = jnp.float32, jnp.bfloat16
CHUNKS = 2
TO_P, TO_Q = 0, 1


def rows_cols(lhs, rhs):
    return lax.dot_general(lhs, rhs, (((1,), (0,)), ((), ())), preferred_element_type=f32)


def rows_rows(lhs, rhs):
    return lax.dot_general(lhs, rhs, (((1,), (1,)), ((), ())), preferred_element_type=f32)


def kernel(ring, planes, scale, adj, src, lw, out,
           a_blk, a_oth, pick, ids, onehot, x1, x2own, x2rcv, part, wg,
           near0, far0, near, far, bc, total,
           load_sem, ssem, rsem, d2d_s, d2d_r, plane_s, plane_r):
    slab = a_oth.shape[0]
    cols_all = a_oth.shape[1]
    src_count = ids.shape[0]
    m = src_count // CHUNKS
    h = m // 2
    tile = 2 * slab // 3
    blk = min(32, h)

    g = lax.axis_index("graph")
    s_me = lax.axis_index("src")
    x, c = g // 2, g % 2
    odd = lax.rem(x, 2)
    chip_p = x + 1 - 2 * odd
    chip_q = lax.rem(x + ring - 1 + 2 * odd, ring)
    chip_far = lax.rem(x + 2, ring)
    to_p = {"graph": chip_p * 2 + c}
    to_q = {"graph": chip_q * 2 + c}
    to_mate = {"graph": x * 2 + (1 - c)}
    chips = (chip_far, chip_p, chip_q, x)
    slot = [pl.ds(i * slab, slab) for i in range(4)]
    FAR, NEAR_P, NEAR_Q, OWN = slot

    loads = {}
    for i, chip in enumerate(chips):
        for own in (0, 1):
            at = pl.ds(pl.multiple_of((chip * 2 + (c if own else 1 - c)) * slab, 128), slab)
            target = a_blk.at[pl.ds(0, slab), slot[i]] if own else a_oth.at[:, slot[i]]
            loads[own, i] = pltpu.make_async_copy(adj.at[:, at], target, load_sem.at[4 * own + i])
    load_order = ((0, 0), (1, 0), (0, 1), (0, 2), (1, 1), (1, 2), (0, 3), (1, 3))
    for at in load_order[:2]:
        loads[at].start()

    barrier = pltpu.get_barrier_semaphore()
    for o in sorted(range(1, planes), key=lambda o: abs(o - planes // 2)):
        there = lax.rem(s_me + o, planes)
        pl.semaphore_signal(barrier, inc=1, device_id={"src": there}, device_id_type=MESH)
        pl.semaphore_signal(barrier, inc=1, device_id={"src": there, "graph": x * 2 + (1 - c)}, device_id_type=MESH)

    for dev in (to_p, to_q, to_mate):
        pl.semaphore_signal(barrier, inc=1, device_id=dev, device_id_type=MESH)

    row = lax.broadcasted_iota(jnp.int32, (src_count, src_count), 0)
    col = lax.broadcasted_iota(jnp.int32, (src_count, src_count), 1)
    ids[...] = jnp.sum(jnp.where(row == col, src[...].astype(f32), 0.0), axis=1, keepdims=True)
    base = g * slab
    base_f = base.astype(f32)
    chip_f = (x * 2 * slab).astype(f32)
    lane = (lax.broadcasted_iota(jnp.int32, (blk, slab), 1) + base).astype(f32)

    def one_hot_rows(i, carry):
        r = pl.ds(pl.multiple_of(i * blk, blk), blk)
        onehot[r, :] = jnp.where(ids[r, :] == lane, 1.0, 0.0).astype(bf16)
        return carry

    lax.fori_loop(0, m // blk, one_hot_rows, 0)

    def mate_copy(i, source, target):
        return pltpu.make_async_remote_copy(src_ref=source, dst_ref=target, send_sem=d2d_s.at[i], recv_sem=d2d_r.at[i],
                                            device_id=to_mate, device_id_type=MESH)

    def ring_copy(stage, k, way, msg, source, target):
        i = ((stage * CHUNKS + k) * 2 + way) * 4 + msg
        return pltpu.make_async_remote_copy(src_ref=source, dst_ref=target, send_sem=ssem.at[i], recv_sem=rsem.at[i],
                                            device_id=to_p if way == TO_P else to_q, device_id_type=MESH)

    lo, hi = pl.ds(0, h), pl.ds(h, h)
    side = [pl.ds(0, slab), pl.ds(slab, slab)]
    own_half, mate_half = side
    merged = [pick.at[pl.ds(src_count + k * m, m), :] for k in range(CHUNKS)]
    two = [pl.ds(0, 2 * slab), pl.ds(2 * slab, 2 * slab)]

    def reduce_copies(stage, k):
        if stage == 0:
            send, nr, fr = merged[k], near0.at[k], far0.at[k]
        else:
            send, nr, fr = part.at[k], near.at[stage - 1, k], far.at[stage - 1, k]
        return {
            (TO_P, 0): ring_copy(stage, k, TO_P, 0, send.at[lo, FAR], fr.at[TO_P]),
            (TO_Q, 0): ring_copy(stage, k, TO_Q, 0, send.at[hi, FAR], fr.at[TO_Q]),
            (TO_P, 1): ring_copy(stage, k, TO_P, 1, send.at[lo, NEAR_P], nr.at[lo, side[TO_P]]),
            (TO_Q, 1): ring_copy(stage, k, TO_Q, 1, send.at[hi, NEAR_Q], nr.at[hi, side[TO_Q]]),
            (TO_P, 2): ring_copy(stage, k, TO_P, 2, send.at[hi, NEAR_P], nr.at[hi, side[TO_P]]),
            (TO_Q, 2): ring_copy(stage, k, TO_Q, 2, send.at[lo, NEAR_Q], nr.at[lo, side[TO_Q]]),
        }

    tail = slab // 256 * 128
    far_parts = [(2, 0, slab - tail), (3, slab - tail, tail)]

    def gather_copies(stage, k):
        buf = wg.at[k] if stage == 3 else part.at[k]
        if (stage, k) == (4, CHUNKS - 1):
            bands = far_parts
        else:
            bands = [(2, 0, slab)]
        relay = {}
        for msg, begin, width in bands:
            from_p, from_q, to_far = [pl.ds(n * slab + begin, width) for n in (1, 2, 0)]
            relay[TO_P, msg] = ring_copy(stage, k, TO_P, msg, buf.at[hi, from_q], buf.at[hi, to_far])
            relay[TO_Q, msg] = ring_copy(stage, k, TO_Q, msg, buf.at[lo, from_p], buf.at[lo, to_far])
        return {
            **relay,
            (TO_P, 0): ring_copy(stage, k, TO_P, 0, buf.at[lo, OWN], buf.at[lo, NEAR_P]),
            (TO_Q, 0): ring_copy(stage, k, TO_Q, 0, buf.at[hi, OWN], buf.at[hi, NEAR_Q]),
            (TO_P, 1): ring_copy(stage, k, TO_P, 1, buf.at[hi, OWN], buf.at[hi, NEAR_P]),
            (TO_Q, 1): ring_copy(stage, k, TO_Q, 1, buf.at[lo, OWN], buf.at[lo, NEAR_Q]),
        }

    copies = {}
    for k in range(CHUNKS):
        for stage in range(5):
            copies[stage, k] = reduce_copies(stage, k) if stage < 3 else gather_copies(stage, k)
    a_copies = [mate_copy(i, a_oth.at[:, slot[i]], a_blk.at[pl.ds(slab, slab), slot[i]]) for i in range(4)]
    m_copies = {(k, i): mate_copy(4 + 4 * k + i, pick.at[pl.ds(k * m, m), slot[i]], merged[k].at[:, slot[i]])
                for k in range(CHUNKS) for i in range(4)}
    first = 4 + 4 * CHUNKS
    x1_copies = [mate_copy(first + k, x1.at[k, :, own_half], x1.at[k, :, mate_half]) for k in range(CHUNKS)]
    x2_copies = [mate_copy(first + CHUNKS + k, x2own.at[k], x2rcv.at[k]) for k in range(CHUNKS)]
    z_copies = [mate_copy(first + 2 * CHUNKS + k, near.at[1, k, :, mate_half], near.at[0, k, :, mate_half]) for k in range(CHUNKS)]

    def by_rows(count, fn):
        def step(i, carry):
            fn(i)
            return carry
        lax.fori_loop(0, count // blk, step, 0)

    def rows_at(i, start=0):
        return pl.ds(pl.multiple_of(start + i * blk, blk), blk)

    def by_tiles(begin, end, fn):
        def step(t, carry):
            fn(pl.ds(pl.multiple_of(t * tile, 128), tile))
            return carry
        lax.fori_loop(begin, end, step, 0)

    def select_other(k, i):
        pick[pl.ds(k * m, m), slot[i]] = rows_cols(onehot[pl.ds(k * m, m), :], a_oth[:, slot[i]]).astype(bf16)

    def select_own(k, i):
        rk = pl.ds(k * m, m)
        here = (ids[rk, :] >= base_f) & (ids[rk, :] < base_f + slab)
        if (k, i) == (0, 0):
            x1[k, :, own_half] = rows_cols(onehot[rk, :], a_blk[pl.ds(0, slab), slot[i]]).astype(bf16)
            other(0, 1)
            m_copies[k, i].wait_recv()
            mine = x1[k, :, own_half].astype(f32)
        else:
            m_copies[k, i].wait_recv()
            mine = rows_cols(onehot[rk, :], a_blk[pl.ds(0, slab), slot[i]])
        merged[k][:, slot[i]] = jnp.where(here, mine, merged[k][:, slot[i]].astype(f32)).astype(bf16)

    def send_first(stage, k):
        cp = copies[stage, k]
        cp[TO_P, 0].start()
        cp[TO_Q, 0].start()
        cp[TO_P, 1].start()

    def start(stage, k):
        cp = copies[stage, k]
        if stage in (1, 2):
            for c_ in copies[stage - 1, k].values():
                c_.wait_send()

            def push(at):
                if stage == 1:
                    part[k, :, at] = rows_cols(x1[k], a_blk[:, at])
                else:
                    both = rows_cols(pick[pl.ds(0, 2 * m), two[0]], a_blk[:, at])
                    part[k, :, at] = both[:m] + both[m:]

            def mate_rows(pair):
                if (stage, k) == (1, 0):
                    for i in pair:
                        a_copies[i].wait_recv()

            mate_rows((0, 1))
            by_tiles(0, 3, push)
            send_first(stage, k)
            mate_rows((2, 3))
            by_tiles(3, 6, push)
            cp[TO_Q, 1].start()
        else:
            for msg in (0, 1):
                cp[TO_P, msg].start()
                cp[TO_Q, msg].start()

    def middle(stage, k):
        cp = copies[stage, k]
        for way in (TO_P, TO_Q):
            cp[way, 0].wait_recv()
            begin = 0 if way == TO_P else h
            dest = NEAR_Q if way == TO_P else NEAR_P
            if stage == 0:
                def select(i):
                    r = rows_at(i, begin)
                    rk = rows_at(i, k * m + begin)
                    here = (ids[rk, :] >= chip_f) & (ids[rk, :] < chip_f + 2 * slab)
                    merged[k][r, dest] = jnp.where(here, merged[k][r, dest].astype(f32),
                                                   far0[k, way, rows_at(i), :].astype(f32)).astype(bf16)
                by_rows(h, select)
            elif stage < 3:
                def add(i):
                    r = rows_at(i, begin)
                    part[k, r, dest] = part[k, r, dest] + far[stage - 1, k, way, rows_at(i), :]
                by_rows(h, add)
            cp[1 - way, 2].start()
            if (1 - way, 3) in cp:
                cp[1 - way, 3].start()

    def pull(buf, k, at, use, meanwhile=None):
        def split(i):
            r = rows_at(i)
            full = buf[k, r, at]
            top = full.astype(bf16)
            rest = full - top.astype(f32)
            mid = rest.astype(bf16)
            pick[r, at] = top
            pick[rows_at(i, m), at] = mid
            pick[rows_at(i, 2 * m), at] = (rest - mid.astype(f32)).astype(bf16)
        by_rows(m, split)

        def product(r):
            three = rows_rows(pick[pl.ds(0, 3 * m), at], a_blk[r, at])
            use(r, three[:m] + three[m:2 * m] + three[2 * m:])
        if meanwhile is None:
            by_tiles(0, 3, product)
        else:
            by_tiles(1, 3, product)
            meanwhile()
            by_tiles(0, 1, product)

    def close(k, at, z):
        bc[:, at] = bc[:, at] + jnp.sum(x1[k, :, at].astype(f32) * z, axis=0, keepdims=True)

    def last_far(n):
        k = CHUNKS - 1
        msg, begin, width = far_parts[n]
        copies[4, k][TO_P, msg].wait_recv()
        copies[4, k][TO_Q, msg].wait_recv()
        pull(part, k, pl.ds(begin, width), functools.partial(close, k))

    def last_own():
        pull(part, CHUNKS - 1, OWN, functools.partial(close, CHUNKS - 1))

    def last_nears():
        k = CHUNKS - 1
        copies[4, k][TO_P, 1].wait_recv()
        copies[4, k][TO_Q, 1].wait_recv()
        pull(part, k, pl.ds(slab, 2 * slab), functools.partial(close, k))

    def nears(stage, k):
        cp = copies[stage, k]
        cp[TO_P, 1].wait_recv()
        cp[TO_Q, 1].wait_recv()

        def keep(r, z):
            if stage == 3:
                near[1, k, :, r] = z
            else:
                close(k, r, z)
        pull(wg if stage == 3 else part, k, pl.ds(slab, 3 * slab), keep)

    def finish(stage, k):
        cp = copies[stage, k]
        for way in (TO_P, TO_Q):
            if stage < 3:
                cp[way, 1].wait_recv()
            cp[way, 2].wait_recv()
        if stage == 0:
            def first_level(i):
                r = rows_at(i)
                x1[k, r, own_half] = (merged[k][r, OWN].astype(f32) + near0[k, r, side[0]].astype(f32)
                                      + near0[k, r, side[1]].astype(f32)).astype(bf16)
            by_rows(m, first_level)
            x1_copies[k].start()
            if k == 0:
                a_copies[3].start()
                for copy in m_copies.values():
                    copy.wait_send()
            x1_copies[k].wait_recv()
        elif stage == 1:
            def second_level(i):
                r = rows_at(i)
                rk = rows_at(i, k * m)
                total = part[k, r, OWN] + near[0, k, r, side[0]] + near[0, k, r, side[1]]
                seen = jnp.maximum(onehot[rk, :].astype(f32), x1[k, r, own_half].astype(f32))
                x2own[k, r, :] = total * (1.0 - seen)
            by_rows(m, second_level)
            x2_copies[k].start()

            def split(i, source, half):
                r = rows_at(i)
                full = source[k, r, :]
                top = full.astype(bf16)
                pick[r, half] = top
                pick[rows_at(i, m), half] = (full - top.astype(f32)).astype(bf16)
            by_rows(m, lambda i: split(i, x2own, own_half))
            x2_copies[k].wait_recv()
            by_rows(m, lambda i: split(i, x2rcv, mate_half))
        elif stage == 2:
            def third_level(i):
                r = rows_at(i)
                rk = rows_at(i, k * m)
                total = part[k, r, OWN] + near[1, k, r, side[0]] + near[1, k, r, side[1]]
                seen = jnp.maximum(onehot[rk, :].astype(f32), x1[k, r, own_half].astype(f32))
                seen = jnp.maximum(seen, jnp.where(x2own[k, r, :] > 0, 1.0, 0.0))
                paths = total * (1.0 - seen)
                reached = paths > 0
                wg[k, r, OWN] = jnp.where(reached, lw[1] / jnp.where(reached, paths, 1.0), 0.0)
            by_rows(m, third_level)
            for c_ in cp.values():
                c_.wait_send()
        elif stage == 3:
            def keep(r, z):
                near[1, k, :, r] = near[1, k, :, r] + z
            pull(wg, k, FAR, keep, z_copies[k].start)
            z_copies[k].wait_recv()

            def second_weights(i):
                r = rows_at(i)
                paths = x2own[k, r, :]
                delta = paths * (near[1, k, r, own_half] + near[0, k, r, mate_half])
                reached = paths > 0
                part[k, r, OWN] = jnp.where(reached, (lw[0] + delta) / jnp.where(reached, paths, 1.0), 0.0)
                bc[:, own_half] = bc[:, own_half] + jnp.sum(delta, axis=0, keepdims=True)
            by_rows(m, second_weights)
        else:
            pull(part, k, FAR, functools.partial(close, k))

    def other(k, i):
        if k == 0:
            loads[0, i].wait()
        if (k, i) == (0, 0):
            for at in load_order[2:]:
                loads[at].start()
        select_other(k, i)
        if (k, i) == (0, 0):
            pl.semaphore_wait(barrier, 3 + 2 * (planes - 1))
        m_copies[k, i].start()

    def own(k, i):
        if k == 0:
            loads[1, i].wait()
        select_own(k, i)

    def first_level_sends(k):
        own(k, 0)
        copies[0, k][TO_P, 0].start()
        copies[0, k][TO_Q, 0].start()
        if k == 0:
            other(0, 2)
            a_copies[0].start()
        own(k, 1)
        copies[0, k][TO_P, 1].start()
        own(k, 2)
        copies[0, k][TO_Q, 1].start()

    other(0, 0)
    first_level_sends(0)
    lax.fori_loop(m // blk, src_count // blk, one_hot_rows, 0)
    bc[...] = jnp.zeros_like(bc)
    for i in range(3):
        other(1, i)
    a_copies[1].start()
    for k in range(CHUNKS):
        other(k, 3)
    a_copies[2].start()
    middle(0, 0)
    first_level_sends(1)
    for k in range(CHUNKS):
        own(k, 3)
    middle(0, 1)
    for stage in range(1, 5):
        finish(stage - 1, 0)
        start(stage, 0)
        if stage == 4:
            nears(3, 1)
        middle(stage, 0)
        finish(stage - 1, 1)
        start(stage, 1)
        if stage >= 3:
            nears(stage, 0)
        if stage == 4:
            last_own()
        middle(stage, 1)
    finish(4, 0)
    last_nears()
    last_far(0)
    last_far(1)

    total[...] = bc[...] * scale
    keep_own = pltpu.make_async_copy(total.at[:, own_half], out.at[s_me], load_sem.at[0])
    keep_own.start()
    for o in range(planes):
        there = lax.rem(s_me + o, planes)
        for other_core in (0, 1):
            if o == 0 and not other_core:
                continue
            device = {"src": there, "graph": x * 2 + (1 - c)} if other_core else {"src": there}
            pltpu.make_async_remote_copy(src_ref=total.at[:, side[other_core]], dst_ref=out.at[other_core * planes + s_me],
                                         send_sem=plane_s, recv_sem=plane_r,
                                         device_id=device, device_id_type=MESH).start()

    for copy in a_copies + x1_copies + x2_copies + z_copies:
        copy.wait_send()
    for k in range(CHUNKS):
        for stage in (3, 4):
            for c_ in copies[stage, k].values():
                c_.wait_send()
    keep_own.wait()
    arrivals = out.at[pl.ds(0, 2 * planes - 1)]
    every = pltpu.make_async_remote_copy(src_ref=arrivals, dst_ref=arrivals, send_sem=plane_s, recv_sem=plane_r,
                                         device_id=to_mate, device_id_type=MESH)
    every.wait_recv()
    every.wait_send()


def solution(mesh):
    planes = mesh.shape["src"]
    ring = mesh.shape["graph"] // 2

    def device_program(adj_slab, src_local, level_weight):
        slab, vertex_count = adj_slab.shape
        src_count = src_local.shape[0]
        m = src_count // CHUNKS
        scale = vertex_count / (src_count * planes * (level_weight.shape[0] + 1) ** 3)
        wide = 4 * slab
        vmem = pltpu.VMEM
        sem = pltpu.SemaphoreType.DMA
        mates = 4 + 7 * CHUNKS
        rings = 5 * CHUNKS * 8
        flops = 2 * 9 * src_count * slab * vertex_count
        bc = pl.pallas_call(
            functools.partial(kernel, ring, planes, scale),
            out_shape=jax.ShapeDtypeStruct((2 * planes, 1, slab), f32),
            in_specs=[pl.BlockSpec(memory_space=pl.ANY), pl.BlockSpec(memory_space=vmem), pl.BlockSpec(memory_space=pltpu.SMEM)],
            out_specs=pl.BlockSpec(memory_space=pl.ANY),
            scratch_shapes=[
                vmem((2 * slab, wide), bf16), vmem((slab, wide), bf16),
                vmem((2 * src_count, wide), bf16), vmem((src_count, 1), f32), vmem((src_count, slab), bf16),
                vmem((CHUNKS, m, 2 * slab), bf16), vmem((CHUNKS, m, slab), f32), vmem((CHUNKS, m, slab), f32),
                vmem((CHUNKS, m, wide), f32), vmem((CHUNKS, m, wide), f32),
                vmem((CHUNKS, m, 2 * slab), bf16), vmem((CHUNKS, 2, m // 2, slab), bf16),
                vmem((2, CHUNKS, m, 2 * slab), f32), vmem((2, CHUNKS, 2, m // 2, slab), f32),
                vmem((1, 2 * slab), f32), vmem((1, 2 * slab), f32),
                sem((8,)), sem((rings,)), sem((rings,)), sem((mates,)), sem((mates,)), sem, sem,
            ],
            compiler_params=pltpu.CompilerParams(collective_id=0, has_side_effects=True, vmem_limit_bytes=67043328),
            cost_estimate=pl.CostEstimate(flops=flops, bytes_accessed=2 * slab * vertex_count, transcendentals=0),
        )(adj_slab, src_local.reshape(1, src_count), level_weight)
        return jnp.sum(bc, axis=(0, 1))

    return jax.shard_map(device_program, mesh=mesh,
                         in_specs=(P(("batch", "graph"), None), P(("batch", "src")), P(None)),
                         out_specs=P(("batch", "graph")), check_vma=False)
```

```python
import functools

import jax
import jax.numpy as jnp
from jax import lax
from jax.experimental import pallas as pl
from jax.experimental.pallas import tpu as pltpu
from jax.sharding import PartitionSpec as P

MESH = pl.DeviceIdType.MESH
f32, bf16 = jnp.float32, jnp.bfloat16
CHUNKS = 2
SIDE = 4
TO_P, TO_Q = 0, 1


def rows_cols(lhs, rhs):
    return lax.dot_general(lhs, rhs, (((1,), (0,)), ((), ())), preferred_element_type=f32)


def rows_rows(lhs, rhs):
    return lax.dot_general(lhs, rhs, (((1,), (1,)), ((), ())), preferred_element_type=f32)


def kernel(ring, planes, scale, adj, src, lw, out,
           a_blk, a_oth, pick, ids, onehot, x1, x2own, x2rcv, part, wg,
           near0, far0, near, far, bc, total,
           load_sem, ssem, rsem, d2d_s, d2d_r, plane_s, plane_r, rounds):
    slab = a_oth.shape[0]
    cols_all = a_oth.shape[1]
    src_count = ids.shape[0]
    m = src_count // CHUNKS
    h = m // 2
    tile = 2 * slab // 3
    blk = min(32, h)

    g = lax.axis_index("graph")
    s_me = lax.axis_index("src")
    x, c = g // 2, g % 2
    odd = lax.rem(x, 2)
    chip_p = x + 1 - 2 * odd
    chip_q = lax.rem(x + ring - 1 + 2 * odd, ring)
    chip_far = lax.rem(x + 2, ring)
    to_p = {"graph": chip_p * 2 + c}
    to_q = {"graph": chip_q * 2 + c}
    to_mate = {"graph": x * 2 + (1 - c)}
    chips = (chip_far, chip_p, chip_q, x)
    slot = [pl.ds(i * slab, slab) for i in range(4)]
    FAR, NEAR_P, NEAR_Q, OWN = slot

    loads = {}
    for i, chip in enumerate(chips):
        for own in (0, 1):
            at = pl.ds(pl.multiple_of((chip * 2 + (c if own else 1 - c)) * slab, 128), slab)
            target = a_blk.at[pl.ds(0, slab), slot[i]] if own else a_oth.at[:, slot[i]]
            loads[own, i] = pltpu.make_async_copy(adj.at[:, at], target, load_sem.at[4 * own + i])
    for own, i in ((0, 0), (1, 0), (0, 1), (0, 2), (1, 1), (1, 2), (0, 3), (1, 3)):
        loads[own, i].start()

    barrier = pltpu.get_barrier_semaphore()
    for dev in (to_p, to_q, to_mate):
        pl.semaphore_signal(barrier, inc=1, device_id=dev, device_id_type=MESH)
    if planes == SIDE * SIDE:
        row_, col_ = s_me // SIDE, lax.rem(s_me, SIDE)
        around = [{"src": row_ * SIDE + lax.rem(col_ + step, SIDE)} for step in (1, SIDE - 1)]
        around += [{"src": lax.rem(row_ + step, SIDE) * SIDE + col_} for step in (1, SIDE - 1)]
    else:
        around = [{"src": lax.rem(s_me + o, planes), "graph": x * 2 + core} for o in range(1, planes) for core in (0, 1)]
    for dev in around:
        pl.semaphore_signal(barrier, inc=1, device_id=dev, device_id_type=MESH)

    def tell(n):
        for dev in around:
            pl.semaphore_signal(rounds.at[n], inc=1, device_id=dev, device_id_type=MESH)

    def hear(n):
        pl.semaphore_wait(rounds.at[n], len(around))

    row = lax.broadcasted_iota(jnp.int32, (src_count, src_count), 0)
    col = lax.broadcasted_iota(jnp.int32, (src_count, src_count), 1)
    ids[...] = jnp.sum(jnp.where(row == col, src[...].astype(f32), 0.0), axis=1, keepdims=True)
    base = g * slab
    base_f = base.astype(f32)
    chip_f = (x * 2 * slab).astype(f32)
    lane = (lax.broadcasted_iota(jnp.int32, (blk, slab), 1) + base).astype(f32)

    def one_hot_rows(i, carry):
        r = pl.ds(pl.multiple_of(i * blk, blk), blk)
        onehot[r, :] = jnp.where(ids[r, :] == lane, 1.0, 0.0).astype(bf16)
        return carry

    lax.fori_loop(0, m // blk, one_hot_rows, 0)

    def mate_copy(i, source, target):
        return pltpu.make_async_remote_copy(src_ref=source, dst_ref=target, send_sem=d2d_s.at[i], recv_sem=d2d_r.at[i],
                                            device_id=to_mate, device_id_type=MESH)

    def ring_copy(stage, k, way, msg, source, target):
        i = ((stage * CHUNKS + k) * 2 + way) * 4 + msg
        return pltpu.make_async_remote_copy(src_ref=source, dst_ref=target, send_sem=ssem.at[i], recv_sem=rsem.at[i],
                                            device_id=to_p if way == TO_P else to_q, device_id_type=MESH)

    lo, hi = pl.ds(0, h), pl.ds(h, h)
    side = [pl.ds(0, slab), pl.ds(slab, slab)]
    own_half, mate_half = side
    merged = [pick.at[pl.ds(src_count + k * m, m), :] for k in range(CHUNKS)]
    two = [pl.ds(0, 2 * slab), pl.ds(2 * slab, 2 * slab)]

    def reduce_copies(stage, k):
        if stage == 0:
            send, nr, fr = merged[k], near0.at[k], far0.at[k]
        else:
            send, nr, fr = part.at[k], near.at[stage - 1, k], far.at[stage - 1, k]
        return {
            (TO_P, 0): ring_copy(stage, k, TO_P, 0, send.at[lo, FAR], fr.at[TO_P]),
            (TO_Q, 0): ring_copy(stage, k, TO_Q, 0, send.at[hi, FAR], fr.at[TO_Q]),
            (TO_P, 1): ring_copy(stage, k, TO_P, 1, send.at[lo, NEAR_P], nr.at[lo, side[TO_P]]),
            (TO_Q, 1): ring_copy(stage, k, TO_Q, 1, send.at[hi, NEAR_Q], nr.at[hi, side[TO_Q]]),
            (TO_P, 2): ring_copy(stage, k, TO_P, 2, send.at[hi, NEAR_P], nr.at[hi, side[TO_P]]),
            (TO_Q, 2): ring_copy(stage, k, TO_Q, 2, send.at[lo, NEAR_Q], nr.at[lo, side[TO_Q]]),
        }

    tail = slab // 256 * 128
    far_parts = [(2, 0, slab - tail), (3, slab - tail, tail)]

    def gather_copies(stage, k):
        buf = wg.at[k] if stage == 3 else part.at[k]
        if (stage, k) == (4, CHUNKS - 1):
            bands = far_parts
        else:
            bands = [(2, 0, slab)]
        relay = {}
        for msg, begin, width in bands:
            from_p, from_q, to_far = [pl.ds(n * slab + begin, width) for n in (1, 2, 0)]
            relay[TO_P, msg] = ring_copy(stage, k, TO_P, msg, buf.at[hi, from_q], buf.at[hi, to_far])
            relay[TO_Q, msg] = ring_copy(stage, k, TO_Q, msg, buf.at[lo, from_p], buf.at[lo, to_far])
        return {
            **relay,
            (TO_P, 0): ring_copy(stage, k, TO_P, 0, buf.at[lo, OWN], buf.at[lo, NEAR_P]),
            (TO_Q, 0): ring_copy(stage, k, TO_Q, 0, buf.at[hi, OWN], buf.at[hi, NEAR_Q]),
            (TO_P, 1): ring_copy(stage, k, TO_P, 1, buf.at[hi, OWN], buf.at[hi, NEAR_P]),
            (TO_Q, 1): ring_copy(stage, k, TO_Q, 1, buf.at[lo, OWN], buf.at[lo, NEAR_Q]),
        }

    copies = {}
    for k in range(CHUNKS):
        for stage in range(5):
            copies[stage, k] = reduce_copies(stage, k) if stage < 3 else gather_copies(stage, k)
    a_copies = [mate_copy(i, a_oth.at[:, slot[i]], a_blk.at[pl.ds(slab, slab), slot[i]]) for i in range(4)]
    m_copies = {(k, i): mate_copy(4 + 4 * k + i, pick.at[pl.ds(k * m, m), slot[i]], merged[k].at[:, slot[i]])
                for k in range(CHUNKS) for i in range(4)}
    first = 4 + 4 * CHUNKS
    x1_copies = [mate_copy(first + k, x1.at[k, :, own_half], x1.at[k, :, mate_half]) for k in range(CHUNKS)]
    x2_copies = [mate_copy(first + CHUNKS + k, x2own.at[k], x2rcv.at[k]) for k in range(CHUNKS)]
    z_copies = [mate_copy(first + 2 * CHUNKS + k, near.at[1, k, :, mate_half], near.at[0, k, :, mate_half]) for k in range(CHUNKS)]

    def by_rows(count, fn):
        def step(i, carry):
            fn(i)
            return carry
        lax.fori_loop(0, count // blk, step, 0)

    def rows_at(i, start=0):
        return pl.ds(pl.multiple_of(start + i * blk, blk), blk)

    def by_tiles(begin, end, fn):
        def step(t, carry):
            fn(pl.ds(pl.multiple_of(t * tile, 128), tile))
            return carry
        lax.fori_loop(begin, end, step, 0)

    def select_other(k, i):
        pick[pl.ds(k * m, m), slot[i]] = rows_cols(onehot[pl.ds(k * m, m), :], a_oth[:, slot[i]]).astype(bf16)

    def select_own(k, i):
        rk = pl.ds(k * m, m)
        here = (ids[rk, :] >= base_f) & (ids[rk, :] < base_f + slab)
        if (k, i) == (0, 0):
            x1[k, :, own_half] = rows_cols(onehot[rk, :], a_blk[pl.ds(0, slab), slot[i]]).astype(bf16)
            other(0, 1)
            m_copies[k, i].wait_recv()
            mine = x1[k, :, own_half].astype(f32)
        else:
            m_copies[k, i].wait_recv()
            mine = rows_cols(onehot[rk, :], a_blk[pl.ds(0, slab), slot[i]])
        merged[k][:, slot[i]] = jnp.where(here, mine, merged[k][:, slot[i]].astype(f32)).astype(bf16)

    def send_first(stage, k):
        cp = copies[stage, k]
        cp[TO_P, 0].start()
        cp[TO_Q, 0].start()
        cp[TO_P, 1].start()

    def start(stage, k):
        cp = copies[stage, k]
        if stage in (1, 2):
            for c_ in copies[stage - 1, k].values():
                c_.wait_send()

            def push(at):
                if stage == 1:
                    part[k, :, at] = rows_cols(x1[k], a_blk[:, at])
                else:
                    both = rows_cols(pick[pl.ds(0, 2 * m), two[0]], a_blk[:, at])
                    part[k, :, at] = both[:m] + both[m:]

            def mate_rows(pair):
                if (stage, k) == (1, 0):
                    for i in pair:
                        a_copies[i].wait_recv()

            mate_rows((0, 1))
            by_tiles(0, 3, push)
            send_first(stage, k)
            mate_rows((2, 3))
            by_tiles(3, 6, push)
            cp[TO_Q, 1].start()
        else:
            for msg in (0, 1):
                cp[TO_P, msg].start()
                cp[TO_Q, msg].start()

    def middle(stage, k):
        cp = copies[stage, k]
        for way in (TO_P, TO_Q):
            cp[way, 0].wait_recv()
            begin = 0 if way == TO_P else h
            dest = NEAR_Q if way == TO_P else NEAR_P
            if stage == 0:
                def select(i):
                    r = rows_at(i, begin)
                    rk = rows_at(i, k * m + begin)
                    here = (ids[rk, :] >= chip_f) & (ids[rk, :] < chip_f + 2 * slab)
                    merged[k][r, dest] = jnp.where(here, merged[k][r, dest].astype(f32),
                                                   far0[k, way, rows_at(i), :].astype(f32)).astype(bf16)
                by_rows(h, select)
            elif stage < 3:
                def add(i):
                    r = rows_at(i, begin)
                    part[k, r, dest] = part[k, r, dest] + far[stage - 1, k, way, rows_at(i), :]
                by_rows(h, add)
            cp[1 - way, 2].start()
            if (1 - way, 3) in cp:
                cp[1 - way, 3].start()

    def pull(buf, k, at, use, meanwhile=None):
        def split(i):
            r = rows_at(i)
            full = buf[k, r, at]
            top = full.astype(bf16)
            rest = full - top.astype(f32)
            mid = rest.astype(bf16)
            pick[r, at] = top
            pick[rows_at(i, m), at] = mid
            pick[rows_at(i, 2 * m), at] = (rest - mid.astype(f32)).astype(bf16)
        by_rows(m, split)

        def product(r):
            three = rows_rows(pick[pl.ds(0, 3 * m), at], a_blk[r, at])
            use(r, three[:m] + three[m:2 * m] + three[2 * m:])
        if meanwhile is None:
            by_tiles(0, 3, product)
        else:
            by_tiles(1, 3, product)
            meanwhile()
            by_tiles(0, 1, product)

    def close(k, at, z):
        bc[:, at] = bc[:, at] + jnp.sum(x1[k, :, at].astype(f32) * z, axis=0, keepdims=True)

    def last_far(n):
        k = CHUNKS - 1
        msg, begin, width = far_parts[n]
        copies[4, k][TO_P, msg].wait_recv()
        copies[4, k][TO_Q, msg].wait_recv()
        pull(part, k, pl.ds(begin, width), functools.partial(close, k))

    def last_own():
        pull(part, CHUNKS - 1, OWN, functools.partial(close, CHUNKS - 1))

    def last_nears():
        k = CHUNKS - 1
        copies[4, k][TO_P, 1].wait_recv()
        copies[4, k][TO_Q, 1].wait_recv()
        pull(part, k, pl.ds(slab, 2 * slab), functools.partial(close, k))

    def nears(stage, k):
        cp = copies[stage, k]
        cp[TO_P, 1].wait_recv()
        cp[TO_Q, 1].wait_recv()

        def keep(r, z):
            if stage == 3:
                near[1, k, :, r] = z
            else:
                close(k, r, z)
        pull(wg if stage == 3 else part, k, pl.ds(slab, 3 * slab), keep)

    def finish(stage, k):
        cp = copies[stage, k]
        for way in (TO_P, TO_Q):
            if stage < 3:
                cp[way, 1].wait_recv()
            cp[way, 2].wait_recv()
        if stage == 0:
            def first_level(i):
                r = rows_at(i)
                x1[k, r, own_half] = (merged[k][r, OWN].astype(f32) + near0[k, r, side[0]].astype(f32)
                                      + near0[k, r, side[1]].astype(f32)).astype(bf16)
            by_rows(m, first_level)
            x1_copies[k].start()
            if k == 0:
                a_copies[3].start()
                for copy in m_copies.values():
                    copy.wait_send()
            x1_copies[k].wait_recv()
        elif stage == 1:
            def second_level(i):
                r = rows_at(i)
                rk = rows_at(i, k * m)
                total = part[k, r, OWN] + near[0, k, r, side[0]] + near[0, k, r, side[1]]
                seen = jnp.maximum(onehot[rk, :].astype(f32), x1[k, r, own_half].astype(f32))
                x2own[k, r, :] = total * (1.0 - seen)
            by_rows(m, second_level)
            x2_copies[k].start()

            def split(i, source, half):
                r = rows_at(i)
                full = source[k, r, :]
                top = full.astype(bf16)
                pick[r, half] = top
                pick[rows_at(i, m), half] = (full - top.astype(f32)).astype(bf16)
            by_rows(m, lambda i: split(i, x2own, own_half))
            x2_copies[k].wait_recv()
            by_rows(m, lambda i: split(i, x2rcv, mate_half))
        elif stage == 2:
            def third_level(i):
                r = rows_at(i)
                rk = rows_at(i, k * m)
                total = part[k, r, OWN] + near[1, k, r, side[0]] + near[1, k, r, side[1]]
                seen = jnp.maximum(onehot[rk, :].astype(f32), x1[k, r, own_half].astype(f32))
                seen = jnp.maximum(seen, jnp.where(x2own[k, r, :] > 0, 1.0, 0.0))
                paths = total * (1.0 - seen)
                reached = paths > 0
                wg[k, r, OWN] = jnp.where(reached, lw[1] / jnp.where(reached, paths, 1.0), 0.0)
            by_rows(m, third_level)
            for c_ in cp.values():
                c_.wait_send()
        elif stage == 3:
            def keep(r, z):
                near[1, k, :, r] = near[1, k, :, r] + z
            pull(wg, k, FAR, keep, z_copies[k].start)
            z_copies[k].wait_recv()

            def second_weights(i):
                r = rows_at(i)
                paths = x2own[k, r, :]
                delta = paths * (near[1, k, r, own_half] + near[0, k, r, mate_half])
                reached = paths > 0
                part[k, r, OWN] = jnp.where(reached, (lw[0] + delta) / jnp.where(reached, paths, 1.0), 0.0)
                bc[:, own_half] = bc[:, own_half] + jnp.sum(delta, axis=0, keepdims=True)
            by_rows(m, second_weights)
        else:
            pull(part, k, FAR, functools.partial(close, k))

    def other(k, i):
        if k == 0:
            loads[0, i].wait()
        select_other(k, i)
        if (k, i) == (0, 0):
            pl.semaphore_wait(barrier, 3 + len(around))
            tell(0)
        m_copies[k, i].start()

    def own(k, i):
        if k == 0:
            loads[1, i].wait()
        select_own(k, i)

    def first_level_sends(k):
        own(k, 0)
        copies[0, k][TO_P, 0].start()
        copies[0, k][TO_Q, 0].start()
        if k == 0:
            other(0, 2)
            a_copies[0].start()
        own(k, 1)
        copies[0, k][TO_P, 1].start()
        own(k, 2)
        copies[0, k][TO_Q, 1].start()

    other(0, 0)
    first_level_sends(0)
    lax.fori_loop(m // blk, src_count // blk, one_hot_rows, 0)
    bc[...] = jnp.zeros_like(bc)
    for i in range(3):
        other(1, i)
    a_copies[1].start()
    for k in range(CHUNKS):
        other(k, 3)
    a_copies[2].start()
    middle(0, 0)
    first_level_sends(1)
    for k in range(CHUNKS):
        own(k, 3)
    middle(0, 1)
    for stage in range(1, 5):
        finish(stage - 1, 0)
        start(stage, 0)
        if stage == 4:
            nears(3, 1)
        middle(stage, 0)
        hear(stage - 1)
        if stage < 4:
            tell(stage)
        finish(stage - 1, 1)
        start(stage, 1)
        if stage >= 3:
            nears(stage, 0)
        if stage == 4:
            last_own()
        middle(stage, 1)
    finish(4, 0)
    last_nears()
    last_far(0)
    last_far(1)

    total[...] = bc[...] * scale
    keep_own = pltpu.make_async_copy(total.at[:, own_half], out.at[s_me], load_sem.at[0])
    keep_own.start()
    for o in range(planes):
        there = lax.rem(s_me + o, planes)
        for other_core in (0, 1):
            if o == 0 and not other_core:
                continue
            device = {"src": there, "graph": x * 2 + (1 - c)} if other_core else {"src": there}
            pltpu.make_async_remote_copy(src_ref=total.at[:, side[other_core]], dst_ref=out.at[other_core * planes + s_me],
                                         send_sem=plane_s, recv_sem=plane_r,
                                         device_id=device, device_id_type=MESH).start()

    for copy in a_copies + x1_copies + x2_copies + z_copies:
        copy.wait_send()
    for k in range(CHUNKS):
        for stage in (3, 4):
            for c_ in copies[stage, k].values():
                c_.wait_send()
    keep_own.wait()
    arrivals = out.at[pl.ds(0, 2 * planes - 1)]
    every = pltpu.make_async_remote_copy(src_ref=arrivals, dst_ref=arrivals, send_sem=plane_s, recv_sem=plane_r,
                                         device_id=to_mate, device_id_type=MESH)
    every.wait_recv()
    every.wait_send()


def solution(mesh):
    planes = mesh.shape["src"]
    ring = mesh.shape["graph"] // 2

    def device_program(adj_slab, src_local, level_weight):
        slab, vertex_count = adj_slab.shape
        src_count = src_local.shape[0]
        m = src_count // CHUNKS
        scale = vertex_count / (src_count * planes * (level_weight.shape[0] + 1) ** 3)
        wide = 4 * slab
        vmem = pltpu.VMEM
        sem = pltpu.SemaphoreType.DMA
        mates = 4 + 7 * CHUNKS
        rings = 5 * CHUNKS * 8
        flops = 2 * 9 * src_count * slab * vertex_count
        bc = pl.pallas_call(
            functools.partial(kernel, ring, planes, scale),
            out_shape=jax.ShapeDtypeStruct((2 * planes, 1, slab), f32),
            in_specs=[pl.BlockSpec(memory_space=pl.ANY), pl.BlockSpec(memory_space=vmem), pl.BlockSpec(memory_space=pltpu.SMEM)],
            out_specs=pl.BlockSpec(memory_space=pl.ANY),
            scratch_shapes=[
                vmem((2 * slab, wide), bf16), vmem((slab, wide), bf16),
                vmem((2 * src_count, wide), bf16), vmem((src_count, 1), f32), vmem((src_count, slab), bf16),
                vmem((CHUNKS, m, 2 * slab), bf16), vmem((CHUNKS, m, slab), f32), vmem((CHUNKS, m, slab), f32),
                vmem((CHUNKS, m, wide), f32), vmem((CHUNKS, m, wide), f32),
                vmem((CHUNKS, m, 2 * slab), bf16), vmem((CHUNKS, 2, m // 2, slab), bf16),
                vmem((2, CHUNKS, m, 2 * slab), f32), vmem((2, CHUNKS, 2, m // 2, slab), f32),
                vmem((1, 2 * slab), f32), vmem((1, 2 * slab), f32),
                sem((8,)), sem((rings,)), sem((rings,)), sem((mates,)), sem((mates,)), sem, sem, pltpu.SemaphoreType.REGULAR((4,)),
            ],
            compiler_params=pltpu.CompilerParams(collective_id=0, has_side_effects=True, vmem_limit_bytes=67043328),
            cost_estimate=pl.CostEstimate(flops=flops, bytes_accessed=2 * slab * vertex_count, transcendentals=0),
        )(adj_slab, src_local.reshape(1, src_count), level_weight)
        return jnp.sum(bc, axis=(0, 1))

    return jax.shard_map(device_program, mesh=mesh,
                         in_specs=(P(("batch", "graph"), None), P(("batch", "src")), P(None)),
                         out_specs=P(("batch", "graph")), check_vma=False)
```

```python
import functools

import jax
import jax.numpy as jnp
from jax import lax
from jax.experimental import pallas as pl
from jax.experimental.pallas import tpu as pltpu
from jax.sharding import PartitionSpec as P

MESH = pl.DeviceIdType.MESH
f32, bf16 = jnp.float32, jnp.bfloat16
CHUNKS = 2
SIDE = 4
TO_P, TO_Q = 0, 1


def rows_cols(lhs, rhs):
    return lax.dot_general(lhs, rhs, (((1,), (0,)), ((), ())), preferred_element_type=f32)


def rows_rows(lhs, rhs):
    return lax.dot_general(lhs, rhs, (((1,), (1,)), ((), ())), preferred_element_type=f32)


def kernel(ring, planes, scale, adj, src, lw, out,
           a_blk, a_oth, pick, ids, onehot, x1, x2own, x2rcv, part, wg,
           near0, far0, near, far, bc, total,
           load_sem, ssem, rsem, d2d_s, d2d_r, plane_s, plane_r, rounds):
    slab = a_oth.shape[0]
    cols_all = a_oth.shape[1]
    src_count = ids.shape[0]
    m = src_count // CHUNKS
    h = m // 2
    tile = 2 * slab // 3
    blk = min(32, h)

    g = lax.axis_index("graph")
    s_me = lax.axis_index("src")
    x, c = g // 2, g % 2
    odd = lax.rem(x, 2)
    chip_p = x + 1 - 2 * odd
    chip_q = lax.rem(x + ring - 1 + 2 * odd, ring)
    chip_far = lax.rem(x + 2, ring)
    to_p = {"graph": chip_p * 2 + c}
    to_q = {"graph": chip_q * 2 + c}
    to_mate = {"graph": x * 2 + (1 - c)}
    chips = (chip_far, chip_p, chip_q, x)
    slot = [pl.ds(i * slab, slab) for i in range(4)]
    FAR, NEAR_P, NEAR_Q, OWN = slot

    loads = {}
    for i, chip in enumerate(chips):
        for own in (0, 1):
            at = pl.ds(pl.multiple_of((chip * 2 + (c if own else 1 - c)) * slab, 128), slab)
            target = a_blk.at[pl.ds(0, slab), slot[i]] if own else a_oth.at[:, slot[i]]
            loads[own, i] = pltpu.make_async_copy(adj.at[:, at], target, load_sem.at[4 * own + i])
    for own, i in ((0, 0), (1, 0), (0, 1), (0, 2), (1, 1), (1, 2), (0, 3), (1, 3)):
        loads[own, i].start()

    barrier = pltpu.get_barrier_semaphore()
    for dev in (to_p, to_q, to_mate):
        pl.semaphore_signal(barrier, inc=1, device_id=dev, device_id_type=MESH)
    if planes == SIDE * SIDE:
        row_, col_ = s_me // SIDE, lax.rem(s_me, SIDE)
        around = [{"src": row_ * SIDE + lax.rem(col_ + step, SIDE)} for step in (1, SIDE - 1)]
        around += [{"src": lax.rem(row_ + step, SIDE) * SIDE + col_} for step in (1, SIDE - 1)]
    else:
        around = [{"src": lax.rem(s_me + o, planes), "graph": x * 2 + core} for o in range(1, planes) for core in (0, 1)]
    for dev in around:
        pl.semaphore_signal(barrier, inc=1, device_id=dev, device_id_type=MESH)

    def tell(n):
        for dev in around:
            pl.semaphore_signal(rounds.at[n], inc=1, device_id=dev, device_id_type=MESH)

    def hear(n):
        pl.semaphore_wait(rounds.at[n], len(around))

    row = lax.broadcasted_iota(jnp.int32, (src_count, src_count), 0)
    col = lax.broadcasted_iota(jnp.int32, (src_count, src_count), 1)
    ids[...] = jnp.sum(jnp.where(row == col, src[...].astype(f32), 0.0), axis=1, keepdims=True)
    base = g * slab
    base_f = base.astype(f32)
    chip_f = (x * 2 * slab).astype(f32)
    lane = (lax.broadcasted_iota(jnp.int32, (blk, slab), 1) + base).astype(f32)

    def one_hot_rows(i, carry):
        r = pl.ds(pl.multiple_of(i * blk, blk), blk)
        onehot[r, :] = jnp.where(ids[r, :] == lane, 1.0, 0.0).astype(bf16)
        return carry

    lax.fori_loop(0, m // blk, one_hot_rows, 0)

    def mate_copy(i, source, target):
        return pltpu.make_async_remote_copy(src_ref=source, dst_ref=target, send_sem=d2d_s.at[i], recv_sem=d2d_r.at[i],
                                            device_id=to_mate, device_id_type=MESH)

    def ring_copy(stage, k, way, msg, source, target):
        i = ((stage * CHUNKS + k) * 2 + way) * 4 + msg
        return pltpu.make_async_remote_copy(src_ref=source, dst_ref=target, send_sem=ssem.at[i], recv_sem=rsem.at[i],
                                            device_id=to_p if way == TO_P else to_q, device_id_type=MESH)

    lo, hi = pl.ds(0, h), pl.ds(h, h)
    side = [pl.ds(0, slab), pl.ds(slab, slab)]
    own_half, mate_half = side
    merged = [pick.at[pl.ds(src_count + k * m, m), :] for k in range(CHUNKS)]
    two = [pl.ds(0, 2 * slab), pl.ds(2 * slab, 2 * slab)]

    def reduce_copies(stage, k):
        if stage == 0:
            send, nr, fr = merged[k], near0.at[k], far0.at[k]
        else:
            send, nr, fr = part.at[k], near.at[stage - 1, k], far.at[stage - 1, k]
        return {
            (TO_P, 0): ring_copy(stage, k, TO_P, 0, send.at[lo, FAR], fr.at[TO_P]),
            (TO_Q, 0): ring_copy(stage, k, TO_Q, 0, send.at[hi, FAR], fr.at[TO_Q]),
            (TO_P, 1): ring_copy(stage, k, TO_P, 1, send.at[lo, NEAR_P], nr.at[lo, side[TO_P]]),
            (TO_Q, 1): ring_copy(stage, k, TO_Q, 1, send.at[hi, NEAR_Q], nr.at[hi, side[TO_Q]]),
            (TO_P, 2): ring_copy(stage, k, TO_P, 2, send.at[hi, NEAR_P], nr.at[hi, side[TO_P]]),
            (TO_Q, 2): ring_copy(stage, k, TO_Q, 2, send.at[lo, NEAR_Q], nr.at[lo, side[TO_Q]]),
        }

    tail = slab // 256 * 128
    far_parts = [(2, 0, slab - tail), (3, slab - tail, tail)]

    def gather_copies(stage, k):
        buf = wg.at[k] if stage == 3 else part.at[k]
        if (stage, k) == (4, CHUNKS - 1):
            bands = far_parts
        else:
            bands = [(2, 0, slab)]
        relay = {}
        for msg, begin, width in bands:
            from_p, from_q, to_far = [pl.ds(n * slab + begin, width) for n in (1, 2, 0)]
            relay[TO_P, msg] = ring_copy(stage, k, TO_P, msg, buf.at[hi, from_q], buf.at[hi, to_far])
            relay[TO_Q, msg] = ring_copy(stage, k, TO_Q, msg, buf.at[lo, from_p], buf.at[lo, to_far])
        return {
            **relay,
            (TO_P, 0): ring_copy(stage, k, TO_P, 0, buf.at[lo, OWN], buf.at[lo, NEAR_P]),
            (TO_Q, 0): ring_copy(stage, k, TO_Q, 0, buf.at[hi, OWN], buf.at[hi, NEAR_Q]),
            (TO_P, 1): ring_copy(stage, k, TO_P, 1, buf.at[hi, OWN], buf.at[hi, NEAR_P]),
            (TO_Q, 1): ring_copy(stage, k, TO_Q, 1, buf.at[lo, OWN], buf.at[lo, NEAR_Q]),
        }

    copies = {}
    for k in range(CHUNKS):
        for stage in range(5):
            copies[stage, k] = reduce_copies(stage, k) if stage < 3 else gather_copies(stage, k)
    a_copies = [mate_copy(i, a_oth.at[:, slot[i]], a_blk.at[pl.ds(slab, slab), slot[i]]) for i in range(4)]
    m_copies = {(k, i): mate_copy(4 + 4 * k + i, pick.at[pl.ds(k * m, m), slot[i]], merged[k].at[:, slot[i]])
                for k in range(CHUNKS) for i in range(4)}
    first = 4 + 4 * CHUNKS
    x1_copies = [mate_copy(first + k, x1.at[k, :, own_half], x1.at[k, :, mate_half]) for k in range(CHUNKS)]
    x2_copies = [mate_copy(first + CHUNKS + k, x2own.at[k], x2rcv.at[k]) for k in range(CHUNKS)]
    z_copies = [mate_copy(first + 2 * CHUNKS + k, near.at[1, k, :, mate_half], near.at[0, k, :, mate_half]) for k in range(CHUNKS)]

    def by_rows(count, fn):
        def step(i, carry):
            fn(i)
            return carry
        lax.fori_loop(0, count // blk, step, 0)

    def rows_at(i, start=0):
        return pl.ds(pl.multiple_of(start + i * blk, blk), blk)

    def by_tiles(begin, end, fn):
        def step(t, carry):
            fn(pl.ds(pl.multiple_of(t * tile, 128), tile))
            return carry
        lax.fori_loop(begin, end, step, 0)

    def select_other(k, i):
        pick[pl.ds(k * m, m), slot[i]] = rows_cols(onehot[pl.ds(k * m, m), :], a_oth[:, slot[i]]).astype(bf16)

    def select_own(k, i):
        rk = pl.ds(k * m, m)
        here = (ids[rk, :] >= base_f) & (ids[rk, :] < base_f + slab)
        if (k, i) == (0, 0):
            x1[k, :, own_half] = rows_cols(onehot[rk, :], a_blk[pl.ds(0, slab), slot[i]]).astype(bf16)
            other(0, 1)
            m_copies[k, i].wait_recv()
            mine = x1[k, :, own_half].astype(f32)
        else:
            m_copies[k, i].wait_recv()
            mine = rows_cols(onehot[rk, :], a_blk[pl.ds(0, slab), slot[i]])
        merged[k][:, slot[i]] = jnp.where(here, mine, merged[k][:, slot[i]].astype(f32)).astype(bf16)

    def send_first(stage, k):
        cp = copies[stage, k]
        cp[TO_P, 0].start()
        cp[TO_Q, 0].start()
        cp[TO_P, 1].start()

    def start(stage, k):
        cp = copies[stage, k]
        if stage in (1, 2):
            for c_ in copies[stage - 1, k].values():
                c_.wait_send()

            def push(at):
                if stage == 1:
                    part[k, :, at] = rows_cols(x1[k], a_blk[:, at])
                else:
                    both = rows_cols(pick[pl.ds(0, 2 * m), two[0]], a_blk[:, at])
                    part[k, :, at] = both[:m] + both[m:]

            def mate_rows(pair):
                if (stage, k) == (1, 0):
                    for i in pair:
                        a_copies[i].wait_recv()

            mate_rows((0, 1))
            by_tiles(0, 3, push)
            send_first(stage, k)
            mate_rows((2, 3))
            by_tiles(3, 6, push)
            cp[TO_Q, 1].start()
        else:
            for msg in (0, 1):
                cp[TO_P, msg].start()
                cp[TO_Q, msg].start()

    def middle(stage, k):
        cp = copies[stage, k]
        for way in (TO_P, TO_Q):
            cp[way, 0].wait_recv()
            begin = 0 if way == TO_P else h
            dest = NEAR_Q if way == TO_P else NEAR_P
            if stage == 0:
                def select(i):
                    r = rows_at(i, begin)
                    rk = rows_at(i, k * m + begin)
                    here = (ids[rk, :] >= chip_f) & (ids[rk, :] < chip_f + 2 * slab)
                    merged[k][r, dest] = jnp.where(here, merged[k][r, dest].astype(f32),
                                                   far0[k, way, rows_at(i), :].astype(f32)).astype(bf16)
                by_rows(h, select)
            elif stage < 3:
                def add(i):
                    r = rows_at(i, begin)
                    part[k, r, dest] = part[k, r, dest] + far[stage - 1, k, way, rows_at(i), :]
                by_rows(h, add)
            cp[1 - way, 2].start()
            if (1 - way, 3) in cp:
                cp[1 - way, 3].start()

    def pull(buf, k, at, use, meanwhile=None):
        def split(i):
            r = rows_at(i)
            full = buf[k, r, at]
            top = full.astype(bf16)
            rest = full - top.astype(f32)
            mid = rest.astype(bf16)
            pick[r, at] = top
            pick[rows_at(i, m), at] = mid
            pick[rows_at(i, 2 * m), at] = (rest - mid.astype(f32)).astype(bf16)
        by_rows(m, split)

        def product(r):
            three = rows_rows(pick[pl.ds(0, 3 * m), at], a_blk[r, at])
            use(r, three[:m] + three[m:2 * m] + three[2 * m:])
        if meanwhile is None:
            by_tiles(0, 3, product)
        else:
            by_tiles(1, 3, product)
            meanwhile()
            by_tiles(0, 1, product)

    def close(k, at, z):
        bc[:, at] = bc[:, at] + jnp.sum(x1[k, :, at].astype(f32) * z, axis=0, keepdims=True)

    def last_far(n):
        k = CHUNKS - 1
        msg, begin, width = far_parts[n]
        copies[4, k][TO_P, msg].wait_recv()
        copies[4, k][TO_Q, msg].wait_recv()
        pull(part, k, pl.ds(begin, width), functools.partial(close, k))

    def last_own():
        pull(part, CHUNKS - 1, OWN, functools.partial(close, CHUNKS - 1))

    def last_nears():
        k = CHUNKS - 1
        copies[4, k][TO_P, 1].wait_recv()
        copies[4, k][TO_Q, 1].wait_recv()
        pull(part, k, pl.ds(slab, 2 * slab), functools.partial(close, k))

    def nears(stage, k):
        cp = copies[stage, k]
        cp[TO_P, 1].wait_recv()
        cp[TO_Q, 1].wait_recv()

        def keep(r, z):
            if stage == 3:
                near[1, k, :, r] = z
            else:
                close(k, r, z)
        pull(wg if stage == 3 else part, k, pl.ds(slab, 3 * slab), keep)

    def finish(stage, k):
        cp = copies[stage, k]
        for way in (TO_P, TO_Q):
            if stage < 3:
                cp[way, 1].wait_recv()
            cp[way, 2].wait_recv()
        if stage == 0:
            def first_level(i):
                r = rows_at(i)
                x1[k, r, own_half] = (merged[k][r, OWN].astype(f32) + near0[k, r, side[0]].astype(f32)
                                      + near0[k, r, side[1]].astype(f32)).astype(bf16)
            by_rows(m, first_level)
            x1_copies[k].start()
            if k == 0:
                a_copies[3].start()
                for copy in m_copies.values():
                    copy.wait_send()
            x1_copies[k].wait_recv()
        elif stage == 1:
            def second_level(i):
                r = rows_at(i)
                rk = rows_at(i, k * m)
                total = part[k, r, OWN] + near[0, k, r, side[0]] + near[0, k, r, side[1]]
                seen = jnp.maximum(onehot[rk, :].astype(f32), x1[k, r, own_half].astype(f32))
                x2own[k, r, :] = total * (1.0 - seen)
            by_rows(m, second_level)
            x2_copies[k].start()

            def split(i, source, half):
                r = rows_at(i)
                full = source[k, r, :]
                top = full.astype(bf16)
                pick[r, half] = top
                pick[rows_at(i, m), half] = (full - top.astype(f32)).astype(bf16)
            by_rows(m, lambda i: split(i, x2own, own_half))
            x2_copies[k].wait_recv()
            by_rows(m, lambda i: split(i, x2rcv, mate_half))
        elif stage == 2:
            def third_level(i):
                r = rows_at(i)
                rk = rows_at(i, k * m)
                total = part[k, r, OWN] + near[1, k, r, side[0]] + near[1, k, r, side[1]]
                seen = jnp.maximum(onehot[rk, :].astype(f32), x1[k, r, own_half].astype(f32))
                seen = jnp.maximum(seen, jnp.where(x2own[k, r, :] > 0, 1.0, 0.0))
                paths = total * (1.0 - seen)
                reached = paths > 0
                wg[k, r, OWN] = jnp.where(reached, lw[1] / jnp.where(reached, paths, 1.0), 0.0)
            by_rows(m, third_level)
            for c_ in cp.values():
                c_.wait_send()
        elif stage == 3:
            def keep(r, z):
                near[1, k, :, r] = near[1, k, :, r] + z
            pull(wg, k, FAR, keep, z_copies[k].start)
            z_copies[k].wait_recv()

            def second_weights(i):
                r = rows_at(i)
                paths = x2own[k, r, :]
                delta = paths * (near[1, k, r, own_half] + near[0, k, r, mate_half])
                reached = paths > 0
                part[k, r, OWN] = jnp.where(reached, (lw[0] + delta) / jnp.where(reached, paths, 1.0), 0.0)
                bc[:, own_half] = bc[:, own_half] + jnp.sum(delta, axis=0, keepdims=True)
            by_rows(m, second_weights)
        else:
            pull(part, k, FAR, functools.partial(close, k))

    def other(k, i):
        if k == 0:
            loads[0, i].wait()
        select_other(k, i)
        if (k, i) == (0, 0):
            pl.semaphore_wait(barrier, 3 + len(around))
            tell(0)
        m_copies[k, i].start()

    def own(k, i):
        if k == 0:
            loads[1, i].wait()
        select_own(k, i)

    def first_level_sends(k):
        own(k, 0)
        copies[0, k][TO_P, 0].start()
        copies[0, k][TO_Q, 0].start()
        if k == 0:
            other(0, 2)
            a_copies[0].start()
        own(k, 1)
        copies[0, k][TO_P, 1].start()
        own(k, 2)
        copies[0, k][TO_Q, 1].start()

    other(0, 0)
    first_level_sends(0)
    lax.fori_loop(m // blk, src_count // blk, one_hot_rows, 0)
    bc[...] = jnp.zeros_like(bc)
    for i in range(3):
        other(1, i)
    a_copies[1].start()
    for k in range(CHUNKS):
        other(k, 3)
    a_copies[2].start()
    middle(0, 0)
    first_level_sends(1)
    for k in range(CHUNKS):
        own(k, 3)
    middle(0, 1)
    for stage in range(1, 5):
        finish(stage - 1, 0)
        start(stage, 0)
        if stage == 4:
            nears(3, 1)
        middle(stage, 0)
        hear(stage - 1)
        if stage < 4:
            tell(stage)
        finish(stage - 1, 1)
        start(stage, 1)
        if stage >= 3:
            nears(stage, 0)
        if stage == 4:
            last_own()
        middle(stage, 1)
    finish(4, 0)
    last_nears()
    last_far(0)
    last_far(1)

    total[...] = bc[...] * scale
    keep_own = pltpu.make_async_copy(total.at[:, own_half], out.at[s_me], load_sem.at[0])
    keep_own.start()
    def distance(o):
        return -sum(min(n, SIDE - n) for n in (o % SIDE, o // SIDE))

    for o in sorted(range(planes), key=distance):
        there = lax.rem(s_me + o, planes)
        for other_core in (0, 1):
            if o == 0 and not other_core:
                continue
            device = {"src": there, "graph": x * 2 + (1 - c)} if other_core else {"src": there}
            pltpu.make_async_remote_copy(src_ref=total.at[:, side[other_core]], dst_ref=out.at[other_core * planes + s_me],
                                         send_sem=plane_s, recv_sem=plane_r,
                                         device_id=device, device_id_type=MESH).start()

    for copy in a_copies + x1_copies + x2_copies + z_copies:
        copy.wait_send()
    for k in range(CHUNKS):
        for stage in (3, 4):
            for c_ in copies[stage, k].values():
                c_.wait_send()
    keep_own.wait()
    arrivals = out.at[pl.ds(0, 2 * planes - 1)]
    every = pltpu.make_async_remote_copy(src_ref=arrivals, dst_ref=arrivals, send_sem=plane_s, recv_sem=plane_r,
                                         device_id=to_mate, device_id_type=MESH)
    every.wait_recv()
    every.wait_send()


def solution(mesh):
    planes = mesh.shape["src"]
    ring = mesh.shape["graph"] // 2

    def device_program(adj_slab, src_local, level_weight):
        slab, vertex_count = adj_slab.shape
        src_count = src_local.shape[0]
        m = src_count // CHUNKS
        scale = vertex_count / (src_count * planes * (level_weight.shape[0] + 1) ** 3)
        wide = 4 * slab
        vmem = pltpu.VMEM
        sem = pltpu.SemaphoreType.DMA
        mates = 4 + 7 * CHUNKS
        rings = 5 * CHUNKS * 8
        flops = 2 * 9 * src_count * slab * vertex_count
        bc = pl.pallas_call(
            functools.partial(kernel, ring, planes, scale),
            out_shape=jax.ShapeDtypeStruct((2 * planes, 1, slab), f32),
            in_specs=[pl.BlockSpec(memory_space=pl.ANY), pl.BlockSpec(memory_space=vmem), pl.BlockSpec(memory_space=pltpu.SMEM)],
            out_specs=pl.BlockSpec(memory_space=pl.ANY),
            scratch_shapes=[
                vmem((2 * slab, wide), bf16), vmem((slab, wide), bf16),
                vmem((2 * src_count, wide), bf16), vmem((src_count, 1), f32), vmem((src_count, slab), bf16),
                vmem((CHUNKS, m, 2 * slab), bf16), vmem((CHUNKS, m, slab), f32), vmem((CHUNKS, m, slab), f32),
                vmem((CHUNKS, m, wide), f32), vmem((CHUNKS, m, wide), f32),
                vmem((CHUNKS, m, 2 * slab), bf16), vmem((CHUNKS, 2, m // 2, slab), bf16),
                vmem((2, CHUNKS, m, 2 * slab), f32), vmem((2, CHUNKS, 2, m // 2, slab), f32),
                vmem((1, 2 * slab), f32), vmem((1, 2 * slab), f32),
                sem((8,)), sem((rings,)), sem((rings,)), sem((mates,)), sem((mates,)), sem, sem, pltpu.SemaphoreType.REGULAR((4,)),
            ],
            compiler_params=pltpu.CompilerParams(collective_id=0, has_side_effects=True, vmem_limit_bytes=67043328),
            cost_estimate=pl.CostEstimate(flops=flops, bytes_accessed=2 * slab * vertex_count, transcendentals=0),
        )(adj_slab, src_local.reshape(1, src_count), level_weight)
        return jnp.sum(bc, axis=(0, 1))

    return jax.shard_map(device_program, mesh=mesh,
                         in_specs=(P(("batch", "graph"), None), P(("batch", "src")), P(None)),
                         out_specs=P(("batch", "graph")), check_vma=False)
```

```python
import functools

import jax
import jax.numpy as jnp
from jax import lax
from jax.experimental import pallas as pl
from jax.experimental.pallas import tpu as pltpu
from jax.sharding import PartitionSpec as P

MESH = pl.DeviceIdType.MESH
f32, bf16 = jnp.float32, jnp.bfloat16
CHUNKS = 2
SIDE = 4
TO_P, TO_Q = 0, 1


def rows_cols(lhs, rhs):
    return lax.dot_general(lhs, rhs, (((1,), (0,)), ((), ())), preferred_element_type=f32)


def rows_rows(lhs, rhs):
    return lax.dot_general(lhs, rhs, (((1,), (1,)), ((), ())), preferred_element_type=f32)


def kernel(ring, planes, scale, adj, src, lw, out,
           a_blk, a_oth, pick, ids, onehot, x1, x2own, x2rcv, part, wg,
           near0, far0, near, far, bc, total,
           load_sem, ssem, rsem, d2d_s, d2d_r, plane_s, plane_r, rounds):
    slab = a_oth.shape[0]
    cols_all = a_oth.shape[1]
    src_count = ids.shape[0]
    m = src_count // CHUNKS
    h = m // 2
    tile = 2 * slab // 3
    blk = min(32, h)

    g = lax.axis_index("graph")
    s_me = lax.axis_index("src")
    x, c = g // 2, g % 2
    odd = lax.rem(x, 2)
    chip_p = x + 1 - 2 * odd
    chip_q = lax.rem(x + ring - 1 + 2 * odd, ring)
    chip_far = lax.rem(x + 2, ring)
    to_p = {"graph": chip_p * 2 + c}
    to_q = {"graph": chip_q * 2 + c}
    to_mate = {"graph": x * 2 + (1 - c)}
    chips = (chip_far, chip_p, chip_q, x)
    slot = [pl.ds(i * slab, slab) for i in range(4)]
    FAR, NEAR_P, NEAR_Q, OWN = slot

    loads = {}
    for i, chip in enumerate(chips):
        for own in (0, 1):
            at = pl.ds(pl.multiple_of((chip * 2 + (c if own else 1 - c)) * slab, 128), slab)
            target = a_blk.at[pl.ds(0, slab), slot[i]] if own else a_oth.at[:, slot[i]]
            loads[own, i] = pltpu.make_async_copy(adj.at[:, at], target, load_sem.at[4 * own + i])
    for own, i in ((0, 0), (1, 0), (0, 1), (0, 2), (1, 1), (1, 2), (0, 3), (1, 3)):
        loads[own, i].start()

    barrier = pltpu.get_barrier_semaphore()
    for dev in (to_p, to_q, to_mate):
        pl.semaphore_signal(barrier, inc=1, device_id=dev, device_id_type=MESH)
    if planes == SIDE * SIDE:
        row_, col_ = s_me // SIDE, lax.rem(s_me, SIDE)
        around = [{"src": row_ * SIDE + lax.rem(col_ + step, SIDE)} for step in (1, SIDE - 1)]
        around += [{"src": lax.rem(row_ + step, SIDE) * SIDE + col_} for step in (1, SIDE - 1)]
    else:
        around = [{"src": lax.rem(s_me + o, planes), "graph": x * 2 + core} for o in range(1, planes) for core in (0, 1)]
    for dev in around:
        pl.semaphore_signal(barrier, inc=1, device_id=dev, device_id_type=MESH)

    def tell(n):
        for dev in around:
            pl.semaphore_signal(rounds.at[n], inc=1, device_id=dev, device_id_type=MESH)

    def hear(n):
        pl.semaphore_wait(rounds.at[n], len(around))

    row = lax.broadcasted_iota(jnp.int32, (src_count, src_count), 0)
    col = lax.broadcasted_iota(jnp.int32, (src_count, src_count), 1)
    ids[...] = jnp.sum(jnp.where(row == col, src[...].astype(f32), 0.0), axis=1, keepdims=True)
    base = g * slab
    base_f = base.astype(f32)
    chip_f = (x * 2 * slab).astype(f32)
    lane = (lax.broadcasted_iota(jnp.int32, (blk, slab), 1) + base).astype(f32)

    def one_hot_rows(i, carry):
        r = pl.ds(pl.multiple_of(i * blk, blk), blk)
        onehot[r, :] = jnp.where(ids[r, :] == lane, 1.0, 0.0).astype(bf16)
        return carry

    lax.fori_loop(0, m // blk, one_hot_rows, 0)

    def mate_copy(i, source, target):
        return pltpu.make_async_remote_copy(src_ref=source, dst_ref=target, send_sem=d2d_s.at[i], recv_sem=d2d_r.at[i],
                                            device_id=to_mate, device_id_type=MESH)

    def ring_copy(stage, k, way, msg, source, target):
        i = ((stage * CHUNKS + k) * 2 + way) * 4 + msg
        return pltpu.make_async_remote_copy(src_ref=source, dst_ref=target, send_sem=ssem.at[i], recv_sem=rsem.at[i],
                                            device_id=to_p if way == TO_P else to_q, device_id_type=MESH)

    lo, hi = pl.ds(0, h), pl.ds(h, h)
    side = [pl.ds(0, slab), pl.ds(slab, slab)]
    own_half, mate_half = side
    merged = [pick.at[pl.ds(src_count + k * m, m), :] for k in range(CHUNKS)]
    two = [pl.ds(0, 2 * slab), pl.ds(2 * slab, 2 * slab)]

    def reduce_copies(stage, k):
        if stage == 0:
            send, nr, fr = merged[k], near0.at[k], far0.at[k]
        else:
            send, nr, fr = part.at[k], near.at[stage - 1, k], far.at[stage - 1, k]
        return {
            (TO_P, 0): ring_copy(stage, k, TO_P, 0, send.at[lo, FAR], fr.at[TO_P]),
            (TO_Q, 0): ring_copy(stage, k, TO_Q, 0, send.at[hi, FAR], fr.at[TO_Q]),
            (TO_P, 1): ring_copy(stage, k, TO_P, 1, send.at[lo, NEAR_P], nr.at[lo, side[TO_P]]),
            (TO_Q, 1): ring_copy(stage, k, TO_Q, 1, send.at[hi, NEAR_Q], nr.at[hi, side[TO_Q]]),
            (TO_P, 2): ring_copy(stage, k, TO_P, 2, send.at[hi, NEAR_P], nr.at[hi, side[TO_P]]),
            (TO_Q, 2): ring_copy(stage, k, TO_Q, 2, send.at[lo, NEAR_Q], nr.at[lo, side[TO_Q]]),
        }

    tail = slab // 256 * 128
    far_parts = [(2, 0, slab - tail), (3, slab - tail, tail)]

    def gather_copies(stage, k):
        buf = wg.at[k] if stage == 3 else part.at[k]
        if (stage, k) == (4, CHUNKS - 1):
            bands = far_parts
        else:
            bands = [(2, 0, slab)]
        relay = {}
        for msg, begin, width in bands:
            from_p, from_q, to_far = [pl.ds(n * slab + begin, width) for n in (1, 2, 0)]
            relay[TO_P, msg] = ring_copy(stage, k, TO_P, msg, buf.at[hi, from_q], buf.at[hi, to_far])
            relay[TO_Q, msg] = ring_copy(stage, k, TO_Q, msg, buf.at[lo, from_p], buf.at[lo, to_far])
        return {
            **relay,
            (TO_P, 0): ring_copy(stage, k, TO_P, 0, buf.at[lo, OWN], buf.at[lo, NEAR_P]),
            (TO_Q, 0): ring_copy(stage, k, TO_Q, 0, buf.at[hi, OWN], buf.at[hi, NEAR_Q]),
            (TO_P, 1): ring_copy(stage, k, TO_P, 1, buf.at[hi, OWN], buf.at[hi, NEAR_P]),
            (TO_Q, 1): ring_copy(stage, k, TO_Q, 1, buf.at[lo, OWN], buf.at[lo, NEAR_Q]),
        }

    copies = {}
    for k in range(CHUNKS):
        for stage in range(5):
            copies[stage, k] = reduce_copies(stage, k) if stage < 3 else gather_copies(stage, k)
    a_copies = [mate_copy(i, a_oth.at[:, slot[i]], a_blk.at[pl.ds(slab, slab), slot[i]]) for i in range(4)]
    m_copies = {(k, i): mate_copy(4 + 4 * k + i, pick.at[pl.ds(k * m, m), slot[i]], merged[k].at[:, slot[i]])
                for k in range(CHUNKS) for i in range(4)}
    first = 4 + 4 * CHUNKS
    x1_copies = [mate_copy(first + k, x1.at[k, :, own_half], x1.at[k, :, mate_half]) for k in range(CHUNKS)]
    x2_copies = [mate_copy(first + CHUNKS + k, x2own.at[k], x2rcv.at[k]) for k in range(CHUNKS)]
    z_copies = [mate_copy(first + 2 * CHUNKS + k, near.at[1, k, :, mate_half], near.at[0, k, :, mate_half]) for k in range(CHUNKS)]

    def by_rows(count, fn):
        def step(i, carry):
            fn(i)
            return carry
        lax.fori_loop(0, count // blk, step, 0)

    def rows_at(i, start=0):
        return pl.ds(pl.multiple_of(start + i * blk, blk), blk)

    def by_tiles(begin, end, fn, unroll=False):
        def step(t, carry):
            fn(pl.ds(pl.multiple_of(t * tile, 128), tile))
            return carry
        lax.fori_loop(begin, end, step, 0, unroll=unroll)

    def select_other(k, i):
        pick[pl.ds(k * m, m), slot[i]] = rows_cols(onehot[pl.ds(k * m, m), :], a_oth[:, slot[i]]).astype(bf16)

    def select_own(k, i):
        rk = pl.ds(k * m, m)
        here = (ids[rk, :] >= base_f) & (ids[rk, :] < base_f + slab)
        if (k, i) == (0, 0):
            x1[k, :, own_half] = rows_cols(onehot[rk, :], a_blk[pl.ds(0, slab), slot[i]]).astype(bf16)
            other(0, 1)
            m_copies[k, i].wait_recv()
            mine = x1[k, :, own_half].astype(f32)
        else:
            m_copies[k, i].wait_recv()
            mine = rows_cols(onehot[rk, :], a_blk[pl.ds(0, slab), slot[i]])
        merged[k][:, slot[i]] = jnp.where(here, mine, merged[k][:, slot[i]].astype(f32)).astype(bf16)

    def send_first(stage, k):
        cp = copies[stage, k]
        cp[TO_P, 0].start()
        cp[TO_Q, 0].start()
        cp[TO_P, 1].start()

    def start(stage, k):
        cp = copies[stage, k]
        if stage in (1, 2):
            for c_ in copies[stage - 1, k].values():
                c_.wait_send()

            def push(at):
                if stage == 1:
                    part[k, :, at] = rows_cols(x1[k], a_blk[:, at])
                else:
                    both = rows_cols(pick[pl.ds(0, 2 * m), two[0]], a_blk[:, at])
                    part[k, :, at] = both[:m] + both[m:]

            def mate_rows(pair):
                if (stage, k) == (1, 0):
                    for i in pair:
                        a_copies[i].wait_recv()

            mate_rows((0, 1))
            by_tiles(0, 3, push)
            send_first(stage, k)
            mate_rows((2, 3))
            by_tiles(3, 6, push)
            cp[TO_Q, 1].start()
        else:
            for msg in (0, 1):
                cp[TO_P, msg].start()
                cp[TO_Q, msg].start()

    def middle(stage, k):
        cp = copies[stage, k]
        for way in (TO_P, TO_Q):
            cp[way, 0].wait_recv()
            begin = 0 if way == TO_P else h
            dest = NEAR_Q if way == TO_P else NEAR_P
            if stage == 0:
                def select(i):
                    r = rows_at(i, begin)
                    rk = rows_at(i, k * m + begin)
                    here = (ids[rk, :] >= chip_f) & (ids[rk, :] < chip_f + 2 * slab)
                    merged[k][r, dest] = jnp.where(here, merged[k][r, dest].astype(f32),
                                                   far0[k, way, rows_at(i), :].astype(f32)).astype(bf16)
                by_rows(h, select)
            elif stage < 3:
                def add(i):
                    r = rows_at(i, begin)
                    part[k, r, dest] = part[k, r, dest] + far[stage - 1, k, way, rows_at(i), :]
                by_rows(h, add)
            cp[1 - way, 2].start()
            if (1 - way, 3) in cp:
                cp[1 - way, 3].start()

    def pull(buf, k, at, use, meanwhile=None, unroll=False):
        def split(i):
            r = rows_at(i)
            full = buf[k, r, at]
            top = full.astype(bf16)
            rest = full - top.astype(f32)
            mid = rest.astype(bf16)
            pick[r, at] = top
            pick[rows_at(i, m), at] = mid
            pick[rows_at(i, 2 * m), at] = (rest - mid.astype(f32)).astype(bf16)
        by_rows(m, split)

        def product(r):
            three = rows_rows(pick[pl.ds(0, 3 * m), at], a_blk[r, at])
            use(r, three[:m] + three[m:2 * m] + three[2 * m:])
        if meanwhile is None:
            by_tiles(0, 3, product, unroll)
        else:
            by_tiles(1, 3, product)
            meanwhile()
            by_tiles(0, 1, product)

    def close(k, at, z):
        bc[:, at] = bc[:, at] + jnp.sum(x1[k, :, at].astype(f32) * z, axis=0, keepdims=True)

    def last_far(n):
        k = CHUNKS - 1
        msg, begin, width = far_parts[n]
        copies[4, k][TO_P, msg].wait_recv()
        copies[4, k][TO_Q, msg].wait_recv()
        pull(part, k, pl.ds(begin, width), functools.partial(close, k), unroll=True)

    def last_own():
        pull(part, CHUNKS - 1, OWN, functools.partial(close, CHUNKS - 1))

    def last_nears():
        k = CHUNKS - 1
        copies[4, k][TO_P, 1].wait_recv()
        copies[4, k][TO_Q, 1].wait_recv()
        pull(part, k, pl.ds(slab, 2 * slab), functools.partial(close, k))

    def nears(stage, k):
        cp = copies[stage, k]
        cp[TO_P, 1].wait_recv()
        cp[TO_Q, 1].wait_recv()

        def keep(r, z):
            if stage == 3:
                near[1, k, :, r] = z
            else:
                close(k, r, z)
        pull(wg if stage == 3 else part, k, pl.ds(slab, 3 * slab), keep)

    def finish(stage, k):
        cp = copies[stage, k]
        for way in (TO_P, TO_Q):
            if stage < 3:
                cp[way, 1].wait_recv()
            cp[way, 2].wait_recv()
        if stage == 0:
            def first_level(i):
                r = rows_at(i)
                x1[k, r, own_half] = (merged[k][r, OWN].astype(f32) + near0[k, r, side[0]].astype(f32)
                                      + near0[k, r, side[1]].astype(f32)).astype(bf16)
            by_rows(m, first_level)
            x1_copies[k].start()
            if k == 0:
                a_copies[3].start()
                for copy in m_copies.values():
                    copy.wait_send()
            x1_copies[k].wait_recv()
        elif stage == 1:
            def second_level(i):
                r = rows_at(i)
                rk = rows_at(i, k * m)
                total = part[k, r, OWN] + near[0, k, r, side[0]] + near[0, k, r, side[1]]
                seen = jnp.maximum(onehot[rk, :].astype(f32), x1[k, r, own_half].astype(f32))
                x2own[k, r, :] = total * (1.0 - seen)
            by_rows(m, second_level)
            x2_copies[k].start()

            def split(i, source, half):
                r = rows_at(i)
                full = source[k, r, :]
                top = full.astype(bf16)
                pick[r, half] = top
                pick[rows_at(i, m), half] = (full - top.astype(f32)).astype(bf16)
            by_rows(m, lambda i: split(i, x2own, own_half))
            x2_copies[k].wait_recv()
            by_rows(m, lambda i: split(i, x2rcv, mate_half))
        elif stage == 2:
            def third_level(i):
                r = rows_at(i)
                rk = rows_at(i, k * m)
                total = part[k, r, OWN] + near[1, k, r, side[0]] + near[1, k, r, side[1]]
                seen = jnp.maximum(onehot[rk, :].astype(f32), x1[k, r, own_half].astype(f32))
                seen = jnp.maximum(seen, jnp.where(x2own[k, r, :] > 0, 1.0, 0.0))
                paths = total * (1.0 - seen)
                reached = paths > 0
                wg[k, r, OWN] = jnp.where(reached, lw[1] / jnp.where(reached, paths, 1.0), 0.0)
            by_rows(m, third_level)
            for c_ in cp.values():
                c_.wait_send()
        elif stage == 3:
            def keep(r, z):
                near[1, k, :, r] = near[1, k, :, r] + z
            pull(wg, k, FAR, keep, z_copies[k].start)
            z_copies[k].wait_recv()

            def second_weights(i):
                r = rows_at(i)
                paths = x2own[k, r, :]
                delta = paths * (near[1, k, r, own_half] + near[0, k, r, mate_half])
                reached = paths > 0
                part[k, r, OWN] = jnp.where(reached, (lw[0] + delta) / jnp.where(reached, paths, 1.0), 0.0)
                bc[:, own_half] = bc[:, own_half] + jnp.sum(delta, axis=0, keepdims=True)
            by_rows(m, second_weights)
        else:
            pull(part, k, FAR, functools.partial(close, k))

    def other(k, i):
        if k == 0:
            loads[0, i].wait()
        select_other(k, i)
        if (k, i) == (0, 0):
            pl.semaphore_wait(barrier, 3 + len(around))
            tell(0)
        m_copies[k, i].start()

    def own(k, i):
        if k == 0:
            loads[1, i].wait()
        select_own(k, i)

    def first_level_sends(k):
        own(k, 0)
        copies[0, k][TO_P, 0].start()
        copies[0, k][TO_Q, 0].start()
        if k == 0:
            other(0, 2)
            a_copies[0].start()
        own(k, 1)
        copies[0, k][TO_P, 1].start()
        own(k, 2)
        copies[0, k][TO_Q, 1].start()

    other(0, 0)
    first_level_sends(0)
    lax.fori_loop(m // blk, src_count // blk, one_hot_rows, 0)
    bc[...] = jnp.zeros_like(bc)
    for i in range(3):
        other(1, i)
    a_copies[1].start()
    for k in range(CHUNKS):
        other(k, 3)
    a_copies[2].start()
    middle(0, 0)
    first_level_sends(1)
    for k in range(CHUNKS):
        own(k, 3)
    middle(0, 1)
    for stage in range(1, 5):
        finish(stage - 1, 0)
        start(stage, 0)
        if stage == 4:
            nears(3, 1)
        middle(stage, 0)
        hear(stage - 1)
        if stage < 4:
            tell(stage)
        finish(stage - 1, 1)
        start(stage, 1)
        if stage >= 3:
            nears(stage, 0)
        if stage == 4:
            last_own()
        middle(stage, 1)
    finish(4, 0)
    last_nears()
    last_far(0)
    last_far(1)

    total[...] = bc[...] * scale
    keep_own = pltpu.make_async_copy(total.at[:, own_half], out.at[s_me], load_sem.at[0])
    keep_own.start()
    for o in range(planes):
        there = lax.rem(s_me + o, planes)
        for other_core in (0, 1):
            if o == 0 and not other_core:
                continue
            device = {"src": there, "graph": x * 2 + (1 - c)} if other_core else {"src": there}
            pltpu.make_async_remote_copy(src_ref=total.at[:, side[other_core]], dst_ref=out.at[other_core * planes + s_me],
                                         send_sem=plane_s, recv_sem=plane_r,
                                         device_id=device, device_id_type=MESH).start()

    for copy in a_copies + x1_copies + x2_copies + z_copies:
        copy.wait_send()
    for k in range(CHUNKS):
        for stage in (3, 4):
            for c_ in copies[stage, k].values():
                c_.wait_send()
    keep_own.wait()
    arrivals = out.at[pl.ds(0, 2 * planes - 1)]
    every = pltpu.make_async_remote_copy(src_ref=arrivals, dst_ref=arrivals, send_sem=plane_s, recv_sem=plane_r,
                                         device_id=to_mate, device_id_type=MESH)
    every.wait_recv()
    every.wait_send()


def solution(mesh):
    planes = mesh.shape["src"]
    ring = mesh.shape["graph"] // 2

    def device_program(adj_slab, src_local, level_weight):
        slab, vertex_count = adj_slab.shape
        src_count = src_local.shape[0]
        m = src_count // CHUNKS
        scale = vertex_count / (src_count * planes * (level_weight.shape[0] + 1) ** 3)
        wide = 4 * slab
        vmem = pltpu.VMEM
        sem = pltpu.SemaphoreType.DMA
        mates = 4 + 7 * CHUNKS
        rings = 5 * CHUNKS * 8
        flops = 2 * 9 * src_count * slab * vertex_count
        bc = pl.pallas_call(
            functools.partial(kernel, ring, planes, scale),
            out_shape=jax.ShapeDtypeStruct((2 * planes, 1, slab), f32),
            in_specs=[pl.BlockSpec(memory_space=pl.ANY), pl.BlockSpec(memory_space=vmem), pl.BlockSpec(memory_space=pltpu.SMEM)],
            out_specs=pl.BlockSpec(memory_space=pl.ANY),
            scratch_shapes=[
                vmem((2 * slab, wide), bf16), vmem((slab, wide), bf16),
                vmem((2 * src_count, wide), bf16), vmem((src_count, 1), f32), vmem((src_count, slab), bf16),
                vmem((CHUNKS, m, 2 * slab), bf16), vmem((CHUNKS, m, slab), f32), vmem((CHUNKS, m, slab), f32),
                vmem((CHUNKS, m, wide), f32), vmem((CHUNKS, m, wide), f32),
                vmem((CHUNKS, m, 2 * slab), bf16), vmem((CHUNKS, 2, m // 2, slab), bf16),
                vmem((2, CHUNKS, m, 2 * slab), f32), vmem((2, CHUNKS, 2, m // 2, slab), f32),
                vmem((1, 2 * slab), f32), vmem((1, 2 * slab), f32),
                sem((8,)), sem((rings,)), sem((rings,)), sem((mates,)), sem((mates,)), sem, sem, pltpu.SemaphoreType.REGULAR((4,)),
            ],
            compiler_params=pltpu.CompilerParams(collective_id=0, has_side_effects=True, vmem_limit_bytes=67043328),
            cost_estimate=pl.CostEstimate(flops=flops, bytes_accessed=2 * slab * vertex_count, transcendentals=0),
        )(adj_slab, src_local.reshape(1, src_count), level_weight)
        return jnp.sum(bc, axis=(0, 1))

    return jax.shard_map(device_program, mesh=mesh,
                         in_specs=(P(("batch", "graph"), None), P(("batch", "src")), P(None)),
                         out_specs=P(("batch", "graph")), check_vma=False)
```
